16 devices in a mesh: rep: 2 (over y, z), dp: 8 (over x, core).
Axes of the slice: x: 4, y: 2, z: 1, core: 2. Of those that a mesh axis runs over, the one named last changes fastest.
The devices are a block of a 4x4x8 slice.
Arguments:
- x: bfloat16 [16, 2048, 1024], P(('rep', 'dp')), parts along dimension 0
- dy: bfloat16 [16, 2048, 1024], P(('rep', 'dp')), parts along dimension 0
- wq: bfloat16 [2, 1024, 1024], P(None, 'dp')
- wk: bfloat16 [2, 1024, 256], P(None, 'dp')
- wv: bfloat16 [2, 1024, 256], P(None, 'dp')
- wo: bfloat16 [2, 1024, 1024], P(None, 'dp')
- w_gate: bfloat16 [2, 1024, 3200], P(None, 'dp')
- w_up: bfloat16 [2, 1024, 3200], P(None, 'dp')
- w_down: bfloat16 [2, 3200, 1024], P(None, 'dp')
- m_wq: float32 [2, 1024, 1024], P(None, 'dp')
- m_wk: float32 [2, 1024, 256], P(None, 'dp')
- m_wv: float32 [2, 1024, 256], P(None, 'dp')
- m_wo: float32 [2, 1024, 1024], P(None, 'dp')
- m_w_gate: float32 [2, 1024, 3200], P(None, 'dp')
- m_w_up: float32 [2, 1024, 3200], P(None, 'dp')
- m_w_down: float32 [2, 3200, 1024], P(None, 'dp')
- v_wq: float32 [2, 1024, 1024], P(None, 'dp')
- v_wk: float32 [2, 1024, 256], P(None, 'dp')
- v_wv: float32 [2, 1024, 256], P(None, 'dp')
- v_wo: float32 [2, 1024, 1024], P(None, 'dp')
- v_w_gate: float32 [2, 1024, 3200], P(None, 'dp')
- v_w_up: float32 [2, 1024, 3200], P(None, 'dp')
- v_w_down: float32 [2, 3200, 1024], P(None, 'dp')
Outputs:
- output 1: bfloat16 [4, 1024, 1024], P('rep', 'dp'), parts along dimension 0
- output 2: bfloat16 [4, 1024, 256], P('rep', 'dp'), parts along dimension 0
- output 3: bfloat16 [4, 1024, 256], P('rep', 'dp'), parts along dimension 0
- output 4: bfloat16 [4, 1024, 1024], P('rep', 'dp'), parts along dimension 0
- output 5: bfloat16 [4, 1024, 3200], P('rep', 'dp'), parts along dimension 0
- output 6: bfloat16 [4, 1024, 3200], P('rep', 'dp'), parts along dimension 0
- output 7: bfloat16 [4, 3200, 1024], P('rep', 'dp'), parts along dimension 0
- output 8: float32 [4, 1024, 1024], P('rep', 'dp'), parts along dimension 0
- output 9: float32 [4, 1024, 256], P('rep', 'dp'), parts along dimension 0
- output 10: float32 [4, 1024, 256], P('rep', 'dp'), parts along dimension 0
- output 11: float32 [4, 1024, 1024], P('rep', 'dp'), parts along dimension 0
- output 12: float32 [4, 1024, 3200], P('rep', 'dp'), parts along dimension 0
- output 13: float32 [4, 1024, 3200], P('rep', 'dp'), parts along dimension 0
- output 14: float32 [4, 3200, 1024], P('rep', 'dp'), parts along dimension 0
- output 15: float32 [4, 1024, 1024], P('rep', 'dp'), parts along dimension 0
- output 16: float32 [4, 1024, 256], P('rep', 'dp'), parts along dimension 0
- output 17: float32 [4, 1024, 256], P('rep', 'dp'), parts along dimension 0
- output 18: float32 [4, 1024, 1024], P('rep', 'dp'), parts along dimension 0
- output 19: float32 [4, 1024, 3200], P('rep', 'dp'), parts along dimension 0
- output 20: float32 [4, 1024, 3200], P('rep', 'dp'), parts along dimension 0
- output 21: float32 [4, 3200, 1024], P('rep', 'dp'), parts along dimension 0
There are 2 independent parts. The reference program is written for one: setup_inputs(seed, part) draws one part's arguments, and reference() takes and returns one part's arrays. A program takes and returns all parts, laid end to end along the dimension named above; an argument that names none is the same for every part.
All inputs are finite; a program needn't handle non-finite values.
Results may differ from the reference program's by a relative error of at most 0.0269.
Values are sent between devices in bfloat16 or wider.
A program may use at most 768 MiB of HBM per device.

```python
import jax
import jax.numpy as jnp
from jax import lax

SEQUENCES = 8
TOKENS = 2048
D = 1024
HEADS = 8
KV_HEADS = 2
HEAD = 128
FF = 3200
LAYERS = 2
THETA = 10000
NAMES = ("wq", "wk", "wv", "wo", "w_gate", "w_up", "w_down")
SHAPES = {
    "wq": (LAYERS, D, HEADS * HEAD),
    "wk": (LAYERS, D, KV_HEADS * HEAD),
    "wv": (LAYERS, D, KV_HEADS * HEAD),
    "wo": (LAYERS, HEADS * HEAD, D),
    "w_gate": (LAYERS, D, FF),
    "w_up": (LAYERS, D, FF),
    "w_down": (LAYERS, FF, D),
}


def bump(key, n, height):
    away = (jnp.arange(n, dtype=jnp.int32) - jax.random.randint(key, (), 0, n, jnp.int32)) % n
    return jnp.where(away < n // 8, height, 1.0)


def together(key, own, strength):
    shared = jax.random.normal(key, own.shape[1:], jnp.float32)
    return (own + strength * shared) * lax.rsqrt(1 + strength * strength)


def setup_inputs(seed: int = 0, part: int = 0) -> dict:
    kx, kdy, ka, kb, kz, kf, kh, kl, *keys = jax.random.split(jax.random.key(seed), 8 + 3 * len(NAMES))
    kx, kdy, ka, kb = (jax.random.fold_in(k, part) for k in (kx, kdy, ka, kb))
    kw, km, kv = (keys[i::3] for i in range(3))
    shape = (SEQUENCES, TOKENS, D)
    much_x, much_dy = jax.random.uniform(kz, (2,), jnp.float32, 0.0, 1.0)
    loud = 2.0 ** jax.random.uniform(jax.random.fold_in(kz, 1), (), jnp.float32, -1.0, 2.0)
    layers = 2.0 ** jax.random.uniform(kl, (LAYERS, 1, 1), jnp.float32, -1.0, 1.0)
    times = {"wq": 1.0, "wk": 1.0, "wv": 2.0, "wo": layers, "w_gate": 1.0, "w_up": bump(kh, FF, 4.0), "w_down": layers}
    x = together(ka, jax.random.normal(kx, shape, jnp.float32), much_x) * bump(kf, D, 4.0)
    dy = together(kb, jax.random.normal(kdy, shape, jnp.float32), much_dy)
    drawn = {"x": x.astype(jnp.bfloat16), "dy": (loud * dy * (SEQUENCES * TOKENS) ** -0.5).astype(jnp.bfloat16)}
    for key, name in zip(kw, NAMES, strict=True):
        drawn[name] = (jax.random.normal(key, SHAPES[name], jnp.float32) * SHAPES[name][1] ** -0.5 * times[name]).astype(jnp.bfloat16)
    for key, name in zip(km, NAMES, strict=True):
        drawn[f"m_{name}"] = 0.1 * jax.random.normal(key, SHAPES[name], jnp.float32)
    for key, name in zip(kv, NAMES, strict=True):
        drawn[f"v_{name}"] = loud * loud * jax.random.uniform(key, SHAPES[name], jnp.float32, 0.2, 0.6)
    return drawn


def matmul(a, w):
    return jnp.dot(a, w, preferred_element_type=jnp.float32).astype(jnp.bfloat16)


def normed(h):
    wide = h.astype(jnp.float32)
    scale = lax.rsqrt(jnp.mean(wide**2, -1, keepdims=True) + 1e-6)
    return (wide * scale).astype(jnp.bfloat16)


def turned(t, theta):
    half = t.shape[-1] // 2
    angle = jnp.arange(t.shape[0], dtype=jnp.float32)[:, None] * theta ** (-jnp.arange(half, dtype=jnp.float32) / half)
    cos, sin = jnp.cos(angle)[:, None], jnp.sin(angle)[:, None]
    a, b = t[..., :half].astype(jnp.float32), t[..., half:].astype(jnp.float32)
    return jnp.concatenate([a * cos - b * sin, b * cos + a * sin], -1).astype(jnp.bfloat16)


def seen_by(q, k, v):
    tokens, kv = q.shape[0], k.shape[1]
    q = q.reshape(tokens, kv, -1, q.shape[-1])
    scores = jnp.einsum("tgsd,ugd->gstu", q.astype(jnp.float32), k.astype(jnp.float32)) * q.shape[-1] ** -0.5
    place = jnp.arange(tokens)
    weights = jax.nn.softmax(jnp.where(place[:, None] >= place, scores, -jnp.inf), -1).astype(jnp.bfloat16)
    return jnp.einsum("gstu,ugd->tgsd", weights.astype(jnp.float32), v.astype(jnp.float32)).astype(jnp.bfloat16).reshape(tokens, -1)


def layer(h, w):
    a = normed(h)
    q, k = (turned(matmul(a, w[name]).reshape(h.shape[0], -1, HEAD), THETA) for name in ("wq", "wk"))
    h = h + matmul(seen_by(q, k, matmul(a, w["wv"]).reshape(h.shape[0], -1, HEAD)), w["wo"])
    b = normed(h)
    gate = jnp.dot(b, w["w_gate"], preferred_element_type=jnp.float32)
    up = jnp.dot(b, w["w_up"], preferred_element_type=jnp.float32)
    return h + matmul((jax.nn.silu(gate) * up).astype(jnp.bfloat16), w["w_down"])


def adamw(w, m, v, g):
    m = 0.9 * m + 0.1 * g
    v = 0.95 * v + 0.05 * g * g
    step = m * lax.rsqrt(v + 1e-8) + 0.1 * w
    return (w - 0.02 * step).astype(jnp.bfloat16), m, v


def stack(weights, h):
    return lax.scan(lambda h, w: (layer(h, w), None), h, weights)[0]


def reference(x, dy, wq, wk, wv, wo, w_gate, w_up, w_down, m_wq, m_wk, m_wv, m_wo, m_w_gate, m_w_up, m_w_down, v_wq, v_wk, v_wv, v_wo, v_w_gate, v_w_up, v_w_down):
    weights = dict(zip(NAMES, (wq, wk, wv, wo, w_gate, w_up, w_down), strict=True))

    def take(so_far, sequence):
        h, by_y = sequence
        _, back = jax.vjp(stack, weights, h)
        by_weights, by_h = back(by_y)
        return jax.tree.map(lambda total, term: total + term.astype(jnp.float32), so_far, by_weights), by_h

    none_yet = {name: jnp.zeros(w.shape, jnp.float32) for name, w in weights.items()}
    by_weights, by_x = lax.scan(take, none_yet, (x, dy))
    gradients = [by_weights[name].astype(jnp.bfloat16).astype(jnp.float32) for name in NAMES]
    first = (m_wq, m_wk, m_wv, m_wo, m_w_gate, m_w_up, m_w_down)
    second = (v_wq, v_wk, v_wv, v_wo, v_w_gate, v_w_up, v_w_down)
    new = [adamw(weights[name].astype(jnp.float32), m, v, g) for name, m, v, g in zip(NAMES, first, second, gradients, strict=True)]
    return tuple(one[which] for which in range(3) for one in new)
```

```python
import functools

import jax
import jax.numpy as jnp
import numpy as np
from jax import lax
from jax.experimental import pallas as pl
from jax.experimental.pallas import tpu as pltpu
from jax.sharding import PartitionSpec as P

f32, bf16 = jnp.float32, jnp.bfloat16
sh = jax.ShapeDtypeStruct
HEAD = 128
THETA = 10000
NEG = -1e30
HIDDEN = 2 * NEG
LOG2E = 1.4426950408889634
ANY = pl.BlockSpec(memory_space=pl.ANY)
BIG = 63 * 2**20


def dot(a, b, ca=1, cb=0):
    return lax.dot_general(a, b, (((ca,), (cb,)), ((), ())), preferred_element_type=f32)


def once(shape, index):
    return pl.BlockSpec(shape, index, pipeline_mode=pl.Buffered(1))


def whole(a):
    return a, once(a.shape, lambda *_: (0,) * a.ndim)


def rms(wide):
    return lax.rsqrt(jnp.mean(wide * wide, -1, keepdims=True) + 1e-6)


def norm_back(wide, db):
    r = rms(wide)
    return r * db - wide * (r * r * r * (jnp.sum(db * wide, -1, keepdims=True) * (1 / wide.shape[1])))


def params(n, **kw):
    return pltpu.CompilerParams(dimension_semantics=("arbitrary",) * n, vmem_limit_bytes=BIG, **kw)


class Place:
    def __init__(self, dp):
        me = lax.axis_index("dp")
        self.chips = dp // 2
        self.chip, self.core = me // 2, lax.rem(me, 2)
        self.other = 1 - self.core

    def at(self, step):
        return lax.rem(self.chip + step + self.chips, self.chips)

    def slot(self, step, core):
        return 2 * self.at(step) + core

    def partner(self):
        return {"dp": self.slot(0, self.other)}

    def neighbour(self, step):
        return {"dp": self.slot(step, self.core)}


def remote(src, dst, send, recv, device):
    return pltpu.make_async_remote_copy(src_ref=src, dst_ref=dst, send_sem=send, recv_sem=recv, device_id=device,
                                        device_id_type=pl.DeviceIdType.MESH)


def _half(rows):
    return -(-rows // 32) * 16


class Gather:
    def __init__(self, w, number, dp):
        self.w, self.number, self.dp = w, number, dp
        self.rows, self.n = w.shape[1:]
        self.inputs = [w]
        self.outs = [sh((dp, self.rows, self.n), w.dtype)]
        self.scratch = [pltpu.VMEM((self.rows, self.n), w.dtype), pltpu.SemaphoreType.DMA((8,)), pltpu.SemaphoreType.DMA((8,)),
                        pltpu.SemaphoreType.DMA((2,))]

    def bind(self, ins, outs, scratch, place):
        bound = object.__new__(Gather)
        bound.__dict__.update(self.__dict__)
        bound.src, bound.out, bound.p = ins[0].at[self.number], outs[0], place
        bound.stage, bound.send, bound.recv, bound.own = scratch
        return bound

    def _copy(self, t, incoming=False):
        p, half = self.p, _half(self.rows)
        whole, top, low = pl.ds(0, self.rows), pl.ds(0, half), pl.ds(half, self.rows - half)
        step, core, rows, to = (
            (0, p.core, whole, 1), (0, p.core, whole, -1), (0, p.core, whole, 0),
            (-1, p.core, top, 1), (1, p.core, low, -1),
            (-1, p.core, whole, 0), (1, p.core, whole, 0), (2, p.core, whole, 0),
        )[t]
        if incoming:
            step, core = (step, p.other) if to == 0 else (step - to, core)
        at = self.out.at[p.slot(step, core), rows]
        src = self.src if t < 3 and not incoming else at
        return remote(src, at, self.send.at[t], self.recv.at[t], p.partner() if to == 0 else p.neighbour(to))

    def _into(self):
        return pltpu.make_async_copy(self.src, self.stage, self.own.at[0])

    def _out_of(self):
        return pltpu.make_async_copy(self.stage, self.out.at[self.p.slot(0, self.p.core)], self.own.at[1])

    def start(self):
        for t in (0, 1, 2):
            self._copy(t).start()
        self._into().start()

    def forward(self):
        self._copy(0, True).wait_recv()
        self._copy(3).start()
        self._copy(5).start()
        self._copy(1, True).wait_recv()
        self._copy(4).start()
        self._copy(6).start()
        self._into().wait()
        self._out_of().start()

    def last(self):
        self._copy(3, True).wait_recv()
        self._copy(4, True).wait_recv()
        self._copy(7).start()

    def finish(self):
        for t in (2, 5, 6, 7):
            self._copy(t, True).wait_recv()
        for t in range(8):
            self._copy(t).wait_send()
        self._out_of().wait()


def greet(place):
    for to in (place.neighbour(1), place.neighbour(-1), place.partner()):
        pl.semaphore_signal(pltpu.get_barrier_semaphore(), inc=1, device_id=to, device_id_type=pl.DeviceIdType.MESH)


def greeted():
    pl.semaphore_wait(pltpu.get_barrier_semaphore(), 3)


def ride(kernel, riders, plan, dp, *, grid, ins, outs, scratch, name, ident):
    counts = (len(ins), len(outs), len(scratch))
    steps = 1
    for n in grid:
        steps *= n

    def body(*refs):
        refs = list(refs)
        take = lambda n: [refs.pop(0) for _ in range(n)]
        own_in, ride_in = take(counts[0]), [take(len(r.inputs)) for r in riders]
        own_out, ride_out = take(counts[1]), [take(len(r.outs)) for r in riders]
        own_scr, ride_scr = take(counts[2]), [take(len(r.scratch)) for r in riders]
        step = 0
        for axis, n in enumerate(grid):
            step = step * n + pl.program_id(axis)
        place = Place(dp) if riders else None
        bound = [r.bind(a, b, c, place) for r, a, b, c in zip(riders, ride_in, ride_out, ride_scr)]
        if riders:
            pl.when(step == 0)(lambda: greet(place))
        kernel(*own_in, *own_out, *own_scr, *([bound] if riders else []))
        for when, what in plan:

            def act(when=when, what=what):
                if (when, what) == plan[0]:
                    greeted()
                for number, action in what:
                    getattr(bound[number], action)()

            pl.when(step == when)(act)

    flat = lambda name: [x for r in riders for x in getattr(r, name)]
    got = pl.pallas_call(
        body, grid=grid,
        in_specs=[s for _, s in ins] + [ANY] * len(flat("inputs")),
        out_specs=[s for _, s in outs] + [ANY] * len(flat("outs")),
        out_shape=[s for s, _ in outs] + flat("outs"),
        scratch_shapes=list(scratch) + flat("scratch"),
        compiler_params=params(len(grid), **(dict(collective_id=ident, has_side_effects=True) if riders else {})), name=name,
    )(*[a for a, _ in ins], *flat("inputs"))
    own, rest = got[: counts[1]], list(got[counts[1] :])
    return own, rest


def _open(freq_ref, cos_ref, sin_ref, riders):
    greeted()
    for r in riders:
        r.start()
    place = lax.broadcasted_iota(jnp.int32, cos_ref.shape, 0).astype(f32)
    angle = place * freq_ref[...]
    left = lax.broadcasted_iota(jnp.int32, sin_ref.shape, 1) < HEAD // 2
    cos_ref[...] = jnp.cos(angle)
    sin = jnp.sin(angle)
    sin_ref[...] = jnp.where(left, -sin, sin)
    for r in riders:
        r.forward()
    for r in riders:
        r.last()
    for r in riders:
        r.finish()


def opening(t, riders, dp, ident):
    half = HEAD // 2
    freq = np.float32(THETA) ** (-np.arange(half, dtype=np.float32) / half)
    freq = jnp.asarray(np.concatenate([freq, freq])[None], f32)
    table = sh((t, HEAD), f32), pl.BlockSpec((t, HEAD), lambda i: (0, 0))
    return ride(_open, riders, [], dp, grid=(1,), ins=[whole(freq)], outs=[table, table], scratch=[], name="opening", ident=ident)


def _qkv(h_ref, wq_ref, wk_ref, wv_ref, cos_ref, sin_ref, at_ref, q_ref, k_ref, v_ref, *_):
    wide = h_ref[...].astype(f32)
    a = (wide * rms(wide)).astype(bf16)
    at_ref[...] = a.T
    cos, sin = cos_ref[...], sin_ref[...]
    for w_ref, out_ref in ((wq_ref, q_ref), (wk_ref, k_ref)):
        t = dot(a, w_ref[...]).astype(bf16).astype(f32)
        for n in range(0, t.shape[1], HEAD):
            one = t[:, n : n + HEAD]
            out_ref[:, n : n + HEAD] = (one * cos + pltpu.roll(one, HEAD // 2, 1) * sin).astype(bf16)
    v_ref[...] = dot(a, wv_ref[...]).astype(bf16)


def qkv(h, wq, wk, wv, cos, sin, riders, plan, dp, ident, tm=512):
    t, d = h.shape
    rows = lambda n: pl.BlockSpec((tm, n), lambda i: (i, 0))
    return ride(
        _qkv, riders, plan, dp, grid=(t // tm,),
        ins=[(h, rows(d)), whole(wq), whole(wk), whole(wv), (cos, rows(HEAD)), (sin, rows(HEAD))],
        outs=[(sh((d, t), bf16), pl.BlockSpec((d, tm), lambda i: (0, i)))] + [(sh((t, w.shape[1]), bf16), rows(w.shape[1])) for w in (wq, wk, wv)],
        scratch=[], name="qkv", ident=ident)


def _below(bk, bq):
    return lax.broadcasted_iota(jnp.int32, (bk, bq), 1) >= lax.broadcasted_iota(jnp.int32, (bk, bq), 0)


def _attn(q_ref, k_ref, v_ref, o_ref, ot_ref, lse_ref, top_s, mix_s, *_):
    bq, nh, kv = q_ref.shape[0], q_ref.shape[1] // HEAD, k_ref.shape[1] // HEAD
    g = nh // kv
    iq = pl.program_id(0)
    e = HEAD**-0.5 * LOG2E
    top_s[...] = jnp.full(top_s.shape, NEG, f32)
    mix_s[...] = jnp.zeros(mix_s.shape, f32)
    ones = jnp.ones((8, bq), bf16)
    at = lambda n: slice(n * HEAD, (n + 1) * HEAD)

    def block(j, masked):
        here = pl.ds(pl.multiple_of(j * bq, bq), bq)
        scores = [dot(k_ref[here, at(n // g)], q_ref[:, at(n)], 1, 1) for n in range(nh)]
        values = [jnp.concatenate([v_ref[here, at(i)].T, ones], axis=0) for i in range(kv)]
        weights, keeps = [], []
        for n, s in enumerate(scores):
            if masked:
                s = jnp.where(_below(bq, bq), s, HIDDEN)
            old = top_s[n : n + 1, :]
            top = jnp.maximum(old, s.max(axis=0, keepdims=True))
            top_s[n : n + 1, :] = top
            weights.append(jnp.exp2((s - top) * e).astype(bf16))
            keeps.append(jnp.exp2((old - top) * e))
        for n, (p, keep) in enumerate(zip(weights, keeps)):
            mix_s[n] = mix_s[n] * keep + dot(values[n // g], p)

    lax.fori_loop(0, iq, lambda j, _: block(j, False), None)
    block(iq, True)
    for n in range(nh):
        total = mix_s[n, HEAD : HEAD + 1, :]
        out = (mix_s[n, :HEAD, :] * (1 / total)).astype(bf16)
        ot_ref[at(n), :] = out
        o_ref[:, at(n)] = out.T
        lse_ref[n : n + 1, :] = top_s[n : n + 1, :] * HEAD**-0.5 + jnp.log(total)


def attn(q, k, v, riders, plan, dp, ident, bq=512):
    t, nd = q.shape
    nh = nd // HEAD
    rows = pl.BlockSpec((bq, nd), lambda i: (i, 0))
    return ride(
        _attn, riders, plan, dp, grid=(t // bq,), ins=[(q, rows), whole(k), whole(v)],
        outs=[(sh((t, nd), bf16), rows), (sh((nd, t), bf16), pl.BlockSpec((nd, bq), lambda i: (0, i))),
              (sh((nh, t), f32), pl.BlockSpec((nh, bq), lambda i: (0, i)))],
        scratch=[pltpu.VMEM((nh, bq), f32), pltpu.VMEM((nh, HEAD + 8, bq), f32)], name="attn", ident=ident)


def _chunks(wg_hbm, wu_hbm, wgu_s, sems, cw):
    def chunk(n):
        at = pl.ds(pl.multiple_of(n * cw, 128), cw)
        return (pltpu.make_async_copy(wg_hbm.at[:, at], wgu_s.at[n, :, pl.ds(0, cw)], sems.at[n, 0]),
                pltpu.make_async_copy(wu_hbm.at[:, at], wgu_s.at[n, :, pl.ds(cw, cw)], sems.at[n, 1]))

    return chunk


def _mlp(cw, nt, h_ref, o_ref, wo_hbm, wg_hbm, wu_hbm, h1_ref, bt_ref, gu_ref, actt_ref, h2_ref,
         wo_s, wgu_s, wd_s, b_s, act_s, h1_s, sems, riders):
    s = pl.program_id(0)
    tm, nc = h_ref.shape[0], wg_hbm.shape[1] // cw
    i, c = s // nc, lax.rem(s, nc)
    chunk = _chunks(wg_hbm, wu_hbm, wgu_s, sems, cw)
    wo_copy = pltpu.make_async_copy(wo_hbm, wo_s, sems.at[nc, 0])
    wd_hbm = riders[0].out
    share = wd_hbm.shape[1]
    wd_copies = [pltpu.make_async_copy(wd_hbm.at[n], wd_s.at[pl.ds(n * share, share)], sems.at[nc + 1 + n // 2, n % 2])
                 for n in range(wd_hbm.shape[0])]

    @pl.when(s == 0)
    def _():
        wo_copy.start()
        for n in range(nc):
            for one in chunk(n):
                one.start()
        wo_copy.wait()

    @pl.when(s < nt * nc)
    def _():
        @pl.when(c == 0)
        def _():
            h1 = h_ref[...] + dot(o_ref[...], wo_s[...]).astype(bf16)
            h1_ref[...] = h1
            h1_s[i] = h1
            wide = h1.astype(f32)
            b = (wide * rms(wide)).astype(bf16)
            b_s[...] = b
            bt_ref[...] = b.T

        @pl.when(s < nc)
        def _():
            for one in chunk(c):
                one.wait()

        gu = dot(b_s[...], wgu_s[c])
        gu_ref[...] = gu
        g, u = gu[:, :cw], gu[:, cw:]
        act = (g * lax.logistic(g) * u).astype(bf16)
        act_s[i, :, pl.ds(pl.multiple_of(c * cw, 128), cw)] = act
        actt_ref[...] = act.T

    @pl.when(s == nt * nc)
    def _():
        riders[0].finish()
        for one in wd_copies:
            one.start()
        for one in wd_copies:
            one.wait()

    @pl.when(s >= nt * nc)
    def _():
        n = s - nt * nc
        h2_ref[...] = h1_s[n] + dot(act_s[n], wd_s[...]).astype(bf16)


def mlp(h, o, wo, wg, wu, riders, plan, dp, ident, tm=512, cw=640):
    t, d = h.shape
    ff = wg.shape[1]
    nc, nt = ff // cw, t // tm
    at = lambda s: jnp.minimum(s // nc, nt - 1)
    col = lambda s: jnp.where(s < nt * nc, lax.rem(s, nc), nc - 1)
    rows = lambda n: pl.BlockSpec((tm, n), lambda s: (at(s), 0))
    return ride(
        functools.partial(_mlp, cw, nt), riders, plan, dp, grid=(nt * nc + nt,),
        ins=[(h, rows(d)), (o, rows(o.shape[1])), (wo, ANY), (wg, ANY), (wu, ANY)],
        outs=[(sh((t, d), bf16), rows(d)), (sh((d, t), bf16), pl.BlockSpec((d, tm), lambda s: (0, at(s)))),
              (sh((t, 2 * ff), f32), pl.BlockSpec((tm, 2 * cw), lambda s: (at(s), col(s)))),
              (sh((ff, t), bf16), pl.BlockSpec((cw, tm), lambda s: (col(s), at(s)))),
              (sh((t, d), bf16), pl.BlockSpec((tm, d), lambda s: (jnp.maximum(s - nt * nc, 0), 0)))],
        scratch=[pltpu.VMEM(wo.shape, bf16), pltpu.VMEM((nc, d, 2 * cw), bf16), pltpu.VMEM((ff, d), bf16), pltpu.VMEM((tm, d), bf16),
                 pltpu.VMEM((nt, tm, ff), bf16), pltpu.VMEM((nt, tm, d), bf16), pltpu.SemaphoreType.DMA((nc + 1 + dp // 2, 2))],
        name="mlp", ident=ident)


def _mlpb(cw, dh_ref, gu_ref, h1_ref, o_ref, wo_hbm, wg_hbm, wu_hbm, wd_hbm, dgu_ref, dh1_ref, do_ref, delta_ref,
          wo_s, wgu_s, wd_s, dact_s, acc_s, sems, *_):
    i, c, nc = pl.program_id(0), pl.program_id(1), pl.num_programs(1)
    chunk = _chunks(wg_hbm, wu_hbm, wgu_s, sems, cw)
    cols = wg_hbm.shape[1] // cw
    wo_copy = pltpu.make_async_copy(wo_hbm, wo_s, sems.at[cols, 0])
    wd_copy = pltpu.make_async_copy(wd_hbm, wd_s, sems.at[cols, 1])

    @pl.when((i == 0) & (c == 0))
    def _():
        wd_copy.start()
        for n in range(cols):
            for one in chunk(n):
                one.start()
        wo_copy.start()
        wd_copy.wait()

    @pl.when(c == 0)
    def _():
        dact_s[...] = dot(dh_ref[...], wd_s[...], 1, 1).astype(bf16)

    @pl.when(i == 0)
    def _():
        for one in chunk(c):
            one.wait()

    dact = dact_s[:, pl.ds(pl.multiple_of(c * cw, 128), cw)].astype(f32)
    g, u = gu_ref[:, :cw], gu_ref[:, cw:]
    s = lax.logistic(g)
    gs = g * s
    dgu = jnp.concatenate([(dact * u * (s + gs * (1 - s))).astype(bf16), (dact * gs).astype(bf16)], axis=1)
    dgu_ref[...] = dgu
    term = dot(dgu, wgu_s[c], 1, 1)

    @pl.when(c == 0)
    def _():
        acc_s[...] = term

    @pl.when(c > 0)
    def _():
        acc_s[...] += term

    @pl.when((i == 0) & (c == nc - 1))
    def _():
        wo_copy.wait()

    @pl.when(c == nc - 1)
    def _():
        db = acc_s[...].astype(bf16).astype(f32)
        dh1 = dh_ref[...] + norm_back(h1_ref[...].astype(f32), db).astype(bf16)
        dh1_ref[...] = dh1
        do = dot(dh1, wo_s[...], 1, 1).astype(bf16)
        do_ref[...] = do
        each = do.astype(f32) * o_ref[...].astype(f32)
        heads = [each[:, n : n + HEAD].sum(-1, keepdims=True) for n in range(0, each.shape[1], HEAD)]
        delta_ref[...] = jnp.concatenate(heads, 1).T


def mlpb(dh, gu, h1, o, wo, wg, wu, wd, riders, plan, dp, ident, tm=512, cw=640):
    t, d = dh.shape
    ff = wg.shape[1]
    nc, nh = ff // cw, o.shape[1] // HEAD
    rows = lambda n: pl.BlockSpec((tm, n), lambda i, c: (i, 0))
    tile = pl.BlockSpec((tm, 2 * cw), lambda i, c: (i, c))
    return ride(
        functools.partial(_mlpb, cw), riders, plan, dp, grid=(t // tm, nc),
        ins=[(dh, rows(d)), (gu, tile), (h1, rows(d)), (o, rows(o.shape[1])), (wo, ANY), (wg, ANY), (wu, ANY), (wd, ANY)],
        outs=[(sh((t, 2 * ff), bf16), tile), (sh((t, d), bf16), rows(d)), (sh(o.shape, bf16), rows(o.shape[1])),
              (sh((nh, t), f32), pl.BlockSpec((nh, tm), lambda i, c: (0, i)))],
        scratch=[pltpu.VMEM(wo.shape, bf16), pltpu.VMEM((nc, d, 2 * cw), bf16), pltpu.VMEM(wd.shape, bf16),
                 pltpu.VMEM((tm, ff), bf16), pltpu.VMEM((tm, d), f32), pltpu.SemaphoreType.DMA((nc + 1, 2))],
        name="mlpb", ident=ident)


def turn_back(t, cos, sin):
    t = t.astype(f32)
    return (t * cos - pltpu.roll(t, HEAD // 2, 1) * sin).astype(bf16)


def _attnb(q_ref, k_ref, v_ref, do_ref, lse_ref, delta_ref, cos_ref, sin_ref, dq_ref, dkv_ref, dq_s, dk_s, dv_s, *_):
    bq, nh, kv = q_ref.shape[0], q_ref.shape[1] // HEAD, k_ref.shape[1] // HEAD
    g = nh // kv
    iq = pl.program_id(0)
    scale = HEAD**-0.5
    e = scale * LOG2E
    at = lambda n: slice(n * HEAD, (n + 1) * HEAD)

    @pl.when(iq == 0)
    def _():
        dk_s[...] = jnp.zeros_like(dk_s)
        dv_s[...] = jnp.zeros_like(dv_s)

    dq_s[...] = jnp.zeros_like(dq_s)

    def block(j, masked):
        here = pl.ds(pl.multiple_of(j * bq, bq), bq)
        ks = [k_ref[here, at(i)] for i in range(kv)]
        vs = [v_ref[here, at(i)] for i in range(kv)]
        for n in range(nh):
            i = n // g
            q, do = q_ref[:, at(n)], do_ref[:, at(n)]
            s = dot(ks[i], q, 1, 1)
            dp = dot(vs[i], do, 1, 1)
            p = jnp.exp2(s * e - lse_ref[n : n + 1, :] * LOG2E)
            if masked:
                p = jnp.where(_below(bq, bq), p, 0.0)
            ds = (p * (dp - delta_ref[n : n + 1, :])).astype(bf16)
            dv_s[i, here, :] += dot(p.astype(bf16), do)
            dk_s[i, here, :] += dot(ds, q)
            dq_s[n] += dot(ks[i].T, ds)

    lax.fori_loop(0, iq, lambda j, _: block(j, False), None)
    block(iq, True)
    mine = pl.ds(pl.multiple_of(iq * bq, bq), bq)
    cos, sin = cos_ref[mine, :], sin_ref[mine, :]
    for n in range(nh):
        dq_ref[:, at(n)] = turn_back((dq_s[n] * scale).astype(bf16).T, cos, sin)

    @pl.when(iq == pl.num_programs(0) - 1)
    def _():
        for i in range(kv):
            dkv_ref[:, at(i)] = turn_back((dk_s[i] * scale).astype(bf16), cos_ref[...], sin_ref[...])
            dkv_ref[:, at(kv + i)] = dv_s[i].astype(bf16)


def attnb(q, k, v, do, lse, delta, cos, sin, riders, plan, dp, ident, bq=512):
    t, nd = q.shape
    nh, kv = nd // HEAD, k.shape[1] // HEAD
    rows = pl.BlockSpec((bq, nd), lambda i: (i, 0))
    stats = pl.BlockSpec((nh, bq), lambda i: (0, i))
    return ride(
        _attnb, riders, plan, dp, grid=(t // bq,),
        ins=[(q, rows), whole(k), whole(v), (do, rows), (lse, stats), (delta, stats), whole(cos), whole(sin)],
        outs=[(sh((t, nd), bf16), rows), (sh((t, 2 * kv * HEAD), bf16), pl.BlockSpec((t, 2 * kv * HEAD), lambda i: (0, 0)))],
        scratch=[pltpu.VMEM((nh, HEAD, bq), f32), pltpu.VMEM((kv, t, HEAD), f32), pltpu.VMEM((kv, t, HEAD), f32)],
        name="attnb", ident=ident)


def _da(dq_ref, dkv_ref, h_ref, dh1_ref, wq_ref, wk_ref, wv_ref, dh_ref, *_):
    nk = wk_ref.shape[1]
    da = dot(dq_ref[...], wq_ref[...], 1, 1) + dot(dkv_ref[:, :nk], wk_ref[...], 1, 1) + dot(dkv_ref[:, nk:], wv_ref[...], 1, 1)
    dh_ref[...] = dh1_ref[...] + norm_back(h_ref[...].astype(f32), da.astype(bf16).astype(f32)).astype(bf16)


def states(dq, dkv, h, dh1, wq, wk, wv, riders, plan, dp, ident, tm=512):
    t, d = h.shape
    rows = lambda n: pl.BlockSpec((tm, n), lambda i: (i, 0))
    return ride(
        _da, riders, plan, dp, grid=(t // tm,),
        ins=[(dq, rows(dq.shape[1])), (dkv, rows(dkv.shape[1])), (h, rows(d)), (dh1, rows(d)), whole(wq), whole(wk), whole(wv)],
        outs=[(sh((t, d), bf16), rows(d))], scratch=[], name="states", ident=ident)


def _wgrad(lhs_ref, *rest):
    rhs, out_ref = rest[:-1], rest[-1]
    kk = pl.program_id(0)
    m = lhs_ref.shape[0] * lhs_ref.shape[2]
    b = rhs[0][...] if len(rhs) == 1 else jnp.concatenate([r[...] for r in rhs], 1)
    out_ref[:, 0] = dot(lhs_ref[:, kk].reshape(m, lhs_ref.shape[3]), b).astype(bf16).reshape(lhs_ref.shape[0], lhs_ref.shape[2], -1)


def wgrad(lhs, rhs, nt, dp):
    m, t = lhs.shape
    l4 = lhs.reshape(dp // 2, 2, m // dp, t)
    n = sum(r.shape[1] for r in rhs)
    w = n // nt
    return pl.pallas_call(
        _wgrad, grid=(2, nt),
        in_specs=[once(l4.shape, lambda k, j: (0, 0, 0, 0))] + [pl.BlockSpec((t, r.shape[1] // nt), lambda k, j: (0, j)) for r in rhs],
        out_specs=pl.BlockSpec((dp // 2, 1, m // dp, w), lambda k, j: (0, k, 0, j)),
        out_shape=sh((dp // 2, 2, m // dp, n), bf16), compiler_params=params(2), name="wgrad",
    )(l4, *rhs).reshape(m, n)


def adamw(w, m, v, g):
    m = 0.9 * m + 0.1 * g
    v = 0.95 * v + 0.05 * g * g
    step = m * lax.rsqrt(v + 1e-8) + 0.1 * w
    return (w - 0.02 * step).astype(jnp.bfloat16), m, v


def solution(mesh):
    dp = mesh.shape["dp"]

    def step(x, dy, *arrays):
        weights, m, v = (arrays[i : i + 7] for i in (0, 7, 14))
        wq, wk, wv, wo, wg, wu, wd = weights
        layers = wq.shape[0]
        h, t = x[0], x.shape[1]
        full = lambda w: w.reshape(-1, w.shape[2])
        gather = lambda number, *ws: [Gather(w, number, dp) for w in ws]
        stages = lambda n: [[(r, act) for r in range(n)] for act in ("start", "forward", "last", "finish")]
        idents = iter(range(1000))

        (cos, sin), got = opening(t, gather(0, wq, wk, wv), dp, next(idents))
        kept, fetched = [], []
        for number in range(layers):
            w_q, w_k, w_v = (full(w) for w in got[:3])
            if number == 0:
                a, b, c, e = stages(1)
                (at, q, k, vv), got = qkv(h, w_q, w_k, w_v, cos, sin, gather(number, wo), [(0, a), (2, b), (3, c + e)], dp, next(idents))
                w_o = full(got[0])
            else:
                (at, q, k, vv), _ = qkv(h, w_q, w_k, w_v, cos, sin, [], [], dp, 0)
                w_o = full(got[3])
            a, b, c, e = stages(2)
            (o, ot, lse), got = attn(q, k, vv, gather(number, wg, wu), [(0, a), (2, b[:1]), (3, b[1:] + c + e)], dp, next(idents))
            w_g, w_u = full(got[0]), full(got[1])
            if number + 1 < layers:
                a, b, c, e = stages(5)
                riders = gather(number, wd) + gather(number + 1, wq, wk, wv, wo)
                plan = [(0, a[:1]), (7, b[:1] + a[1:]), (11, c[:1] + b[1:]), (18, c[1:]), (23, e[1:])]
            else:
                a, b, c, e = stages(1)
                riders = gather(number, wd)
                plan = [(0, a), (7, b), (11, c)]
            (h1, bt, gu, actt, h2), got = mlp(h, o, w_o, w_g, w_u, riders, plan, dp, next(idents))
            w_d = full(got[0])
            got = got[1:]
            kept.append((h, at, q, k, vv, o, ot, lse, h1, bt, gu, actt))
            fetched.append((w_q, w_k, w_v, w_o, w_g, w_u, w_d))
            h = h2
        dh, grads = dy[0], [None] * layers
        scatter = lambda g: lax.psum_scatter(g, "dp", scatter_dimension=0, tiled=True)
        for number in reversed(range(layers)):
            h, at, q, k, vv, o, ot, lse, h1, bt, gu, actt = kept[number]
            w_q, w_k, w_v, w_o, w_g, w_u, w_d = fetched[number]
            g_d = scatter(wgrad(actt, [dh], 4, dp))
            (dgu, dh1, do, delta), _ = mlpb(dh, gu, h1, o, w_o, w_g, w_u, w_d, [], [], dp, 0)
            g_gu = scatter(wgrad(bt, [dgu], 5, dp))
            g_o = scatter(wgrad(ot, [dh1], 1, dp))
            (dq, dkv), _ = attnb(q, k, vv, do, lse, delta, cos, sin, [], [], dp, 0)
            g_qkv = scatter(wgrad(at, [dq, dkv], 1, dp))
            if number:
                (dh,), _ = states(dq, dkv, h, dh1, w_q, w_k, w_v, [], [], dp, 0)
            pair = g_gu.reshape(g_gu.shape[0], -1, 2, 640)
            nq, nk = q.shape[1], k.shape[1]
            grads[number] = (g_qkv[:, :nq], g_qkv[:, nq : nq + nk], g_qkv[:, nq + nk :], g_o,
                             pair[:, :, 0].reshape(g_gu.shape[0], -1), pair[:, :, 1].reshape(g_gu.shape[0], -1), g_d)
        gradients = [jnp.stack([grads[number][i] for number in range(layers)]).astype(f32) for i in range(7)]
        new = [adamw(w.astype(f32), m, v, g) for w, m, v, g in zip(weights, m, v, gradients, strict=True)]
        return tuple(one[which] for which in range(3) for one in new)

    rows, cut = P(("rep", "dp"), None, None), P(None, "dp", None)
    return jax.shard_map(
        step,
        mesh=mesh,
        in_specs=(rows, rows) + (cut,) * 21,
        out_specs=(P("rep", "dp", None),) * 21,
        check_vma=False,
    )
```

```python
import functools

import jax
import jax.numpy as jnp
import numpy as np
from jax import lax
from jax.experimental import pallas as pl
from jax.experimental.pallas import tpu as pltpu
from jax.sharding import PartitionSpec as P

f32, bf16 = jnp.float32, jnp.bfloat16
sh = jax.ShapeDtypeStruct
HEAD = 128
THETA = 10000
NEG = -1e30
HIDDEN = 2 * NEG
LOG2E = 1.4426950408889634
ANY = pl.BlockSpec(memory_space=pl.ANY)
BIG = 63 * 2**20


def dot(a, b, ca=1, cb=0):
    return lax.dot_general(a, b, (((ca,), (cb,)), ((), ())), preferred_element_type=f32)


def once(shape, index):
    return pl.BlockSpec(shape, index, pipeline_mode=pl.Buffered(1))


def whole(a):
    return a, once(a.shape, lambda *_: (0,) * a.ndim)


def rms(wide):
    return lax.rsqrt(jnp.mean(wide * wide, -1, keepdims=True) + 1e-6)


def norm_back(wide, db):
    r = rms(wide)
    return r * db - wide * (r * r * r * (jnp.sum(db * wide, -1, keepdims=True) * (1 / wide.shape[1])))


def params(n, **kw):
    return pltpu.CompilerParams(dimension_semantics=("arbitrary",) * n, vmem_limit_bytes=BIG, **kw)


class Place:
    def __init__(self, dp):
        me = lax.axis_index("dp")
        self.chips = dp // 2
        self.chip, self.core = me // 2, lax.rem(me, 2)
        self.other = 1 - self.core

    def at(self, step):
        return lax.rem(self.chip + step + self.chips, self.chips)

    def slot(self, step, core):
        return 2 * self.at(step) + core

    def partner(self):
        return {"dp": self.slot(0, self.other)}

    def neighbour(self, step):
        return {"dp": self.slot(step, self.core)}


def remote(src, dst, send, recv, device):
    return pltpu.make_async_remote_copy(src_ref=src, dst_ref=dst, send_sem=send, recv_sem=recv, device_id=device,
                                        device_id_type=pl.DeviceIdType.MESH)


def _half(rows):
    return -(-rows // 32) * 16


class Rider:
    greets = ()

    def bind(self, ins, outs, scratch, place):
        bound = object.__new__(type(self))
        bound.__dict__.update(self.__dict__)
        bound.p = place
        bound.refs(ins, outs, scratch)
        return bound


class Gather(Rider):
    greets = (1, -1, 0)

    def __init__(self, w, number, dp):
        self.number = number
        self.rows, self.n = w.shape[1:]
        self.inputs = [w]
        self.outs = [sh((dp, self.rows, self.n), w.dtype)]
        self.scratch = [pltpu.VMEM((self.rows, self.n), w.dtype), pltpu.SemaphoreType.DMA((8,)), pltpu.SemaphoreType.DMA((8,)),
                        pltpu.SemaphoreType.DMA((2,))]

    def refs(self, ins, outs, scratch):
        self.src, self.out = ins[0].at[self.number], outs[0]
        self.stage, self.send, self.recv, self.own = scratch

    def _copy(self, t, incoming=False):
        p, half = self.p, _half(self.rows)
        whole, top, low = pl.ds(0, self.rows), pl.ds(0, half), pl.ds(half, self.rows - half)
        step, core, rows, to = (
            (0, p.core, whole, 1), (0, p.core, whole, -1), (0, p.core, whole, 0),
            (-1, p.core, top, 1), (1, p.core, low, -1),
            (-1, p.core, whole, 0), (1, p.core, whole, 0), (2, p.core, whole, 0),
        )[t]
        if incoming:
            step, core = (step, p.other) if to == 0 else (step - to, core)
        at = self.out.at[p.slot(step, core), rows]
        src = self.src if t < 3 and not incoming else at
        return remote(src, at, self.send.at[t], self.recv.at[t], p.partner() if to == 0 else p.neighbour(to))

    def _into(self):
        return pltpu.make_async_copy(self.src, self.stage, self.own.at[0])

    def _out_of(self):
        return pltpu.make_async_copy(self.stage, self.out.at[self.p.slot(0, self.p.core)], self.own.at[1])

    def start(self):
        for t in (0, 1, 2):
            self._copy(t).start()
        self._into().start()

    def forward(self):
        self._copy(0, True).wait_recv()
        self._copy(3).start()
        self._copy(5).start()
        self._copy(1, True).wait_recv()
        self._copy(4).start()
        self._copy(6).start()
        self._into().wait()
        self._out_of().start()

    def last(self):
        self._copy(3, True).wait_recv()
        self._copy(4, True).wait_recv()
        self._copy(7).start()

    def finish(self):
        for t in (2, 5, 6, 7):
            self._copy(t, True).wait_recv()
        for t in range(8):
            self._copy(t).wait_send()
        self._out_of().wait()


class Reduce(Rider):
    greets = (1, -1)

    def __init__(self, blocks):
        self.rows, self.n = blocks.shape[1:]
        half = _half(self.rows)
        self.inputs = [blocks]
        self.outs = [sh((self.rows, self.n), blocks.dtype)] * 2
        parts = [pltpu.VMEM((half, self.n), blocks.dtype), pltpu.VMEM((self.rows - half, self.n), blocks.dtype)]
        self.scratch = parts + parts + [pltpu.SemaphoreType.DMA((6,)), pltpu.SemaphoreType.DMA((6,)), pltpu.SemaphoreType.DMA((2,))]

    def refs(self, ins, outs, scratch):
        self.blocks, (self.before, self.after) = ins[0], outs
        self.top, self.low, self.own_top, self.own_low, self.send, self.recv, self.local = scratch

    def _copy(self, t):
        p, half = self.p, _half(self.rows)
        top, low = pl.ds(0, half), pl.ds(half, self.rows - half)
        block = lambda step, rows: self.blocks.at[p.at(step), rows]
        src, dst, to = (
            (block(2, top), self.top, 1), (block(2, low), self.low, -1),
            (self.own_top, self.before.at[top], 1), (block(1, low), self.before.at[low], 1),
            (block(-1, top), self.after.at[top], -1), (self.own_low, self.after.at[low], -1),
        )[t]
        return remote(src, dst, self.send.at[t], self.recv.at[t], p.neighbour(to))

    def _own(self):
        p, half = self.p, _half(self.rows)
        return (pltpu.make_async_copy(self.blocks.at[p.at(1), pl.ds(0, half)], self.own_top, self.local.at[0]),
                pltpu.make_async_copy(self.blocks.at[p.at(-1), pl.ds(half, self.rows - half)], self.own_low, self.local.at[1]))

    def start(self):
        for t in (0, 1, 3, 4):
            self._copy(t).start()
        for one in self._own():
            one.start()

    def add(self):
        for one in self._own():
            one.wait()
        self._copy(0).wait_recv()
        self.own_top[...] = (self.own_top[...].astype(f32) + self.top[...].astype(f32)).astype(bf16)
        self._copy(1).wait_recv()
        self.own_low[...] = (self.own_low[...].astype(f32) + self.low[...].astype(f32)).astype(bf16)

    def pass_on(self):
        for t in (2, 5):
            self._copy(t).start()

    def finish(self):
        for t in (2, 3, 4, 5):
            self._copy(t).wait_recv()
        for t in range(6):
            self._copy(t).wait_send()


def greet(place, whom):
    for to in whom:
        pl.semaphore_signal(pltpu.get_barrier_semaphore(), inc=1, device_id=place.neighbour(to) if to else place.partner(),
                            device_id_type=pl.DeviceIdType.MESH)


def greeted(whom):
    pl.semaphore_wait(pltpu.get_barrier_semaphore(), len(whom))


def ride(kernel, riders, plan, dp, *, grid, ins, outs, scratch, name, ident, greets=(), meet=None):
    counts = (len(ins), len(outs), len(scratch))
    steps = 1
    for n in grid:
        steps *= n
    whom = tuple(to for to in (1, -1, 0) if to in greets or any(to in r.greets for r in riders))
    plan = ([(meet, [])] if meet is not None else []) + list(plan)

    def body(*refs):
        refs = list(refs)
        take = lambda n: [refs.pop(0) for _ in range(n)]
        own_in, ride_in = take(counts[0]), [take(len(r.inputs)) for r in riders]
        own_out, ride_out = take(counts[1]), [take(len(r.outs)) for r in riders]
        own_scr, ride_scr = take(counts[2]), [take(len(r.scratch)) for r in riders]
        step = 0
        for axis, n in enumerate(grid):
            step = step * n + pl.program_id(axis)
        place = Place(dp) if whom else None
        bound = [r.bind(a, b, c, place) for r, a, b, c in zip(riders, ride_in, ride_out, ride_scr)]

        def act(half):
            for k, (when, what) in enumerate(plan):
                if int(2 * when) % 2 == half:

                    def do(k=k, what=what):
                        if k == 0:
                            greeted(whom)
                        for number, action in what:
                            getattr(bound[number], action)()

                    pl.when(step == int(when))(do)

        if whom:
            pl.when(step == 0)(lambda: greet(place, whom))
        act(0)
        kernel(*own_in, *own_out, *own_scr, place, bound)
        act(1)

    flat = lambda name: [x for r in riders for x in getattr(r, name)]
    got = pl.pallas_call(
        body, grid=grid,
        in_specs=[s for _, s in ins] + [ANY] * len(flat("inputs")),
        out_specs=[s for _, s in outs] + [ANY] * len(flat("outs")),
        out_shape=[s for s, _ in outs] + flat("outs"),
        scratch_shapes=list(scratch) + flat("scratch"),
        compiler_params=params(len(grid), **(dict(collective_id=ident, has_side_effects=True) if whom else {})), name=name,
    )(*[a for a, _ in ins], *flat("inputs"))
    own, rest = got[: counts[1]], list(got[counts[1] :])
    return own, rest


def _open(freq_ref, cos_ref, sin_ref, _, riders):
    greeted(Gather.greets)
    for r in riders:
        r.start()
    place = lax.broadcasted_iota(jnp.int32, cos_ref.shape, 0).astype(f32)
    angle = place * freq_ref[...]
    left = lax.broadcasted_iota(jnp.int32, sin_ref.shape, 1) < HEAD // 2
    cos_ref[...] = jnp.cos(angle)
    sin = jnp.sin(angle)
    sin_ref[...] = jnp.where(left, -sin, sin)
    for r in riders:
        r.forward()
    for r in riders:
        r.last()
    for r in riders:
        r.finish()


def opening(t, riders, dp, ident):
    half = HEAD // 2
    freq = np.float32(THETA) ** (-np.arange(half, dtype=np.float32) / half)
    freq = jnp.asarray(np.concatenate([freq, freq])[None], f32)
    table = sh((t, HEAD), f32), pl.BlockSpec((t, HEAD), lambda i: (0, 0))
    return ride(_open, riders, [], dp, grid=(1,), ins=[whole(freq)], outs=[table, table], scratch=[], name="opening", ident=ident)


def _qkv(h_ref, wq_ref, wk_ref, wv_ref, cos_ref, sin_ref, at_ref, q_ref, k_ref, v_ref, *_):
    wide = h_ref[...].astype(f32)
    a = (wide * rms(wide)).astype(bf16)
    at_ref[...] = a.T
    cos, sin = cos_ref[...], sin_ref[...]
    for w_ref, out_ref in ((wq_ref, q_ref), (wk_ref, k_ref)):
        t = dot(a, w_ref[...]).astype(bf16).astype(f32)
        for n in range(0, t.shape[1], HEAD):
            one = t[:, n : n + HEAD]
            out_ref[:, n : n + HEAD] = (one * cos + pltpu.roll(one, HEAD // 2, 1) * sin).astype(bf16)
    v_ref[...] = dot(a, wv_ref[...]).astype(bf16)


def qkv(h, wq, wk, wv, cos, sin, riders, plan, dp, ident, tm=512):
    t, d = h.shape
    rows = lambda n: pl.BlockSpec((tm, n), lambda i: (i, 0))
    return ride(
        _qkv, riders, plan, dp, grid=(t // tm,),
        ins=[(h, rows(d)), whole(wq), whole(wk), whole(wv), (cos, rows(HEAD)), (sin, rows(HEAD))],
        outs=[(sh((d, t), bf16), pl.BlockSpec((d, tm), lambda i: (0, i)))] + [(sh((t, w.shape[1]), bf16), rows(w.shape[1])) for w in (wq, wk, wv)],
        scratch=[], name="qkv", ident=ident)


def _below(bk, bq):
    return lax.broadcasted_iota(jnp.int32, (bk, bq), 1) >= lax.broadcasted_iota(jnp.int32, (bk, bq), 0)


def _attn(q_ref, k_ref, v_ref, o_ref, ot_ref, lse_ref, top_s, mix_s, *_):
    bq, nh, kv = q_ref.shape[0], q_ref.shape[1] // HEAD, k_ref.shape[1] // HEAD
    g = nh // kv
    iq = pl.program_id(0)
    e = HEAD**-0.5 * LOG2E
    top_s[...] = jnp.full(top_s.shape, NEG, f32)
    mix_s[...] = jnp.zeros(mix_s.shape, f32)
    ones = jnp.ones((8, bq), bf16)
    at = lambda n: slice(n * HEAD, (n + 1) * HEAD)

    def block(j, masked):
        here = pl.ds(pl.multiple_of(j * bq, bq), bq)
        scores = [dot(k_ref[here, at(n // g)], q_ref[:, at(n)], 1, 1) for n in range(nh)]
        values = [jnp.concatenate([v_ref[here, at(i)].T, ones], axis=0) for i in range(kv)]
        weights, keeps = [], []
        for n, s in enumerate(scores):
            if masked:
                s = jnp.where(_below(bq, bq), s, HIDDEN)
            old = top_s[n : n + 1, :]
            top = jnp.maximum(old, s.max(axis=0, keepdims=True))
            top_s[n : n + 1, :] = top
            weights.append(jnp.exp2((s - top) * e).astype(bf16))
            keeps.append(jnp.exp2((old - top) * e))
        for n, (p, keep) in enumerate(zip(weights, keeps)):
            mix_s[n] = mix_s[n] * keep + dot(values[n // g], p)

    lax.fori_loop(0, iq, lambda j, _: block(j, False), None)
    block(iq, True)
    for n in range(nh):
        total = mix_s[n, HEAD : HEAD + 1, :]
        out = (mix_s[n, :HEAD, :] * (1 / total)).astype(bf16)
        ot_ref[at(n), :] = out
        o_ref[:, at(n)] = out.T
        lse_ref[n : n + 1, :] = top_s[n : n + 1, :] * HEAD**-0.5 + jnp.log(total)


def attn(q, k, v, riders, plan, dp, ident, bq=512):
    t, nd = q.shape
    nh = nd // HEAD
    rows = pl.BlockSpec((bq, nd), lambda i: (i, 0))
    return ride(
        _attn, riders, plan, dp, grid=(t // bq,), ins=[(q, rows), whole(k), whole(v)],
        outs=[(sh((t, nd), bf16), rows), (sh((nd, t), bf16), pl.BlockSpec((nd, bq), lambda i: (0, i))),
              (sh((nh, t), f32), pl.BlockSpec((nh, bq), lambda i: (0, i)))],
        scratch=[pltpu.VMEM((nh, bq), f32), pltpu.VMEM((nh, HEAD + 8, bq), f32)], name="attn", ident=ident)


def _chunks(wg_hbm, wu_hbm, wgu_s, sems, cw):
    def chunk(n):
        at = pl.ds(pl.multiple_of(n * cw, 128), cw)
        return (pltpu.make_async_copy(wg_hbm.at[:, at], wgu_s.at[n, :, pl.ds(0, cw)], sems.at[n, 0]),
                pltpu.make_async_copy(wu_hbm.at[:, at], wgu_s.at[n, :, pl.ds(cw, cw)], sems.at[n, 1]))

    return chunk


def _mlp(cw, nt, h_ref, o_ref, wo_hbm, wg_hbm, wu_hbm, h1_ref, bt_ref, gu_ref, actt_ref, h2_ref,
         wo_s, wgu_s, wd_s, b_s, act_s, h1_s, sems, _, riders):
    s = pl.program_id(0)
    tm, nc = h_ref.shape[0], wg_hbm.shape[1] // cw
    i, c = s // nc, lax.rem(s, nc)
    chunk = _chunks(wg_hbm, wu_hbm, wgu_s, sems, cw)
    wo_copy = pltpu.make_async_copy(wo_hbm, wo_s, sems.at[nc, 0])
    wd_hbm = riders[0].out
    share = wd_hbm.shape[1]
    wd_copies = [pltpu.make_async_copy(wd_hbm.at[n], wd_s.at[pl.ds(n * share, share)], sems.at[nc + 1 + n // 2, n % 2])
                 for n in range(wd_hbm.shape[0])]

    @pl.when(s == 0)
    def _():
        wo_copy.start()
        for n in range(nc):
            for one in chunk(n):
                one.start()
        wo_copy.wait()

    @pl.when(s < nt * nc)
    def _():
        @pl.when(c == 0)
        def _():
            h1 = h_ref[...] + dot(o_ref[...], wo_s[...]).astype(bf16)
            h1_ref[...] = h1
            h1_s[i] = h1
            wide = h1.astype(f32)
            b = (wide * rms(wide)).astype(bf16)
            b_s[...] = b
            bt_ref[...] = b.T

        @pl.when(s < nc)
        def _():
            for one in chunk(c):
                one.wait()

        gu = dot(b_s[...], wgu_s[c])
        gu_ref[...] = gu
        g, u = gu[:, :cw], gu[:, cw:]
        act = (g * lax.logistic(g) * u).astype(bf16)
        act_s[i, :, pl.ds(pl.multiple_of(c * cw, 128), cw)] = act
        actt_ref[...] = act.T

    @pl.when(s == nt * nc)
    def _():
        riders[0].finish()
        for one in wd_copies:
            one.start()
        for one in wd_copies:
            one.wait()

    @pl.when(s >= nt * nc)
    def _():
        n = s - nt * nc
        h2_ref[...] = h1_s[n] + dot(act_s[n], wd_s[...]).astype(bf16)


def mlp(h, o, wo, wg, wu, riders, plan, dp, ident, tm=512, cw=640):
    t, d = h.shape
    ff = wg.shape[1]
    nc, nt = ff // cw, t // tm
    at = lambda s: jnp.minimum(s // nc, nt - 1)
    col = lambda s: jnp.where(s < nt * nc, lax.rem(s, nc), nc - 1)
    rows = lambda n: pl.BlockSpec((tm, n), lambda s: (at(s), 0))
    return ride(
        functools.partial(_mlp, cw, nt), riders, plan, dp, grid=(nt * nc + nt,),
        ins=[(h, rows(d)), (o, rows(o.shape[1])), (wo, ANY), (wg, ANY), (wu, ANY)],
        outs=[(sh((t, d), bf16), rows(d)), (sh((d, t), bf16), pl.BlockSpec((d, tm), lambda s: (0, at(s)))),
              (sh((t, 2 * ff), f32), pl.BlockSpec((tm, 2 * cw), lambda s: (at(s), col(s)))),
              (sh((ff, t), bf16), pl.BlockSpec((cw, tm), lambda s: (col(s), at(s)))),
              (sh((t, d), bf16), pl.BlockSpec((tm, d), lambda s: (jnp.maximum(s - nt * nc, 0), 0)))],
        scratch=[pltpu.VMEM(wo.shape, bf16), pltpu.VMEM((nc, d, 2 * cw), bf16), pltpu.VMEM((ff, d), bf16), pltpu.VMEM((tm, d), bf16),
                 pltpu.VMEM((nt, tm, ff), bf16), pltpu.VMEM((nt, tm, d), bf16), pltpu.SemaphoreType.DMA((nc + 1 + dp // 2, 2))],
        name="mlp", ident=ident)


def _mlpb(cw, dh_ref, gu_ref, h1_ref, o_ref, wo_hbm, wg_hbm, wu_hbm, wd_hbm, dgu_ref, dh1_ref, do_ref, delta_ref,
          wo_s, wgu_s, wd_s, dact_s, acc_s, sems, *_):
    i, c, nc = pl.program_id(0), pl.program_id(1), pl.num_programs(1)
    chunk = _chunks(wg_hbm, wu_hbm, wgu_s, sems, cw)
    cols = wg_hbm.shape[1] // cw
    wo_copy = pltpu.make_async_copy(wo_hbm, wo_s, sems.at[cols, 0])
    wd_copy = pltpu.make_async_copy(wd_hbm, wd_s, sems.at[cols, 1])

    @pl.when((i == 0) & (c == 0))
    def _():
        wd_copy.start()
        for n in range(cols):
            for one in chunk(n):
                one.start()
        wo_copy.start()
        wd_copy.wait()

    @pl.when(c == 0)
    def _():
        dact_s[...] = dot(dh_ref[...], wd_s[...], 1, 1).astype(bf16)

    @pl.when(i == 0)
    def _():
        for one in chunk(c):
            one.wait()

    dact = dact_s[:, pl.ds(pl.multiple_of(c * cw, 128), cw)].astype(f32)
    g, u = gu_ref[:, :cw], gu_ref[:, cw:]
    s = lax.logistic(g)
    gs = g * s
    dgu = jnp.concatenate([(dact * u * (s + gs * (1 - s))).astype(bf16), (dact * gs).astype(bf16)], axis=1)
    dgu_ref[...] = dgu
    term = dot(dgu, wgu_s[c], 1, 1)

    @pl.when(c == 0)
    def _():
        acc_s[...] = term

    @pl.when(c > 0)
    def _():
        acc_s[...] += term

    @pl.when((i == 0) & (c == nc - 1))
    def _():
        wo_copy.wait()

    @pl.when(c == nc - 1)
    def _():
        db = acc_s[...].astype(bf16).astype(f32)
        dh1 = dh_ref[...] + norm_back(h1_ref[...].astype(f32), db).astype(bf16)
        dh1_ref[...] = dh1
        do = dot(dh1, wo_s[...], 1, 1).astype(bf16)
        do_ref[...] = do
        each = do.astype(f32) * o_ref[...].astype(f32)
        heads = [each[:, n : n + HEAD].sum(-1, keepdims=True) for n in range(0, each.shape[1], HEAD)]
        delta_ref[...] = jnp.concatenate(heads, 1).T


def mlpb(dh, gu, h1, o, wo, wg, wu, wd, riders, plan, dp, ident, tm=512, cw=640):
    t, d = dh.shape
    ff = wg.shape[1]
    nc, nh = ff // cw, o.shape[1] // HEAD
    rows = lambda n: pl.BlockSpec((tm, n), lambda i, c: (i, 0))
    tile = pl.BlockSpec((tm, 2 * cw), lambda i, c: (i, c))
    return ride(
        functools.partial(_mlpb, cw), riders, plan, dp, grid=(t // tm, nc),
        ins=[(dh, rows(d)), (gu, tile), (h1, rows(d)), (o, rows(o.shape[1])), (wo, ANY), (wg, ANY), (wu, ANY), (wd, ANY)],
        outs=[(sh((t, 2 * ff), bf16), tile), (sh((t, d), bf16), rows(d)), (sh(o.shape, bf16), rows(o.shape[1])),
              (sh((nh, t), f32), pl.BlockSpec((nh, tm), lambda i, c: (0, i)))],
        scratch=[pltpu.VMEM(wo.shape, bf16), pltpu.VMEM((nc, d, 2 * cw), bf16), pltpu.VMEM(wd.shape, bf16),
                 pltpu.VMEM((tm, ff), bf16), pltpu.VMEM((tm, d), f32), pltpu.SemaphoreType.DMA((nc + 1, 2))],
        name="mlpb", ident=ident)


def turn_back(t, cos, sin):
    t = t.astype(f32)
    return (t * cos - pltpu.roll(t, HEAD // 2, 1) * sin).astype(bf16)


def _attnb(q_ref, k_ref, v_ref, do_ref, lse_ref, delta_ref, cos_ref, sin_ref, dq_ref, dkv_ref, dq_s, dk_s, dv_s, *_):
    bq, nh, kv = q_ref.shape[0], q_ref.shape[1] // HEAD, k_ref.shape[1] // HEAD
    g = nh // kv
    iq = pl.program_id(0)
    scale = HEAD**-0.5
    e = scale * LOG2E
    at = lambda n: slice(n * HEAD, (n + 1) * HEAD)

    @pl.when(iq == 0)
    def _():
        dk_s[...] = jnp.zeros_like(dk_s)
        dv_s[...] = jnp.zeros_like(dv_s)

    dq_s[...] = jnp.zeros_like(dq_s)

    def block(j, masked):
        here = pl.ds(pl.multiple_of(j * bq, bq), bq)
        ks = [k_ref[here, at(i)] for i in range(kv)]
        vs = [v_ref[here, at(i)] for i in range(kv)]
        for n in range(nh):
            i = n // g
            q, do = q_ref[:, at(n)], do_ref[:, at(n)]
            s = dot(ks[i], q, 1, 1)
            dp = dot(vs[i], do, 1, 1)
            p = jnp.exp2(s * e - lse_ref[n : n + 1, :] * LOG2E)
            if masked:
                p = jnp.where(_below(bq, bq), p, 0.0)
            ds = (p * (dp - delta_ref[n : n + 1, :])).astype(bf16)
            dv_s[i, here, :] += dot(p.astype(bf16), do)
            dk_s[i, here, :] += dot(ds, q)
            dq_s[n] += dot(ks[i].T, ds)

    lax.fori_loop(0, iq, lambda j, _: block(j, False), None)
    block(iq, True)
    mine = pl.ds(pl.multiple_of(iq * bq, bq), bq)
    cos, sin = cos_ref[mine, :], sin_ref[mine, :]
    for n in range(nh):
        dq_ref[:, at(n)] = turn_back((dq_s[n] * scale).astype(bf16).T, cos, sin)

    @pl.when(iq == pl.num_programs(0) - 1)
    def _():
        for i in range(kv):
            dkv_ref[:, at(i)] = turn_back((dk_s[i] * scale).astype(bf16), cos_ref[...], sin_ref[...])
            dkv_ref[:, at(kv + i)] = dv_s[i].astype(bf16)


def attnb(q, k, v, do, lse, delta, cos, sin, riders, plan, dp, ident, bq=512):
    t, nd = q.shape
    nh, kv = nd // HEAD, k.shape[1] // HEAD
    rows = pl.BlockSpec((bq, nd), lambda i: (i, 0))
    stats = pl.BlockSpec((nh, bq), lambda i: (0, i))
    return ride(
        _attnb, riders, plan, dp, grid=(t // bq,),
        ins=[(q, rows), whole(k), whole(v), (do, rows), (lse, stats), (delta, stats), whole(cos), whole(sin)],
        outs=[(sh((t, nd), bf16), rows), (sh((t, 2 * kv * HEAD), bf16), pl.BlockSpec((t, 2 * kv * HEAD), lambda i: (0, 0)))],
        scratch=[pltpu.VMEM((nh, HEAD, bq), f32), pltpu.VMEM((kv, t, HEAD), f32), pltpu.VMEM((kv, t, HEAD), f32)],
        name="attnb", ident=ident)


def _da(dq_ref, dkv_ref, h_ref, dh1_ref, wq_ref, wk_ref, wv_ref, dh_ref, *_):
    nk = wk_ref.shape[1]
    da = dot(dq_ref[...], wq_ref[...], 1, 1) + dot(dkv_ref[:, :nk], wk_ref[...], 1, 1) + dot(dkv_ref[:, nk:], wv_ref[...], 1, 1)
    dh_ref[...] = dh1_ref[...] + norm_back(h_ref[...].astype(f32), da.astype(bf16).astype(f32)).astype(bf16)


def states(dq, dkv, h, dh1, wq, wk, wv, riders, plan, dp, ident, tm=512):
    t, d = h.shape
    rows = lambda n: pl.BlockSpec((tm, n), lambda i: (i, 0))
    return ride(
        _da, riders, plan, dp, grid=(t // tm,),
        ins=[(dq, rows(dq.shape[1])), (dkv, rows(dkv.shape[1])), (h, rows(d)), (dh1, rows(d)), whole(wq), whole(wk), whole(wv)],
        outs=[(sh((t, d), bf16), rows(d))], scratch=[], name="states", ident=ident)


def _wgrad(nt, nr, splits, lhs_ref, *refs):
    place, _ = refs[-2:]
    rhs, refs = refs[:nr], refs[nr:-2]
    sends, owns, (stage, got, acc, send_sem, recv_sem) = refs[: len(splits)], refs[len(splits) : 2 * len(splits)], refs[2 * len(splits) :]
    s = pl.program_id(0)
    chips, _, rows, t = lhs_ref.shape
    first = s < nt
    tile = lambda n: remote(stage.at[n], got.at[n], send_sem.at[n], recv_sem.at[n], place.partner())

    @pl.when((s > 0) & (s <= nt))
    def _():
        tile(s - 1).start()

    kk = jnp.where(first, place.other, place.core)
    b = rhs[0][...] if nr == 1 else jnp.concatenate([r[...] for r in rhs], 1)
    term = dot(lhs_ref[:, kk].reshape(chips * rows, t), b).reshape(chips, rows, -1)

    @pl.when(first)
    def _():
        stage[s] = term.astype(bf16)

    @pl.when(s >= nt)
    def _():
        n = s - nt
        tile(n).wait_recv()
        total = term + got[n].astype(f32)
        acc[...] = total
        for (lo, hi), send, own in zip(splits, sends, owns):
            send[...] = total[:, :, lo:hi].astype(bf16)
            own[...] = acc[place.chip, :, lo:hi]

    @pl.when(s == 2 * nt - 1)
    def _():
        for n in range(nt):
            tile(n).wait_send()


def wgrad(lhs, rhs, nt, splits, riders, plan, dp, ident):
    m, t = lhs.shape
    chips, rows = dp // 2, m // dp
    w = sum(r.shape[1] for r in rhs) // nt
    at = lambda s: jnp.maximum(s - nt, 0)
    sends = [(sh((chips, rows, nt * (hi - lo)), bf16), pl.BlockSpec((chips, rows, hi - lo), lambda s: (0, 0, at(s)))) for lo, hi in splits]
    owns = [(sh((rows, nt * (hi - lo)), f32), pl.BlockSpec((rows, hi - lo), lambda s: (0, at(s)))) for lo, hi in splits]
    got, rest = ride(
        functools.partial(_wgrad, nt, len(rhs), splits), riders, plan, dp, grid=(2 * nt,),
        ins=[whole(lhs.reshape(chips, 2, rows, t))] + [(r, pl.BlockSpec((t, r.shape[1] // nt), lambda s: (0, lax.rem(s, nt)))) for r in rhs],
        outs=sends + owns,
        scratch=[pltpu.VMEM((nt, chips, rows, w), bf16), pltpu.VMEM((nt, chips, rows, w), bf16), pltpu.VMEM((chips, rows, w), f32),
                 pltpu.SemaphoreType.DMA((nt,)), pltpu.SemaphoreType.DMA((nt,))],
        name="wgrad", ident=ident, greets=(0,), meet=1)
    return list(zip(got[: len(splits)], got[len(splits) :])), rest


def adamw(w, m, v, g):
    m = 0.9 * m + 0.1 * g
    v = 0.95 * v + 0.05 * g * g
    step = m * lax.rsqrt(v + 1e-8) + 0.1 * w
    return (w - 0.02 * step).astype(jnp.bfloat16), m, v


def solution(mesh):
    dp = mesh.shape["dp"]

    def step(x, dy, *arrays):
        weights, m, v = (arrays[i : i + 7] for i in (0, 7, 14))
        wq, wk, wv, wo, wg, wu, wd = weights
        layers = wq.shape[0]
        h, t = x[0], x.shape[1]
        full = lambda w: w.reshape(-1, w.shape[2])
        gather = lambda number, *ws: [Gather(w, number, dp) for w in ws]
        of = lambda act, riders: [(r, act) for r in riders]
        stages = lambda n: [of(act, range(n)) for act in ("start", "forward", "last", "finish")]
        sums = lambda n: [of(act, range(n)) for act in ("start", "add", "pass_on", "finish")]
        idents = iter(range(1000))

        (cos, sin), got = opening(t, gather(0, wq, wk, wv), dp, next(idents))
        kept, fetched = [], []
        for number in range(layers):
            w_q, w_k, w_v = (full(w) for w in got[:3])
            if number == 0:
                a, b, c, e = stages(1)
                (at, q, k, vv), got = qkv(h, w_q, w_k, w_v, cos, sin, gather(number, wo), [(0, a), (2.5, b), (3.5, c + e)], dp, next(idents))
                w_o = full(got[0])
            else:
                (at, q, k, vv), _ = qkv(h, w_q, w_k, w_v, cos, sin, [], [], dp, 0)
                w_o = full(got[3])
            a, b, c, e = stages(2)
            (o, ot, lse), got = attn(q, k, vv, gather(number, wg, wu), [(0, a), (2.5, b[:1]), (3.5, b[1:] + c + e)], dp, next(idents))
            w_g, w_u = full(got[0]), full(got[1])
            if number + 1 < layers:
                a, b, c, e = stages(5)
                riders = gather(number, wd) + gather(number + 1, wq, wk, wv, wo)
                plan = [(0, a[:1]), (7.5, b[:1] + a[1:]), (11.5, c[:1] + b[1:]), (18.5, c[1:]), (23.5, e[1:])]
            else:
                a, b, c, e = stages(1)
                riders = gather(number, wd)
                plan = [(0, a), (7.5, b), (11.5, c)]
            (h1, bt, gu, actt, h2), got = mlp(h, o, w_o, w_g, w_u, riders, plan, dp, next(idents))
            w_d = full(got[0])
            got = got[1:]
            kept.append((h, at, q, k, vv, o, ot, lse, h1, bt, gu, actt))
            fetched.append((w_q, w_k, w_v, w_o, w_g, w_u, w_d))
            h = h2

        dh, owns, sent, waiting = dy[0], {}, {}, []

        def done(names, number, pairs):
            for name, (send, own) in zip(names, pairs, strict=True):
                owns[name, number] = own
                waiting.append((name, number, send))

        def board():
            names, riders = [w[:2] for w in waiting], [Reduce(w[2]) for w in waiting]
            waiting.clear()
            return riders, lambda got: sent.update({name: tuple(got[2 * n : 2 * n + 2]) for n, name in enumerate(names)})

        for number in reversed(range(layers)):
            h, at, q, k, vv, o, ot, lse, h1, bt, gu, actt = kept[number]
            w_q, w_k, w_v, w_o, w_g, w_u, w_d = fetched[number]
            pairs, _ = wgrad(actt, [dh], 4, ((0, 256),), [], [], dp, next(idents))
            done(["w_down"], number, pairs)
            riders, land = board()
            a, b, c, e = sums(len(riders))
            (dgu, dh1, do, delta), got = mlpb(dh, gu, h1, o, w_o, w_g, w_u, w_d, riders, [(0.5, a), (7.5, b), (8.5, c), (19.5, e)], dp, next(idents))
            land(got)
            pairs, _ = wgrad(bt, [dgu], 5, ((0, 640), (640, 1280)), [], [], dp, next(idents))
            done(["w_gate", "w_up"], number, pairs)
            if number == 0:
                pairs, _ = wgrad(ot, [dh1], 1, ((0, ot.shape[0]),), [], [], dp, next(idents))
                done(["wo"], number, pairs)
            riders, land = board()
            a, b, c, e = sums(len(riders))
            (dq, dkv), got = attnb(q, k, vv, do, lse, delta, cos, sin, riders, [(0, a), (1.5, b), (2, c), (3.5, e)], dp, next(idents))
            land(got)
            nq, nk = q.shape[1], k.shape[1]
            pairs, _ = wgrad(at, [dq, dkv], 1, ((0, nq), (nq, nq + nk), (nq + nk, nq + 2 * nk)), [], [], dp, next(idents))
            done(["wq", "wk", "wv"], number, pairs)
            if number:
                pairs, _ = wgrad(ot, [dh1], 1, ((0, ot.shape[0]),), [], [], dp, next(idents))
                done(["wo"], number, pairs)
                (dh,), _ = states(dq, dkv, h, dh1, w_q, w_k, w_v, [], [], dp, 0)
        riders, land = board()
        a, b, c, e = sums(len(riders))
        _, got = ride(lambda *_: None, riders, [(0, a), (0.5, b + c + e)], dp, grid=(1,), ins=[], outs=[], scratch=[], name="closing", ident=next(idents))
        land(got)
        names = ("wq", "wk", "wv", "wo", "w_gate", "w_up", "w_down")
        gradient = lambda name, n: (owns[name, n] + sent[name, n][0].astype(f32) + sent[name, n][1].astype(f32)).astype(bf16).astype(f32)
        gradients = [jnp.stack([gradient(name, number) for number in range(layers)]) for name in names]
        new = [adamw(w.astype(f32), m, v, g) for w, m, v, g in zip(weights, m, v, gradients, strict=True)]
        return tuple(one[which] for which in range(3) for one in new)

    rows, cut = P(("rep", "dp"), None, None), P(None, "dp", None)
    return jax.shard_map(
        step,
        mesh=mesh,
        in_specs=(rows, rows) + (cut,) * 21,
        out_specs=(P("rep", "dp", None),) * 21,
        check_vma=False,
    )
```

```python
import functools

import jax
import jax.numpy as jnp
import numpy as np
from jax import lax
from jax.experimental import pallas as pl
from jax.experimental.pallas import tpu as pltpu
from jax.sharding import PartitionSpec as P

f32, bf16 = jnp.float32, jnp.bfloat16
sh = jax.ShapeDtypeStruct
HEAD = 128
THETA = 10000
NEG = -1e30
HIDDEN = 2 * NEG
LOG2E = 1.4426950408889634
ANY = pl.BlockSpec(memory_space=pl.ANY)
BIG = 63 * 2**20


def dot(a, b, ca=1, cb=0):
    return lax.dot_general(a, b, (((ca,), (cb,)), ((), ())), preferred_element_type=f32)


def _fit(size, want):
    return max(n for n in range(128, want + 1, 128) if size % n == 0)


def once(shape, index):
    return pl.BlockSpec(shape, index, pipeline_mode=pl.Buffered(1))


def whole(a):
    return a, once(a.shape, lambda *_: (0,) * a.ndim)


def rms(wide):
    return lax.rsqrt(jnp.mean(wide * wide, -1, keepdims=True) + 1e-6)


def norm_back(wide, db):
    r = rms(wide)
    return r * db - wide * (r * r * r * (jnp.sum(db * wide, -1, keepdims=True) * (1 / wide.shape[1])))


def params(n, **kw):
    return pltpu.CompilerParams(dimension_semantics=("arbitrary",) * n, vmem_limit_bytes=BIG, **kw)


class Place:
    def __init__(self, dp):
        me = lax.axis_index("dp")
        self.chips = dp // 2
        self.chip, self.core = me // 2, lax.rem(me, 2)
        self.other = 1 - self.core

    def at(self, step):
        return lax.rem(self.chip + step + self.chips, self.chips)

    def slot(self, step, core):
        return 2 * self.at(step) + core

    def partner(self):
        return {"dp": self.slot(0, self.other)}

    def neighbour(self, step):
        return {"dp": self.slot(step, self.core)}


def remote(src, dst, send, recv, device):
    return pltpu.make_async_remote_copy(src_ref=src, dst_ref=dst, send_sem=send, recv_sem=recv, device_id=device,
                                        device_id_type=pl.DeviceIdType.MESH)


def _half(rows):
    return -(-rows // 32) * 16


class Rider:
    greets = ()

    def bind(self, ins, outs, scratch, place):
        bound = object.__new__(type(self))
        bound.__dict__.update(self.__dict__)
        bound.p = place
        bound.refs(ins, outs, scratch)
        return bound


class Gather(Rider):
    greets = (1, -1, 0)

    def __init__(self, w, number, dp, cols=None):
        self.number = number
        self.first, end = cols or (0, w.shape[2])
        self.rows, self.n = w.shape[1], end - self.first
        self.inputs = [w]
        self.outs = [sh((dp, self.rows, self.n), w.dtype)]
        self.scratch = [pltpu.VMEM((self.rows, self.n), w.dtype), pltpu.SemaphoreType.DMA((8,)), pltpu.SemaphoreType.DMA((8,)),
                        pltpu.SemaphoreType.DMA((2,))]

    def refs(self, ins, outs, scratch):
        self.src, self.out = ins[0].at[self.number, :, pl.ds(self.first, self.n)], outs[0]
        self.stage, self.send, self.recv, self.own = scratch

    def _copy(self, t, incoming=False):
        p, half = self.p, _half(self.rows)
        whole, top, low = pl.ds(0, self.rows), pl.ds(0, half), pl.ds(half, self.rows - half)
        step, core, rows, to = (
            (0, p.core, whole, 1), (0, p.core, whole, -1), (0, p.core, whole, 0),
            (-1, p.core, top, 1), (1, p.core, low, -1),
            (-1, p.core, whole, 0), (1, p.core, whole, 0), (2, p.core, whole, 0),
        )[t]
        if incoming:
            step, core = (step, p.other) if to == 0 else (step - to, core)
        at = self.out.at[p.slot(step, core), rows]
        src = self.src if t < 3 and not incoming else at
        return remote(src, at, self.send.at[t], self.recv.at[t], p.partner() if to == 0 else p.neighbour(to))

    def _into(self):
        return pltpu.make_async_copy(self.src, self.stage, self.own.at[0])

    def _out_of(self):
        return pltpu.make_async_copy(self.stage, self.out.at[self.p.slot(0, self.p.core)], self.own.at[1])

    def start(self):
        for t in (0, 1, 2):
            self._copy(t).start()
        self._into().start()

    def forward(self):
        self._copy(0, True).wait_recv()
        self._copy(3).start()
        self._copy(5).start()
        self._copy(1, True).wait_recv()
        self._copy(4).start()
        self._copy(6).start()
        self._into().wait()
        self._out_of().start()

    def last(self):
        self._copy(3, True).wait_recv()
        self._copy(4, True).wait_recv()
        self._copy(7).start()

    def finish(self):
        for t in (2, 5, 6, 7):
            self._copy(t, True).wait_recv()
        for t in range(8):
            self._copy(t).wait_send()
        self._out_of().wait()


class Reduce(Rider):
    greets = (1, -1)

    def __init__(self, blocks):
        self.rows, self.n = blocks.shape[1:]
        half = _half(self.rows)
        self.inputs = [blocks]
        self.outs = [sh((self.rows, self.n), blocks.dtype)] * 2
        parts = [pltpu.VMEM((half, self.n), blocks.dtype), pltpu.VMEM((self.rows - half, self.n), blocks.dtype)]
        self.scratch = parts + parts + [pltpu.SemaphoreType.DMA((6,)), pltpu.SemaphoreType.DMA((6,)), pltpu.SemaphoreType.DMA((2,))]

    def refs(self, ins, outs, scratch):
        self.blocks, (self.before, self.after) = ins[0], outs
        self.top, self.low, self.own_top, self.own_low, self.send, self.recv, self.local = scratch

    def _copy(self, t):
        p, half = self.p, _half(self.rows)
        top, low = pl.ds(0, half), pl.ds(half, self.rows - half)
        block = lambda step, rows: self.blocks.at[p.at(step), rows]
        src, dst, to = (
            (block(2, top), self.top, 1), (block(2, low), self.low, -1),
            (self.own_top, self.before.at[top], 1), (block(1, low), self.before.at[low], 1),
            (block(-1, top), self.after.at[top], -1), (self.own_low, self.after.at[low], -1),
        )[t]
        return remote(src, dst, self.send.at[t], self.recv.at[t], p.neighbour(to))

    def _own(self):
        p, half = self.p, _half(self.rows)
        return (pltpu.make_async_copy(self.blocks.at[p.at(1), pl.ds(0, half)], self.own_top, self.local.at[0]),
                pltpu.make_async_copy(self.blocks.at[p.at(-1), pl.ds(half, self.rows - half)], self.own_low, self.local.at[1]))

    def start(self):
        for t in (0, 1):
            self._copy(t).start()
        for one in self._own():
            one.start()

    def rest(self):
        for t in (3, 4):
            self._copy(t).start()

    def add(self):
        for one in self._own():
            one.wait()
        self._copy(0).wait_recv()
        self.own_top[...] = (self.own_top[...].astype(f32) + self.top[...].astype(f32)).astype(bf16)
        self._copy(1).wait_recv()
        self.own_low[...] = (self.own_low[...].astype(f32) + self.low[...].astype(f32)).astype(bf16)

    def pass_on(self):
        for t in (2, 5):
            self._copy(t).start()

    def finish(self):
        for t in (2, 3, 4, 5):
            self._copy(t).wait_recv()
        for t in range(6):
            self._copy(t).wait_send()


def greet(place, whom):
    for to in whom:
        pl.semaphore_signal(pltpu.get_barrier_semaphore(), inc=1, device_id=place.neighbour(to) if to else place.partner(),
                            device_id_type=pl.DeviceIdType.MESH)


def greeted(whom):
    pl.semaphore_wait(pltpu.get_barrier_semaphore(), len(whom))


def ride(kernel, riders, plan, dp, ident, *, grid, ins, outs, scratch, name, greets=(), meet=None):
    counts = (len(ins), len(outs), len(scratch))
    steps = 1
    for n in grid:
        steps *= n
    whom = tuple(to for to in (1, -1, 0) if to in greets or any(to in r.greets for r in riders))
    plan = ([(meet, [])] if meet is not None else []) + list(plan)

    def body(*refs):
        refs = list(refs)
        take = lambda n: [refs.pop(0) for _ in range(n)]
        own_in, ride_in = take(counts[0]), [take(len(r.inputs)) for r in riders]
        own_out, ride_out = take(counts[1]), [take(len(r.outs)) for r in riders]
        own_scr, ride_scr = take(counts[2]), [take(len(r.scratch)) for r in riders]
        step = 0
        for axis, n in enumerate(grid):
            step = step * n + pl.program_id(axis)
        place = Place(dp) if whom else None
        bound = [r.bind(a, b, c, place) for r, a, b, c in zip(riders, ride_in, ride_out, ride_scr)]

        def act(half):
            for k, (when, what) in enumerate(plan):
                if int(2 * when) % 2 == half:

                    def do(k=k, what=what):
                        if k == 0:
                            greeted(whom)
                        for number, action in what:
                            getattr(bound[number], action)()

                    pl.when(step == int(when))(do)

        if whom:
            pl.when(step == 0)(lambda: greet(place, whom))
        act(0)
        kernel(*own_in, *own_out, *own_scr, place, bound)
        act(1)

    flat = lambda name: [x for r in riders for x in getattr(r, name)]
    got = pl.pallas_call(
        body, grid=grid,
        in_specs=[s for _, s in ins] + [ANY] * len(flat("inputs")),
        out_specs=[s for _, s in outs] + [ANY] * len(flat("outs")),
        out_shape=[s for s, _ in outs] + flat("outs"),
        scratch_shapes=list(scratch) + flat("scratch"),
        compiler_params=params(len(grid), **(dict(collective_id=ident, has_side_effects=True) if whom else {})), name=name,
    )(*[a for a, _ in ins], *flat("inputs"))
    own, rest = got[: counts[1]], list(got[counts[1] :])
    return own, rest


def _open(freq_ref, cos_ref, sin_ref, _, riders):
    greeted(Gather.greets)
    for r in riders:
        r.start()
    place = lax.broadcasted_iota(jnp.int32, cos_ref.shape, 0).astype(f32)
    angle = place * freq_ref[...]
    left = lax.broadcasted_iota(jnp.int32, sin_ref.shape, 1) < HEAD // 2
    cos_ref[...] = jnp.cos(angle)
    sin = jnp.sin(angle)
    sin_ref[...] = jnp.where(left, -sin, sin)
    for r in riders:
        r.forward()
    for r in riders:
        r.last()
    for r in riders:
        r.finish()


def opening(t, riders, dp, ident):
    half = HEAD // 2
    freq = np.float32(THETA) ** (-np.arange(half, dtype=np.float32) / half)
    freq = jnp.asarray(np.concatenate([freq, freq])[None], f32)
    table = sh((t, HEAD), f32), pl.BlockSpec((t, HEAD), lambda i: (0, 0))
    return ride(_open, riders, [], dp, grid=(1,), ins=[whole(freq)], outs=[table, table], scratch=[], name="opening", ident=ident)


def _qkv(h_ref, wq_ref, wk_ref, wv_ref, cos_ref, sin_ref, at_ref, q_ref, k_ref, v_ref, *_):
    wide = h_ref[...].astype(f32)
    a = (wide * rms(wide)).astype(bf16)
    at_ref[...] = a.T
    cos, sin = cos_ref[...], sin_ref[...]
    for w_ref, out_ref in ((wq_ref, q_ref), (wk_ref, k_ref)):
        t = dot(a, w_ref[...]).astype(bf16).astype(f32)
        for n in range(0, t.shape[1], HEAD):
            one = t[:, n : n + HEAD]
            out_ref[:, n : n + HEAD] = (one * cos + pltpu.roll(one, HEAD // 2, 1) * sin).astype(bf16)
    v_ref[...] = dot(a, wv_ref[...]).astype(bf16)


def qkv(h, wq, wk, wv, cos, sin, riders, plan, dp, ident, tm=512):
    t, d = h.shape
    rows = lambda n: pl.BlockSpec((tm, n), lambda i: (i, 0))
    return ride(
        _qkv, riders, plan, dp, grid=(t // tm,),
        ins=[(h, rows(d)), whole(wq), whole(wk), whole(wv), (cos, rows(HEAD)), (sin, rows(HEAD))],
        outs=[(sh((d, t), bf16), pl.BlockSpec((d, tm), lambda i: (0, i)))] + [(sh((t, w.shape[1]), bf16), rows(w.shape[1])) for w in (wq, wk, wv)],
        scratch=[], name="qkv", ident=ident)


def _below(bk, bq):
    return lax.broadcasted_iota(jnp.int32, (bk, bq), 1) >= lax.broadcasted_iota(jnp.int32, (bk, bq), 0)


def _attn(q_ref, k_ref, v_ref, o_ref, ot_ref, lse_ref, top_s, mix_s, *_):
    bq, nh, kv = q_ref.shape[0], q_ref.shape[1] // HEAD, k_ref.shape[1] // HEAD
    g = nh // kv
    iq = pl.program_id(0)
    e = HEAD**-0.5 * LOG2E
    top_s[...] = jnp.full(top_s.shape, NEG, f32)
    mix_s[...] = jnp.zeros(mix_s.shape, f32)
    ones = jnp.ones((8, bq), bf16)
    at = lambda n: slice(n * HEAD, (n + 1) * HEAD)

    def block(j, masked):
        here = pl.ds(pl.multiple_of(j * bq, bq), bq)
        scores = [dot(k_ref[here, at(n // g)], q_ref[:, at(n)], 1, 1) for n in range(nh)]
        values = [jnp.concatenate([v_ref[here, at(i)].T, ones], axis=0) for i in range(kv)]
        weights, keeps = [], []
        for n, s in enumerate(scores):
            if masked:
                s = jnp.where(_below(bq, bq), s, HIDDEN)
            old = top_s[n : n + 1, :]
            top = jnp.maximum(old, s.max(axis=0, keepdims=True))
            top_s[n : n + 1, :] = top
            weights.append(jnp.exp2((s - top) * e).astype(bf16))
            keeps.append(jnp.exp2((old - top) * e))
        for n, (p, keep) in enumerate(zip(weights, keeps)):
            mix_s[n] = mix_s[n] * keep + dot(values[n // g], p)

    lax.fori_loop(0, iq, lambda j, _: block(j, False), None)
    block(iq, True)
    for n in range(nh):
        total = mix_s[n, HEAD : HEAD + 1, :]
        out = (mix_s[n, :HEAD, :] * (1 / total)).astype(bf16)
        ot_ref[at(n), :] = out
        o_ref[:, at(n)] = out.T
        lse_ref[n : n + 1, :] = top_s[n : n + 1, :] * HEAD**-0.5 + jnp.log(total)


def attn(q, k, v, riders, plan, dp, ident, bq=512):
    t, nd = q.shape
    nh = nd // HEAD
    rows = pl.BlockSpec((bq, nd), lambda i: (i, 0))
    return ride(
        _attn, riders, plan, dp, grid=(t // bq,), ins=[(q, rows), whole(k), whole(v)],
        outs=[(sh((t, nd), bf16), rows), (sh((nd, t), bf16), pl.BlockSpec((nd, bq), lambda i: (0, i))),
              (sh((nh, t), f32), pl.BlockSpec((nh, bq), lambda i: (0, i)))],
        scratch=[pltpu.VMEM((nh, bq), f32), pltpu.VMEM((nh, HEAD + 8, bq), f32)], name="attn", ident=ident)


def _mlp(cw, nt, nc, early, h_ref, o_ref, wo_hbm, *refs):
    riders, refs = refs[-1], list(refs[:-2])
    pairs = [(refs.pop(0), refs.pop(0)) for _ in range(early)] + [(riders[2 * n].out, riders[2 * n + 1].out) for n in range(nc - early)]
    wd_hbm = riders[2 * (nc - early)].out
    h1_ref, bt_ref, gu_ref, actt_ref, h2_ref, wo_s, wgu_s, wd_s, b_s, act_s, h1_s, sems = refs
    s = pl.program_id(0)
    gu0, down0 = nt, nt + nt * nc
    slots = wgu_s.shape[0]

    def chunk(n):
        return [pltpu.make_async_copy(src, wgu_s.at[n % slots, :, :, pl.ds(k * cw, cw)], sems.at[n % slots, k]) for k, src in enumerate(pairs[n])]

    wo_copy = pltpu.make_async_copy(wo_hbm, wo_s, sems.at[slots, 0])
    wd_copy = pltpu.make_async_copy(wd_hbm, wd_s, sems.at[slots, 1])

    def load(n):
        if n >= early:
            riders[2 * (n - early)].finish()
            riders[2 * (n - early) + 1].finish()
        for one in chunk(n):
            one.start()

    @pl.when(s == 0)
    def _():
        wo_copy.start()
        load(0)
        wo_copy.wait()

    for n in range(nc):

        @pl.when(s == gu0 + n * nt)
        def _(n=n):
            for one in chunk(n):
                one.wait()

        if n + 1 < nc:

            @pl.when(s == gu0 + n * nt + nt - 2)
            def _(n=n):
                load(n + 1)

    @pl.when(s < gu0)
    def _():
        h1 = h_ref[...] + dot(o_ref[...], wo_s[...]).astype(bf16)
        h1_ref[...] = h1
        h1_s[s] = h1
        wide = h1.astype(f32)
        b = (wide * rms(wide)).astype(bf16)
        b_s[s] = b
        bt_ref[...] = b.T

    @pl.when((s >= gu0) & (s < down0))
    def _():
        n, i = (s - gu0) // nt, lax.rem(s - gu0, nt)
        gu = dot(b_s[i], wgu_s[lax.rem(n, slots)].reshape(b_s.shape[2], 2 * cw))
        gu_ref[...] = gu
        g, u = gu[:, :cw], gu[:, cw:]
        act = (g * lax.logistic(g) * u).astype(bf16)
        act_s[i, :, pl.ds(pl.multiple_of(n * cw, 128), cw)] = act
        actt_ref[...] = act.T

    @pl.when(s == down0 - 2)
    def _():
        riders[2 * (nc - early)].finish()
        wd_copy.start()

    @pl.when(s == down0)
    def _():
        wd_copy.wait()

    @pl.when(s >= down0)
    def _():
        n = s - down0
        h2_ref[...] = h1_s[n] + dot(act_s[n], wd_s[...].reshape(-1, wd_s.shape[2])).astype(bf16)


def mlp(h, o, wo, chunks, riders, nc, plan, dp, ident, tm=512):
    t, d = h.shape
    cw, ff = chunks[0][0].shape[2], riders[2 * (nc - len(chunks))].rows * dp
    nt = t // tm
    row = lambda s: jnp.minimum(s, nt - 1)
    at = lambda s: lax.rem(jnp.clip(s - nt, 0, nt * nc - 1), nt)
    col = lambda s: jnp.clip(s - nt, 0, nt * nc - 1) // nt
    rows = lambda n: pl.BlockSpec((tm, n), lambda s: (row(s), 0))
    return ride(
        functools.partial(_mlp, cw, nt, nc, len(chunks)), riders, plan, dp, grid=(nt * (nc + 2),),
        ins=[(h, rows(d)), (o, rows(o.shape[1])), (wo, ANY)] + [(a, ANY) for pair in chunks for a in pair],
        outs=[(sh((t, d), bf16), rows(d)), (sh((d, t), bf16), pl.BlockSpec((d, tm), lambda s: (0, row(s)))),
              (sh((t, 2 * ff), f32), pl.BlockSpec((tm, 2 * cw), lambda s: (at(s), col(s)))),
              (sh((ff, t), bf16), pl.BlockSpec((cw, tm), lambda s: (col(s), at(s)))),
              (sh((t, d), bf16), pl.BlockSpec((tm, d), lambda s: (jnp.maximum(s - nt * (nc + 1), 0), 0)))],
        scratch=[pltpu.VMEM(wo.shape, bf16), pltpu.VMEM((2, dp, d // dp, 2 * cw), bf16), pltpu.VMEM((dp, ff // dp, d), bf16),
                 pltpu.VMEM((nt, tm, d), bf16), pltpu.VMEM((nt, tm, ff), bf16), pltpu.VMEM((nt, tm, d), bf16), pltpu.SemaphoreType.DMA((3, 2))],
        name="mlp", ident=ident)


def _mlpb(cw, cols, dh_ref, gu_ref, h1_ref, o_ref, wo_hbm, wd_hbm, *refs):
    pairs, refs = [refs[2 * n : 2 * n + 2] for n in range(cols)], refs[2 * cols : -2]
    dgu_ref, dh1_ref, do_ref, delta_ref, wo_s, wgu_s, wd_s, dact_s, acc_s, sems = refs
    i, c, nc = pl.program_id(0), pl.program_id(1), pl.num_programs(1)

    def chunk(n):
        return [pltpu.make_async_copy(src, wgu_s.at[n, :, pl.ds(k * cw, cw)], sems.at[n, k]) for k, src in enumerate(pairs[n])]

    wo_copy = pltpu.make_async_copy(wo_hbm, wo_s, sems.at[cols, 0])
    wd_copy = pltpu.make_async_copy(wd_hbm, wd_s, sems.at[cols, 1])

    @pl.when((i == 0) & (c == 0))
    def _():
        wd_copy.start()
        for n in range(cols):
            for one in chunk(n):
                one.start()
        wo_copy.start()
        wd_copy.wait()

    @pl.when(c == 0)
    def _():
        dact_s[...] = dot(dh_ref[...], wd_s[...], 1, 1).astype(bf16)

    for n in range(cols):

        @pl.when((i == 0) & (c == n))
        def _(n=n):
            for one in chunk(n):
                one.wait()

    dact = dact_s[:, pl.ds(pl.multiple_of(c * cw, 128), cw)].astype(f32)
    g, u = gu_ref[:, :cw], gu_ref[:, cw:]
    s = lax.logistic(g)
    gs = g * s
    dgu = jnp.concatenate([(dact * u * (s + gs * (1 - s))).astype(bf16), (dact * gs).astype(bf16)], axis=1)
    dgu_ref[...] = dgu
    term = dot(dgu, wgu_s[c], 1, 1)

    @pl.when(c == 0)
    def _():
        acc_s[...] = term

    @pl.when(c > 0)
    def _():
        acc_s[...] += term

    @pl.when((i == 0) & (c == nc - 1))
    def _():
        wo_copy.wait()

    @pl.when(c == nc - 1)
    def _():
        db = acc_s[...].astype(bf16).astype(f32)
        dh1 = dh_ref[...] + norm_back(h1_ref[...].astype(f32), db).astype(bf16)
        dh1_ref[...] = dh1
        do = dot(dh1, wo_s[...], 1, 1).astype(bf16)
        do_ref[...] = do
        each = do.astype(f32) * o_ref[...].astype(f32)
        heads = [each[:, n : n + HEAD].sum(-1, keepdims=True) for n in range(0, each.shape[1], HEAD)]
        delta_ref[...] = jnp.concatenate(heads, 1).T


def mlpb(dh, gu, h1, o, wo, chunks, wd, riders, plan, dp, ident, tm=512):
    t, d = dh.shape
    cw, ff = chunks[0][0].shape[1], wd.shape[0]
    nc, nh = ff // cw, o.shape[1] // HEAD
    rows = lambda n: pl.BlockSpec((tm, n), lambda i, c: (i, 0))
    tile = pl.BlockSpec((tm, 2 * cw), lambda i, c: (i, c))
    return ride(
        functools.partial(_mlpb, cw, len(chunks)), riders, plan, dp, grid=(t // tm, nc),
        ins=[(dh, rows(d)), (gu, tile), (h1, rows(d)), (o, rows(o.shape[1])), (wo, ANY), (wd, ANY)] + [(a, ANY) for pair in chunks for a in pair],
        outs=[(sh((t, 2 * ff), bf16), tile), (sh((t, d), bf16), rows(d)), (sh(o.shape, bf16), rows(o.shape[1])),
              (sh((nh, t), f32), pl.BlockSpec((nh, tm), lambda i, c: (0, i)))],
        scratch=[pltpu.VMEM(wo.shape, bf16), pltpu.VMEM((nc, d, 2 * cw), bf16), pltpu.VMEM(wd.shape, bf16),
                 pltpu.VMEM((tm, ff), bf16), pltpu.VMEM((tm, d), f32), pltpu.SemaphoreType.DMA((nc + 1, 2))],
        name="mlpb", ident=ident)


def turn_back(t, cos, sin):
    t = t.astype(f32)
    return (t * cos - pltpu.roll(t, HEAD // 2, 1) * sin).astype(bf16)


def _attnb(q_ref, k_ref, v_ref, do_ref, lse_ref, delta_ref, cos_ref, sin_ref, dq_ref, dkv_ref, dq_s, dk_s, dv_s, *_):
    bq, nh, kv = q_ref.shape[0], q_ref.shape[1] // HEAD, k_ref.shape[1] // HEAD
    g = nh // kv
    iq = pl.program_id(0)
    scale = HEAD**-0.5
    e = scale * LOG2E
    at = lambda n: slice(n * HEAD, (n + 1) * HEAD)

    @pl.when(iq == 0)
    def _():
        dk_s[...] = jnp.zeros_like(dk_s)
        dv_s[...] = jnp.zeros_like(dv_s)

    dq_s[...] = jnp.zeros_like(dq_s)

    def block(j, masked):
        here = pl.ds(pl.multiple_of(j * bq, bq), bq)
        ks = [k_ref[here, at(i)] for i in range(kv)]
        vs = [v_ref[here, at(i)] for i in range(kv)]
        for n in range(nh):
            i = n // g
            q, do = q_ref[:, at(n)], do_ref[:, at(n)]
            s = dot(ks[i], q, 1, 1)
            dp = dot(vs[i], do, 1, 1)
            p = jnp.exp2(s * e - lse_ref[n : n + 1, :] * LOG2E)
            if masked:
                p = jnp.where(_below(bq, bq), p, 0.0)
            ds = (p * (dp - delta_ref[n : n + 1, :])).astype(bf16)
            dv_s[i, here, :] += dot(p.astype(bf16), do)
            dk_s[i, here, :] += dot(ds, q)
            dq_s[n] += dot(ks[i].T, ds)

    lax.fori_loop(0, iq, lambda j, _: block(j, False), None)
    block(iq, True)
    mine = pl.ds(pl.multiple_of(iq * bq, bq), bq)
    cos, sin = cos_ref[mine, :], sin_ref[mine, :]
    for n in range(nh):
        dq_ref[:, at(n)] = turn_back((dq_s[n] * scale).astype(bf16).T, cos, sin)

    @pl.when(iq == pl.num_programs(0) - 1)
    def _():
        for i in range(kv):
            dkv_ref[:, at(i)] = turn_back((dk_s[i] * scale).astype(bf16), cos_ref[...], sin_ref[...])
            dkv_ref[:, at(kv + i)] = dv_s[i].astype(bf16)


def attnb(q, k, v, do, lse, delta, cos, sin, riders, plan, dp, ident, bq=512):
    t, nd = q.shape
    nh, kv = nd // HEAD, k.shape[1] // HEAD
    rows = pl.BlockSpec((bq, nd), lambda i: (i, 0))
    stats = pl.BlockSpec((nh, bq), lambda i: (0, i))
    return ride(
        _attnb, riders, plan, dp, grid=(t // bq,),
        ins=[(q, rows), whole(k), whole(v), (do, rows), (lse, stats), (delta, stats), whole(cos), whole(sin)],
        outs=[(sh((t, nd), bf16), rows), (sh((t, 2 * kv * HEAD), bf16), pl.BlockSpec((t, 2 * kv * HEAD), lambda i: (0, 0)))],
        scratch=[pltpu.VMEM((nh, HEAD, bq), f32), pltpu.VMEM((kv, t, HEAD), f32), pltpu.VMEM((kv, t, HEAD), f32)],
        name="attnb", ident=ident)


def _da(dq_ref, dkv_ref, h_ref, dh1_ref, wq_ref, wk_ref, wv_ref, dh_ref, *_):
    nk = wk_ref.shape[1]
    da = dot(dq_ref[...], wq_ref[...], 1, 1) + dot(dkv_ref[:, :nk], wk_ref[...], 1, 1) + dot(dkv_ref[:, nk:], wv_ref[...], 1, 1)
    dh_ref[...] = dh1_ref[...] + norm_back(h_ref[...].astype(f32), da.astype(bf16).astype(f32)).astype(bf16)


def states(dq, dkv, h, dh1, wq, wk, wv, riders, plan, dp, ident, tm=512):
    t, d = h.shape
    rows = lambda n: pl.BlockSpec((tm, n), lambda i: (i, 0))
    return ride(
        _da, riders, plan, dp, grid=(t // tm,),
        ins=[(dq, rows(dq.shape[1])), (dkv, rows(dkv.shape[1])), (h, rows(d)), (dh1, rows(d)), whole(wq), whole(wk), whole(wv)],
        outs=[(sh((t, d), bf16), rows(d))], scratch=[], name="states", ident=ident)


def _wgrad(nt, nr, splits, lhs_ref, *refs):
    place, _ = refs[-2:]
    rhs, refs = refs[:nr], refs[nr:-2]
    sends, owns, (stage, got, acc, send_sem, recv_sem) = refs[: len(splits)], refs[len(splits) : 2 * len(splits)], refs[2 * len(splits) :]
    s = pl.program_id(0)
    chips, _, rows, t = lhs_ref.shape
    first = s < nt
    tile = lambda n: remote(stage.at[n], got.at[n], send_sem.at[n], recv_sem.at[n], place.partner())

    @pl.when((s > 0) & (s <= nt))
    def _():
        tile(s - 1).start()

    kk = jnp.where(first, place.other, place.core)
    b = rhs[0][...] if nr == 1 else jnp.concatenate([r[...] for r in rhs], 1)
    term = dot(lhs_ref[:, kk].reshape(chips * rows, t), b).reshape(chips, rows, -1)

    @pl.when(first)
    def _():
        stage[s] = term.astype(bf16)

    @pl.when(s >= nt)
    def _():
        n = s - nt
        tile(n).wait_recv()
        total = term + got[n].astype(f32)
        acc[...] = total
        for (lo, hi), send, own in zip(splits, sends, owns):
            send[...] = total[:, :, lo:hi].astype(bf16)
            own[...] = acc[place.chip, :, lo:hi]

    @pl.when(s == 2 * nt - 1)
    def _():
        for n in range(nt):
            tile(n).wait_send()


def wgrad(lhs, rhs, nt, splits, riders, plan, dp, ident):
    m, t = lhs.shape
    chips, rows = dp // 2, m // dp
    w = sum(r.shape[1] for r in rhs) // nt
    at = lambda s: jnp.maximum(s - nt, 0)
    sends = [(sh((chips, rows, nt * (hi - lo)), bf16), pl.BlockSpec((chips, rows, hi - lo), lambda s: (0, 0, at(s)))) for lo, hi in splits]
    owns = [(sh((rows, nt * (hi - lo)), f32), pl.BlockSpec((rows, hi - lo), lambda s: (0, at(s)))) for lo, hi in splits]
    got, rest = ride(
        functools.partial(_wgrad, nt, len(rhs), splits), riders, plan, dp, grid=(2 * nt,),
        ins=[whole(lhs.reshape(chips, 2, rows, t))] + [(r, pl.BlockSpec((t, r.shape[1] // nt), lambda s: (0, lax.rem(s, nt)))) for r in rhs],
        outs=sends + owns,
        scratch=[pltpu.VMEM((nt, chips, rows, w), bf16), pltpu.VMEM((nt, chips, rows, w), bf16), pltpu.VMEM((chips, rows, w), f32),
                 pltpu.SemaphoreType.DMA((nt,)), pltpu.SemaphoreType.DMA((nt,))],
        name="wgrad", ident=ident, greets=(0,), meet=1)
    return list(zip(got[: len(splits)], got[len(splits) :], strict=True)), rest


def _adamw(count, layers, *refs):
    refs = list(refs)
    take = lambda n: [refs.pop(0) for _ in range(n)]
    weights, ms, vs = take(count), take(count), take(count)
    terms = [[take(3) for _ in range(count)] for _ in range(layers)]
    outs = take(count), take(count), take(count)
    for number in range(layers):

        @pl.when(pl.program_id(0) == number)
        def _(number=number):
            for k in range(count):
                own, before, after = terms[number][k]
                g = (own[...] + before[...].astype(f32) + after[...].astype(f32)).astype(bf16).astype(f32)
                w = weights[k][0].astype(f32)
                m = 0.9 * ms[k][0] + 0.1 * g
                v = 0.95 * vs[k][0] + 0.05 * g * g
                move = m * lax.rsqrt(v + 1e-8) + 0.1 * w
                outs[0][k][0] = (w - 0.02 * move).astype(bf16)
                outs[1][k][0], outs[2][k][0] = m, v


def adamw(weights, ms, vs, terms, shares=8):
    count, layers = len(weights), weights[0].shape[0]
    specs, grads = [], [[] for _ in range(layers)]
    for w in weights:
        _, rows, n = w.shape
        by_rows = rows % (16 * shares) == 0
        block = (rows // shares, n) if by_rows else (rows, n // shares)
        place = (lambda i: (i, 0)) if by_rows else (lambda i: (0, i))
        specs.append(pl.BlockSpec((1, *block), lambda l, i, place=place: (l, *place(i))))
        for number in range(layers):
            share = lambda l, i, number=number, place=place: place(jnp.where(l < number, 0, jnp.where(l > number, shares - 1, i)))
            grads[number] += [pl.BlockSpec(block, share)] * 3
    outs = pl.pallas_call(
        functools.partial(_adamw, count, layers), grid=(layers, shares),
        in_specs=specs * 3 + [s for one in grads for s in one], out_specs=specs * 3,
        out_shape=[sh(w.shape, bf16) for w in weights] + [sh(w.shape, f32) for w in weights] * 2,
        compiler_params=params(2), name="adamw",
    )(*weights, *ms, *vs, *[a for layer in terms for one in layer for a in one])
    return tuple(outs)


def solution(mesh):
    dp = mesh.shape["dp"]

    def step(x, dy, *arrays):
        weights, ms, vs = (arrays[i : i + 7] for i in (0, 7, 14))
        wq, wk, wv, wo, wg, wu, wd = weights
        layers, ff = wq.shape[0], wg.shape[2]
        cw = _fit(ff, 640)
        nc = ff // cw
        early = nc - nc // 2
        h, t = x[0], x.shape[1]
        full = lambda w: w.reshape(-1, w.shape[2])
        gather = lambda number, *ws: [Gather(w, number, dp) for w in ws]
        chunks = lambda number, which: [Gather(w, number, dp, (n * cw, n * cw + cw)) for n in which for w in (wg, wu)]
        pairs_of = lambda got: list(zip(got[::2], got[1::2]))
        do = lambda *named: [(r, act) for act, which in named for r in which]
        idents = iter(range(1000))

        (cos, sin), got = opening(t, gather(0, wq, wk, wv), dp, next(idents))
        kept, fetched = [], []
        for number in range(layers):
            w_q, w_k, w_v = (full(w) for w in got)
            plan = [(0, do(("start", [0]))), (1.5, do(("forward", [0]))), (2.5, do(("last", [0]))), (3.5, do(("finish", [0])))]
            (at, q, k, vv), got = qkv(h, w_q, w_k, w_v, cos, sin, gather(number, wo), plan, dp, next(idents))
            w_o = full(got[0])
            every = list(range(2 * early))
            plan = [(0, do(("start", every))), (1.5, do(("forward", every[:2]))), (2.5, do(("forward", every[2:]))),
                    (3.5, do(("last", every), ("finish", every)))]
            (o, ot, lse), first = attn(q, k, vv, chunks(number, range(early)), plan, dp, next(idents))
            first = pairs_of(first)
            riders = chunks(number, range(early, nc)) + gather(number, wd)
            late, down = list(range(len(riders) - 1)), [len(riders) - 1]
            near, far = late[:2], late[2:]
            plan = [(0, do(("start", late))), (3.5, do(("forward", near), ("start", down))), (6.5, do(("forward", far))), (8.5, do(("last", near)))]
            if number + 1 < layers:
                more = list(range(len(riders), len(riders) + 3))
                riders += gather(number + 1, wq, wk, wv)
                plan += [(16.5, do(("forward", down), ("last", far), ("start", more))), (20.5, do(("last", down))), (23.5, do(("forward", more))),
                         (27.5, do(("last", more), ("finish", more)))]
            else:
                plan += [(16.5, do(("forward", down), ("last", far))), (20.5, do(("last", down)))]
            (h1, bt, gu, actt, h2), got = mlp(h, o, w_o, first, riders, nc, plan, dp, next(idents))
            pairs = first + pairs_of(got[: len(late)])
            w_d, got = full(got[len(late)]), got[len(late) + 1 :]
            kept.append((h, at, q, k, vv, o, ot, lse, h1, bt, gu, actt))
            fetched.append((w_q, w_k, w_v, w_o, [(full(a), full(b)) for a, b in pairs], w_d))
            h = h2

        dh, owns, sent, waiting = dy[0], {}, {}, []

        def done(names, number, pairs):
            for name, (send, own) in zip(names, pairs, strict=True):
                owns[name, number] = own
                waiting.append((name, number, send))

        def ridden(call, times):
            names, riders = [w[:2] for w in waiting], [Reduce(w[2]) for w in waiting]
            waiting.clear()
            every = range(len(riders))
            plan = [(when, do(*((act, every) for act in acts))) for when, acts in times] if riders else []
            own, got = call(riders, plan, dp, next(idents))
            sent.update({name: tuple(got[2 * n : 2 * n + 2]) for n, name in enumerate(names)})
            return own

        for number in reversed(range(layers)):
            h, at, q, k, vv, o, ot, lse, h1, bt, gu, actt = kept[number]
            w_q, w_k, w_v, w_o, pairs, w_d = fetched[number]
            sums, _ = wgrad(actt, [dh], 4, ((0, 256),), [], [], dp, next(idents))
            done(["w_down"], number, sums)
            dgu, dh1, d_o, delta = ridden(functools.partial(mlpb, dh, gu, h1, o, w_o, pairs, w_d),
                                          [(0.5, ["start", "rest"]), (7.5, ["add"]), (8.5, ["pass_on"]), (19.5, ["finish"])])
            sums, _ = wgrad(ot, [dh1], 1, ((0, ot.shape[0]),), [], [], dp, next(idents))
            done(["wo"], number, sums)
            sums = ridden(functools.partial(wgrad, bt, [dgu], nc, ((0, cw), (cw, 2 * cw))),
                          [(1, ["start", "rest"]), (3.5, ["add"]), (4.5, ["pass_on"]), (9.5, ["finish"])])
            done(["w_gate", "w_up"], number, sums)
            dq, dkv = ridden(functools.partial(attnb, q, k, vv, d_o, lse, delta, cos, sin),
                             [(0, ["start", "rest"]), (1.5, ["add"]), (2, ["pass_on"]), (3.5, ["finish"])])
            nq, nk = q.shape[1], k.shape[1]
            sums, _ = wgrad(at, [dq, dkv], 1, ((0, nq), (nq, nq + nk), (nq + nk, nq + 2 * nk)), [], [], dp, next(idents))
            done(["wq", "wk", "wv"], number, sums)
            if number:
                (dh,), _ = states(dq, dkv, h, dh1, w_q, w_k, w_v, [], [], dp, 0)
        ridden(functools.partial(ride, lambda *_: None, grid=(1,), ins=[], outs=[], scratch=[], name="closing"),
               [(0, ["start", "rest"]), (0.5, ["add", "pass_on", "finish"])])
        names = ("wq", "wk", "wv", "wo", "w_gate", "w_up", "w_down")
        return adamw(weights, ms, vs, [[(owns[name, number], *sent[name, number]) for name in names] for number in range(layers)])

    rows, cut = P(("rep", "dp"), None, None), P(None, "dp", None)
    return jax.shard_map(
        step,
        mesh=mesh,
        in_specs=(rows, rows) + (cut,) * 21,
        out_specs=(P("rep", "dp", None),) * 21,
        check_vma=False,
    )
```

```python
import functools

import jax
import jax.numpy as jnp
import numpy as np
from jax import lax
from jax.experimental import pallas as pl
from jax.experimental.pallas import tpu as pltpu
from jax.sharding import PartitionSpec as P

f32, bf16 = jnp.float32, jnp.bfloat16
sh = jax.ShapeDtypeStruct
HEAD = 128
THETA = 10000
NEG = -1e30
HIDDEN = 2 * NEG
LOG2E = 1.4426950408889634
ANY = pl.BlockSpec(memory_space=pl.ANY)
BIG = 63 * 2**20


def dot(a, b, ca=1, cb=0):
    return lax.dot_general(a, b, (((ca,), (cb,)), ((), ())), preferred_element_type=f32)


def _fit(size, want):
    return max(n for n in range(128, want + 1, 128) if size % n == 0)


def once(shape, index):
    return pl.BlockSpec(shape, index, pipeline_mode=pl.Buffered(1))


def whole(a):
    return a, once(a.shape, lambda *_: (0,) * a.ndim)


def rms(wide):
    return lax.rsqrt(jnp.mean(wide * wide, -1, keepdims=True) + 1e-6)


def norm_back(wide, db):
    r = rms(wide)
    return r * db - wide * (r * r * r * (jnp.sum(db * wide, -1, keepdims=True) * (1 / wide.shape[1])))


def params(n, **kw):
    return pltpu.CompilerParams(dimension_semantics=("arbitrary",) * n, vmem_limit_bytes=BIG, **kw)


class Place:
    def __init__(self, dp):
        me = lax.axis_index("dp")
        self.chips = dp // 2
        self.chip, self.core = me // 2, lax.rem(me, 2)
        self.other = 1 - self.core

    def at(self, step):
        return lax.rem(self.chip + step + self.chips, self.chips)

    def slot(self, step, core):
        return 2 * self.at(step) + core

    def partner(self):
        return {"dp": self.slot(0, self.other)}

    def neighbour(self, step):
        return {"dp": self.slot(step, self.core)}


def remote(src, dst, send, recv, device):
    return pltpu.make_async_remote_copy(src_ref=src, dst_ref=dst, send_sem=send, recv_sem=recv, device_id=device,
                                        device_id_type=pl.DeviceIdType.MESH)


def _half(rows):
    return -(-rows // 32) * 16


class Rider:
    greets = ()

    def bind(self, ins, outs, scratch, place):
        bound = object.__new__(type(self))
        bound.__dict__.update(self.__dict__)
        bound.p = place
        bound.refs(ins, outs, scratch)
        return bound


class Gather(Rider):
    greets = (1, -1, 0)

    def __init__(self, w, number, dp, cols=None):
        self.number = number
        self.first, end = cols or (0, w.shape[2])
        self.rows, self.n = w.shape[1], end - self.first
        self.inputs = [w]
        self.outs = [sh((dp, self.rows, self.n), w.dtype)]
        self.scratch = [pltpu.VMEM((self.rows, self.n), w.dtype), pltpu.SemaphoreType.DMA((8,)), pltpu.SemaphoreType.DMA((8,)),
                        pltpu.SemaphoreType.DMA((2,))]

    def refs(self, ins, outs, scratch):
        self.src, self.out = ins[0].at[self.number, :, pl.ds(self.first, self.n)], outs[0]
        self.stage, self.send, self.recv, self.own = scratch

    def _copy(self, t, incoming=False):
        p, half = self.p, _half(self.rows)
        whole, top, low = pl.ds(0, self.rows), pl.ds(0, half), pl.ds(half, self.rows - half)
        step, core, rows, to = (
            (0, p.core, whole, 1), (0, p.core, whole, -1), (0, p.core, whole, 0),
            (-1, p.core, top, 1), (1, p.core, low, -1),
            (-1, p.core, whole, 0), (1, p.core, whole, 0), (2, p.core, whole, 0),
        )[t]
        if incoming:
            step, core = (step, p.other) if to == 0 else (step - to, core)
        at = self.out.at[p.slot(step, core), rows]
        src = self.src if t < 3 and not incoming else at
        return remote(src, at, self.send.at[t], self.recv.at[t], p.partner() if to == 0 else p.neighbour(to))

    def _into(self):
        return pltpu.make_async_copy(self.src, self.stage, self.own.at[0])

    def _out_of(self):
        return pltpu.make_async_copy(self.stage, self.out.at[self.p.slot(0, self.p.core)], self.own.at[1])

    def start(self):
        for t in (0, 1, 2):
            self._copy(t).start()
        self._into().start()

    def forward(self):
        self._copy(0, True).wait_recv()
        self._copy(3).start()
        self._copy(5).start()
        self._copy(1, True).wait_recv()
        self._copy(4).start()
        self._copy(6).start()
        self._into().wait()
        self._out_of().start()

    def last(self):
        self._copy(3, True).wait_recv()
        self._copy(4, True).wait_recv()
        self._copy(7).start()

    def finish(self):
        for t in (2, 5, 6, 7):
            self._copy(t, True).wait_recv()
        for t in range(8):
            self._copy(t).wait_send()
        self._out_of().wait()


class Reduce(Rider):
    greets = (1, -1)

    def __init__(self, blocks):
        self.rows, self.n = blocks.shape[1:]
        half = _half(self.rows)
        self.inputs = [blocks]
        self.outs = [sh((self.rows, self.n), blocks.dtype)] * 2
        parts = [pltpu.VMEM((half, self.n), blocks.dtype), pltpu.VMEM((self.rows - half, self.n), blocks.dtype)]
        self.scratch = parts + parts + [pltpu.SemaphoreType.DMA((6,)), pltpu.SemaphoreType.DMA((6,)), pltpu.SemaphoreType.DMA((2,))]

    def refs(self, ins, outs, scratch):
        self.blocks, (self.before, self.after) = ins[0], outs
        self.top, self.low, self.own_top, self.own_low, self.send, self.recv, self.local = scratch

    def _copy(self, t):
        p, half = self.p, _half(self.rows)
        top, low = pl.ds(0, half), pl.ds(half, self.rows - half)
        block = lambda step, rows: self.blocks.at[p.at(step), rows]
        src, dst, to = (
            (block(2, top), self.top, 1), (block(2, low), self.low, -1),
            (self.own_top, self.before.at[top], 1), (block(1, low), self.before.at[low], 1),
            (block(-1, top), self.after.at[top], -1), (self.own_low, self.after.at[low], -1),
        )[t]
        return remote(src, dst, self.send.at[t], self.recv.at[t], p.neighbour(to))

    def _own(self):
        p, half = self.p, _half(self.rows)
        return (pltpu.make_async_copy(self.blocks.at[p.at(1), pl.ds(0, half)], self.own_top, self.local.at[0]),
                pltpu.make_async_copy(self.blocks.at[p.at(-1), pl.ds(half, self.rows - half)], self.own_low, self.local.at[1]))

    def start(self):
        for t in (0, 1):
            self._copy(t).start()
        for one in self._own():
            one.start()

    def rest(self):
        for t in (3, 4):
            self._copy(t).start()

    def add(self):
        for one in self._own():
            one.wait()
        self._copy(0).wait_recv()
        self.own_top[...] = (self.own_top[...].astype(f32) + self.top[...].astype(f32)).astype(bf16)
        self._copy(1).wait_recv()
        self.own_low[...] = (self.own_low[...].astype(f32) + self.low[...].astype(f32)).astype(bf16)

    def pass_on(self):
        for t in (2, 5):
            self._copy(t).start()

    def finish(self):
        for t in (2, 3, 4, 5):
            self._copy(t).wait_recv()
        for t in range(6):
            self._copy(t).wait_send()


def greet(place, whom):
    for to in whom:
        pl.semaphore_signal(pltpu.get_barrier_semaphore(), inc=1, device_id=place.neighbour(to) if to else place.partner(),
                            device_id_type=pl.DeviceIdType.MESH)


def greeted(whom):
    pl.semaphore_wait(pltpu.get_barrier_semaphore(), len(whom))


def ride(kernel, riders, plan, dp, ident, *, grid, ins, outs, scratch, name, greets=(), meet=None):
    counts = (len(ins), len(outs), len(scratch))
    steps = 1
    for n in grid:
        steps *= n
    whom = tuple(to for to in (1, -1, 0) if to in greets or any(to in r.greets for r in riders))
    plan = ([(meet, [])] if meet is not None else []) + list(plan)

    def body(*refs):
        refs = list(refs)
        take = lambda n: [refs.pop(0) for _ in range(n)]
        own_in, ride_in = take(counts[0]), [take(len(r.inputs)) for r in riders]
        own_out, ride_out = take(counts[1]), [take(len(r.outs)) for r in riders]
        own_scr, ride_scr = take(counts[2]), [take(len(r.scratch)) for r in riders]
        step = 0
        for axis, n in enumerate(grid):
            step = step * n + pl.program_id(axis)
        place = Place(dp) if whom else None
        bound = [r.bind(a, b, c, place) for r, a, b, c in zip(riders, ride_in, ride_out, ride_scr)]

        def act(half):
            for k, (when, what) in enumerate(plan):
                if int(2 * when) % 2 == half:

                    def do(k=k, what=what):
                        if k == 0:
                            greeted(whom)
                        for number, action in what:
                            getattr(bound[number], action)()

                    pl.when(step == int(when))(do)

        if whom:
            pl.when(step == 0)(lambda: greet(place, whom))
        act(0)
        kernel(*own_in, *own_out, *own_scr, place, bound)
        act(1)

    flat = lambda name: [x for r in riders for x in getattr(r, name)]
    got = pl.pallas_call(
        body, grid=grid,
        in_specs=[s for _, s in ins] + [ANY] * len(flat("inputs")),
        out_specs=[s for _, s in outs] + [ANY] * len(flat("outs")),
        out_shape=[s for s, _ in outs] + flat("outs"),
        scratch_shapes=list(scratch) + flat("scratch"),
        compiler_params=params(len(grid), **(dict(collective_id=ident, has_side_effects=True) if whom else {})), name=name,
    )(*[a for a, _ in ins], *flat("inputs"))
    own, rest = got[: counts[1]], list(got[counts[1] :])
    return own, rest


class Voyage:
    def __init__(self, hbm, hold, sems, gathers, place):
        self.hbm, self.hold, self.sems, self.gathers, self.place = hbm, hold, sems, gathers, place

    def start(self, group):
        for r in self.gathers[group]:
            r.start()

    def forward(self, group):
        for r in self.gathers[group]:
            r.forward()

    def last(self, group):
        for r in self.gathers[group]:
            r.last()

    def finish(self, group):
        for r in self.gathers[group]:
            r.finish()

    def _loads(self, group):
        name, slot = group[0], group[-1] % 2
        at = {"qkv": 0, "wo": 3, "gu": 4 + 2 * slot, "wd": 8}[name]
        first, copies = 0, []
        for n, r in enumerate(self.gathers[group]):
            dst = self.hold[name].at[slot] if name == "gu" else self.hold[name]
            copies.append(pltpu.make_async_copy(r.out, dst.at[:, :, pl.ds(first, r.n)], self.sems.at[at + n]))
            first += r.n
        return copies

    def load(self, group):
        for one in self._loads(group):
            one.start()

    def loaded(self, group):
        for one in self._loads(group):
            one.wait()


def _matrix(ref):
    return ref[...].reshape(-1, ref.shape[-1])


def _qkv(s, ship, h_ref, a_ref, q_ref, k_ref, v_ref):
    tm = h_ref.shape[0]
    wide = h_ref[...].astype(f32)
    a = (wide * rms(wide)).astype(bf16)
    a_ref[...] = a
    rows = pl.ds(pl.multiple_of(s * tm, tm), tm)
    cos, sin = ship.hold["cos"][rows, :], ship.hold["sin"][rows, :]
    t = dot(a, _matrix(ship.hold["qkv"])).astype(bf16)
    first = 0
    for out_ref in (q_ref, k_ref):
        for n in range(0, out_ref.shape[1], HEAD):
            one = t[:, first + n : first + n + HEAD].astype(f32)
            out_ref[:, n : n + HEAD] = (one * cos + pltpu.roll(one, HEAD // 2, 1) * sin).astype(bf16)
        first += out_ref.shape[1]
    v_ref[...] = t[:, first:]


def _below(bk, bq):
    return lax.broadcasted_iota(jnp.int32, (bk, bq), 1) >= lax.broadcasted_iota(jnp.int32, (bk, bq), 0)


def _attn(iq, ship, q_ref, k_ref, v_ref, o_ref, lse_ref, top_s, mix_s):
    bq, nh, kv = q_ref.shape[0], q_ref.shape[1] // HEAD, k_ref.shape[1] // HEAD
    g = nh // kv
    e = HEAD**-0.5 * LOG2E
    top_s[...] = jnp.full(top_s.shape, NEG, f32)
    mix_s[...] = jnp.zeros(mix_s.shape, f32)
    ones = jnp.ones((8, bq), bf16)
    at = lambda n: slice(n * HEAD, (n + 1) * HEAD)

    def block(j, _):
        here = pl.ds(pl.multiple_of(j * bq, bq), bq)
        scores = [dot(k_ref[here, at(n // g)], q_ref[:, at(n)], 1, 1) for n in range(nh)]
        values = [jnp.concatenate([v_ref[here, at(i)].T, ones], axis=0) for i in range(kv)]
        weights, keeps = [], []
        for n, s in enumerate(scores):
            old = top_s[n : n + 1, :]
            top = jnp.maximum(old, s.max(axis=0, keepdims=True))
            top_s[n : n + 1, :] = top
            weights.append(jnp.exp2((s - top) * e).astype(bf16))
            keeps.append(jnp.exp2((old - top) * e))
        for n, (p, keep) in enumerate(zip(weights, keeps, strict=True)):
            mix_s[n] = mix_s[n] * keep + dot(values[n // g], p)

    def diagonal():
        half = bq // 2
        keys = [pl.ds(pl.multiple_of(iq * bq + n * half, half), half) for n in range(2)]
        both = [(dot(k_ref[keys[0], at(n // g)], q_ref[:, at(n)], 1, 1), dot(k_ref[keys[1], at(n // g)], q_ref[half:, at(n)], 1, 1))
                for n in range(nh)]
        values = [[jnp.concatenate([v_ref[rows, at(i)].T, ones[:, :half]], axis=0) for rows in keys] for i in range(kv)]
        weights, keeps = [], []
        for n, (s, s2) in enumerate(both):
            s, s2 = jnp.where(_below(half, bq), s, HIDDEN), jnp.where(_below(half, half), s2, HIDDEN)
            old = top_s[n : n + 1, :]
            top = jnp.maximum(old, s.max(axis=0, keepdims=True))
            top = jnp.concatenate([top[:, :half], jnp.maximum(top[:, half:], s2.max(axis=0, keepdims=True))], 1)
            top_s[n : n + 1, :] = top
            weights.append((jnp.exp2((s - top) * e).astype(bf16), jnp.exp2((s2 - top[:, half:]) * e).astype(bf16)))
            keeps.append(jnp.exp2((old - top) * e))
        for n, ((p, p2), keep) in enumerate(zip(weights, keeps, strict=True)):
            mix_s[n] = mix_s[n] * keep + dot(values[n // g][0], p)
            mix_s[n, :, half:] += dot(values[n // g][1], p2)

    lax.fori_loop(0, iq, block, None)
    diagonal()
    for n in range(nh):
        total = mix_s[n, HEAD : HEAD + 1, :]
        o_ref[:, at(n)] = (mix_s[n, :HEAD, :] * (1 / total)).astype(bf16).T
        lse_ref[n : n + 1, :] = top_s[n : n + 1, :] * HEAD**-0.5 + jnp.log(total)


def _wo(s, ship, h_ref, o_ref, h1_ref, b_ref):
    h1 = h_ref[...] + dot(o_ref[...], _matrix(ship.hold["wo"])).astype(bf16)
    h1_ref[...] = h1
    wide = h1.astype(f32)
    b_ref[...] = (wide * rms(wide)).astype(bf16)


def _gu(per, first, s, ship, b_ref, gu_ref, actt_ref):
    cw = actt_ref.shape[0]
    gu = dot(b_ref[...], _matrix(ship.hold["gu"].at[lax.rem(s // per + first, 2)]))
    g, u = gu[:, :cw], gu[:, cw:]
    p = lax.logistic(g)
    silu = g * p
    gu_ref[:, :cw] = u * (p + silu * (1 - p))
    gu_ref[:, cw:] = silu
    actt_ref[...] = (silu * u).astype(bf16).T


def _down(s, ship, actt_ref, h1_ref, h2_ref):
    h2_ref[...] = h1_ref[...] + dot(actt_ref[...], _matrix(ship.hold["wd"]), 0, 0).astype(bf16)


RATE, HOP, SIDE = 91.0, 4.0, 2.5
STEPS = {"qkv": [3.0] * 4, "attn": [3.3, 6.2, 9.2, 12.2], "wo": [3.3] * 2, "gu": [3.8] * 10, "down": [4.6] * 4}
AHEAD = 12.0


def timetable(phases, groups, need, size, clear):
    script = [{} for _ in phases]
    state = {g: ["wait", 0.0] for g in groups}
    now, link, here = 0.0, 0.0, (0, 0.0)

    def put(act, g):
        script[here[0]].setdefault(here[1], []).append((act, g))

    def step(g, force=False):
        nonlocal now, link
        what, ready = state[g]
        if what in ("wait", "held") or (ready > now and not force):
            return False
        now = max(now, ready)
        if what == "sent":
            link = max(link, now) + size[g] / RATE / 1e3
            state[g] = ["passed", link + HOP]
            put("forward", g)
        elif what == "passed":
            state[g] = ["aside", now + SIDE]
            put("last", g)
        elif what == "aside":
            if clear[g] is not None and (here[0], here[1]) < clear[g]:
                return False
            state[g] = ["held", now + 2.0]
            put("finish", g)
            if g in need:
                put("load", g)
        return True

    def send(g):
        nonlocal link
        link = max(link, now) + 2 * size[g] / RATE / 1e3
        state[g] = ["sent", link + HOP]
        put("start", g)

    def settle():
        for g in groups:
            while step(g):
                pass
        for g in groups:
            if state[g][0] == "wait" and link - now < AHEAD:
                send(g)

    for p, (_, _, durations) in enumerate(phases):
        for k, d in enumerate(durations):
            here = (p, float(k))
            for g in groups:
                if need.get(g) == (p, k):
                    if state[g][0] == "wait":
                        send(g)
                    while state[g][0] != "held":
                        step(g, True)
                        if state[g][0] != "held":
                            settle()
                    now = max(now, state[g][1])
                    put("loaded", g)
            settle() if k == 0 and p == 0 else None
            now += d
            here = (p, k + 0.5)
            settle()
    for g in groups:
        if state[g][0] == "wait":
            send(g)
        while state[g][0] != "held":
            step(g, True)
    return script, now


def voyage(h, weights, dp, ident, tm=512, bq=512, tb=1024):
    wq, wk, wv, wo, wg, wu, wd = weights
    t, d = h.shape
    layers, ff = wq.shape[0], wg.shape[2]
    nq, nk = wq.shape[2], wk.shape[2]
    cw = _fit(ff, 640)
    nc, per = ff // cw, t // tb
    half = HEAD // 2
    freq = np.float32(THETA) ** (-np.arange(half, dtype=np.float32) / half)
    freq = jnp.asarray(np.concatenate([freq, freq])[None], f32)

    gathers, shapes = {}, {("cos",): sh((t, HEAD), f32), ("sin",): sh((t, HEAD), f32)}
    phases, need, clear = [("open", 0, [5.0])], {}, {}
    for n in range(layers):
        gathers["qkv", n] = [Gather(w, n, dp) for w in (wq, wk, wv)]
        gathers["wo", n] = [Gather(wo, n, dp)]
        for c in range(nc):
            gathers["gu", n, n * nc + c] = [Gather(w, n, dp, (c * cw, c * cw + cw)) for w in (wg, wu)]
        gathers["wd", n] = [Gather(wd, n, dp)]
        first = len(phases)
        names = ["qkv", "attn", "wo", "gu"] + (["down"] if n + 1 < layers else [])
        phases += [(name, n, STEPS[name]) for name in names]
        need["qkv", n], need["wo", n] = (first, 0), (first + 2, 0)
        for c in range(nc):
            need["gu", n, n * nc + c] = (first + 3, c * per)
            clear["gu", n, n * nc + c + 2] = (first + 3, c * per + per - 0.5)
        if n + 1 < layers:
            need["wd", n] = (first + 4, 0)
        clear["qkv", n + 1], clear["wo", n + 1], clear["wd", n + 1] = (first, 3.5), (first + 2, 1.5), (first + 4, 3.5)
        for name, shape, kind in (("a", (t, d), bf16), ("q", (t, nq), bf16), ("k", (t, nk), bf16), ("v", (t, nk), bf16), ("o", (t, nq), bf16),
                                  ("lse", (nq // HEAD, t), f32), ("h1", (t, d), bf16), ("b", (t, d), bf16), ("gu", (t, 2 * ff), f32),
                                  ("actt", (ff, t), bf16)):
            shapes[name, n] = sh(shape, kind)
        if n + 1 < layers:
            shapes["h", n + 1] = sh((t, d), bf16)
    order = [g for g in gathers if g[0] == "gu"]
    for one, later in zip(order, order[2:]):
        p, k = need[one]
        clear[later] = (p, k + per - 0.5)
    groups = list(gathers)
    size = {g: sum(r.rows * r.n * 2 for r in gathers[g]) for g in groups}
    script, _ = timetable(phases, groups, need, size, {g: clear.get(g) for g in groups})

    rows = lambda n, m=tm: pl.BlockSpec((m, n), lambda s: (s, 0))
    all_of = lambda n: pl.BlockSpec((t, n), lambda s: (0, 0))
    nh = nq // HEAD

    def specs(name, n):
        return {
            "qkv": (_qkv, t // tm, [("h", rows(d))], [("a", rows(d)), ("q", rows(nq)), ("k", rows(nk)), ("v", rows(nk))], []),
            "attn": (_attn, t // bq, [("q", rows(nq, bq)), ("k", all_of(nk)), ("v", all_of(nk))],
                     [("o", rows(nq, bq)), ("lse", pl.BlockSpec((nh, bq), lambda s: (0, s)))],
                     [pltpu.VMEM((nh, bq), f32), pltpu.VMEM((nh, HEAD + 8, bq), f32)]),
            "wo": (_wo, t // tb, [("h", rows(d, tb)), ("o", rows(nq, tb))], [("h1", rows(d, tb)), ("b", rows(d, tb))], []),
            "gu": (functools.partial(_gu, per, n * nc), nc * per, [("b", pl.BlockSpec((tb, d), lambda s: (lax.rem(s, per), 0)))],
                   [("gu", pl.BlockSpec((tb, 2 * cw), lambda s: (lax.rem(s, per), s // per))),
                    ("actt", pl.BlockSpec((cw, tb), lambda s: (s // per, lax.rem(s, per))))], []),
            "down": (_down, t // tm, [("actt", pl.BlockSpec((ff, tm), lambda s: (0, s))), ("h1", rows(d))], [(("h", n + 1), rows(d))], []),
        }[name]

    share = d // dp
    hold = {"cos": ((t, HEAD), f32), "sin": ((t, HEAD), f32), "qkv": ((dp, share, nq + 2 * nk), bf16), "wo": ((dp, nq // dp, d), bf16),
            "gu": ((2, dp, share, 2 * cw), bf16), "wd": ((dp, ff // dp, d), bf16)}
    riders = [r for g in groups for r in gathers[g]]
    given, keys = [freq, h, *weights], list(shapes)

    def body(*refs):
        refs = list(refs)
        take = lambda n: [refs.pop(0) for _ in range(n)]
        freq_ref, h_ref, *w_refs = take(len(given))
        hbm = dict(zip(keys, take(len(keys)), strict=True))
        hbm["h", 0] = h_ref
        landed = take(len(riders))
        held = dict(zip(hold, take(len(hold)), strict=True))
        sems, table_sems = take(2)
        place = Place(dp)
        which = {id(w): ref for w, ref in zip(weights, w_refs, strict=True)}
        bound, left = {}, list(landed)
        for g in groups:
            bound[g] = [r.bind([which[id(r.inputs[0])]], [left.pop(0)], take(len(r.scratch)), place) for r in gathers[g]]
        ship = Voyage(hbm, held, sems, bound, place)

        def hook(p, s, part):
            for when, acts in script[p].items():
                if int(2 * when) % 2 == part:

                    @pl.when(s == int(when))
                    def _(acts=acts):
                        for act, g in acts:
                            getattr(ship, act)(g)

        greet(place, Gather.greets)
        greeted(Gather.greets)
        hook(0, 0, 0)
        angle = lax.broadcasted_iota(jnp.int32, (t, HEAD), 0).astype(f32) * freq_ref[...]
        held["cos"][...] = jnp.cos(angle)
        sin = jnp.sin(angle)
        held["sin"][...] = jnp.where(lax.broadcasted_iota(jnp.int32, (t, HEAD), 1) < half, -sin, sin)
        hook(0, 0, 1)
        for p, (name, n, _) in enumerate(phases):
            if p == 0:
                continue
            kernel, steps, ins, outs, scratch = specs(name, n)
            ref = lambda key: hbm[key if isinstance(key, tuple) else (key, n)]

            def inside(*scr, p=p, kernel=kernel, steps=steps, ins=ins, outs=outs, ref=ref):
                def at_step(step, *blocks):
                    s = step.index[0]
                    hook(p, s, 0)
                    kernel(s, ship, *blocks, *scr)
                    hook(p, s, 1)

                pltpu.emit_pipeline(at_step, grid=(steps,), in_specs=[x for _, x in ins], out_specs=[x for _, x in outs], _explicit_indices=True)(
                    *[ref(key) for key, _ in ins], *[ref(key) for key, _ in outs])

            pl.run_scoped(inside, *scratch)
        tables = [pltpu.make_async_copy(held[key], hbm[key,], table_sems.at[n]) for n, key in enumerate(("cos", "sin"))]
        for one in tables:
            one.start()
        for one in tables:
            one.wait()

    got = list(pl.pallas_call(
        body,
        in_specs=[pl.BlockSpec(memory_space=pltpu.VMEM)] + [ANY] * (len(given) - 1),
        out_specs=[ANY] * (len(keys) + len(riders)),
        out_shape=list(shapes.values()) + [r.outs[0] for r in riders],
        scratch_shapes=[pltpu.VMEM(*x) for x in hold.values()] + [pltpu.SemaphoreType.DMA((9,)), pltpu.SemaphoreType.DMA((2,))]
        + [x for r in riders for x in r.scratch],
        compiler_params=pltpu.CompilerParams(vmem_limit_bytes=BIG, collective_id=ident, has_side_effects=True), name="voyage",
    )(*given))
    saved = dict(zip(keys, got, strict=False))
    saved["h", 0] = h
    full, left = {}, got[len(keys) :]
    for g in groups:
        full[g] = [left.pop(0).reshape(-1, r.n) for r in gathers[g]]
    pairs = lambda n: [tuple(full["gu", n, n * nc + c]) for c in range(nc)]
    return saved, [(*full["qkv", n], full["wo", n][0], pairs(n), full["wd", n][0]) for n in range(layers)]


def _mlpb(cw, nc, dh_ref, h1_ref, o_ref, gu_hbm, wo_hbm, wd_hbm, *refs):
    pairs, refs = [refs[2 * n : 2 * n + 2] for n in range(nc)], refs[2 * nc : -2]
    dgu_hbm, dh1_ref, do_ref, delta_ref, wo_s, wgu_s, wd_s, gu_s, dgu_s, dact_s, acc_s, sems, gu_sems, dgu_sems = refs
    i, last = pl.program_id(0), pl.num_programs(0) - 1
    tm, ring = dh_ref.shape[0], gu_s.shape[0]
    chunk = lambda n: [pltpu.make_async_copy(src, wgu_s.at[n, :, pl.ds(k * cw, cw)], sems.at[n, k]) for k, src in enumerate(pairs[n])]
    wo_copy = pltpu.make_async_copy(wo_hbm, wo_s, sems.at[nc, 0])
    wd_copy = pltpu.make_async_copy(wd_hbm, wd_s, sems.at[nc, 1])
    rows = lambda n: pl.ds(pl.multiple_of(n * tm, tm), tm)
    place = lambda n: lax.rem(i * nc + n, ring)
    fetch = lambda block, n, at: pltpu.make_async_copy(gu_hbm.at[rows(block), pl.ds(n * 2 * cw, 2 * cw)], gu_s.at[at], gu_sems.at[at])
    give = lambda block, n: pltpu.make_async_copy(dgu_s.at[n], dgu_hbm.at[rows(block), pl.ds(n * 2 * cw, 2 * cw)], dgu_sems.at[n])

    @pl.when(i == 0)
    def _():
        wd_copy.start()
        for n in range(ring):
            fetch(0, n, n).start()
        for n in range(nc):
            for one in chunk(n):
                one.start()
        wo_copy.start()
        wd_copy.wait()

    def elementwise(n):
        fetch(i, n, place(n)).wait()

        @pl.when(i > 0)
        def _():
            give(i - 1, n).wait()

        both = gu_s.at[place(n)]
        dact = dact_s[:, n * cw : (n + 1) * cw].astype(f32)
        dgu_s[n, :, :cw] = (dact * both[:, :cw]).astype(bf16)
        dgu_s[n, :, cw:] = (dact * both[:, cw:]).astype(bf16)

    def done(n):
        give(i, n).start()
        later = n + ring
        if later < nc:
            fetch(i, later, place(later)).start()
        else:

            @pl.when(i < last)
            def _():
                fetch(i + 1, later - nc, place(later)).start()

    dact_s[...] = dot(dh_ref[...], wd_s[...], 1, 1).astype(bf16)
    elementwise(0)
    for n in range(nc):
        done(n)

        @pl.when(i == 0)
        def _(n=n):
            for one in chunk(n):
                one.wait()

        term = dot(dgu_s[n], wgu_s[n], 1, 1)
        acc_s[...] = term if n == 0 else acc_s[...] + term
        if n + 1 < nc:
            elementwise(n + 1)

    @pl.when(i == 0)
    def _():
        wo_copy.wait()

    db = acc_s[...].astype(bf16).astype(f32)
    dh1 = dh_ref[...] + norm_back(h1_ref[...].astype(f32), db).astype(bf16)
    dh1_ref[...] = dh1
    do = dot(dh1, wo_s[...], 1, 1).astype(bf16)
    do_ref[...] = do
    each = do.astype(f32) * o_ref[...].astype(f32)
    heads = [each[:, n : n + HEAD].sum(-1, keepdims=True) for n in range(0, each.shape[1], HEAD)]
    delta_ref[...] = jnp.concatenate(heads, 1).T

    @pl.when(i == last)
    def _():
        for n in range(nc):
            give(i, n).wait()


def mlpb(dh, gu, h1, o, wo, chunks, wd, riders, plan, dp, ident, tm=512, ring=3):
    t, d = dh.shape
    cw, ff, nc = chunks[0][0].shape[1], wd.shape[0], len(chunks)
    nh = o.shape[1] // HEAD
    rows = lambda n: pl.BlockSpec((tm, n), lambda i: (i, 0))
    return ride(
        functools.partial(_mlpb, cw, nc), riders, plan, dp, ident, grid=(t // tm,),
        ins=[(dh, rows(d)), (h1, rows(d)), (o, rows(o.shape[1])), (gu, ANY), (wo, ANY), (wd, ANY)] + [(a, ANY) for pair in chunks for a in pair],
        outs=[(sh((t, 2 * ff), bf16), ANY), (sh((t, d), bf16), rows(d)), (sh(o.shape, bf16), rows(o.shape[1])),
              (sh((nh, t), f32), pl.BlockSpec((nh, tm), lambda i: (0, i)))],
        scratch=[pltpu.VMEM(wo.shape, bf16), pltpu.VMEM((nc, d, 2 * cw), bf16), pltpu.VMEM(wd.shape, bf16),
                 pltpu.VMEM((ring, tm, 2 * cw), f32), pltpu.VMEM((nc, tm, 2 * cw), bf16), pltpu.VMEM((tm, ff), bf16), pltpu.VMEM((tm, d), f32),
                 pltpu.SemaphoreType.DMA((nc + 1, 2)), pltpu.SemaphoreType.DMA((ring,)), pltpu.SemaphoreType.DMA((nc,))],
        name="mlpb")


def turn_back(t, cos, sin):
    t = t.astype(f32)
    return (t * cos - pltpu.roll(t, HEAD // 2, 1) * sin).astype(bf16)


def _attnb(q_ref, k_ref, v_ref, do_ref, lse_ref, delta_ref, cos_ref, sin_ref, dq_ref, dkv_ref, dq_s, dk_s, dv_s, *_):
    bq, nh, kv = q_ref.shape[0], q_ref.shape[1] // HEAD, k_ref.shape[1] // HEAD
    g = nh // kv
    iq = pl.program_id(0)
    scale = HEAD**-0.5
    e = scale * LOG2E
    at = lambda n: slice(n * HEAD, (n + 1) * HEAD)

    @pl.when(iq == 0)
    def _():
        dk_s[...] = jnp.zeros_like(dk_s)
        dv_s[...] = jnp.zeros_like(dv_s)

    dq_s[...] = jnp.zeros_like(dq_s)

    def block(first, size, queries, masked):
        here = pl.ds(pl.multiple_of(first, size), size)
        ks = [k_ref[here, at(i)] for i in range(kv)]
        vs = [v_ref[here, at(i)] for i in range(kv)]
        for n in range(nh):
            i = n // g
            q, do = q_ref[queries:, at(n)], do_ref[queries:, at(n)]
            s = dot(ks[i], q, 1, 1)
            dp = dot(vs[i], do, 1, 1)
            p = jnp.exp2(s * e - lse_ref[n : n + 1, queries:] * LOG2E)
            if masked:
                p = jnp.where(_below(size, bq - queries), p, 0.0)
            ds = (p * (dp - delta_ref[n : n + 1, queries:])).astype(bf16)
            dv_s[i, here, :] += dot(p.astype(bf16), do)
            dk_s[i, here, :] += dot(ds, q)
            dq_s[n, :, queries:] += dot(ks[i].T, ds)

    lax.fori_loop(0, iq, lambda j, _: block(j * bq, bq, 0, False), None)
    half = bq // 2
    block(iq * bq, half, 0, True)
    block(iq * bq + half, half, half, True)
    mine = pl.ds(pl.multiple_of(iq * bq, bq), bq)
    cos, sin = cos_ref[mine, :], sin_ref[mine, :]
    for n in range(nh):
        dq_ref[:, at(n)] = turn_back((dq_s[n] * scale).astype(bf16).T, cos, sin)

    @pl.when(iq == pl.num_programs(0) - 1)
    def _():
        for i in range(kv):
            dkv_ref[:, at(i)] = turn_back((dk_s[i] * scale).astype(bf16), cos_ref[...], sin_ref[...])
            dkv_ref[:, at(kv + i)] = dv_s[i].astype(bf16)


def attnb(q, k, v, do, lse, delta, cos, sin, riders, plan, dp, ident, bq=512):
    t, nd = q.shape
    nh, kv = nd // HEAD, k.shape[1] // HEAD
    rows = pl.BlockSpec((bq, nd), lambda i: (i, 0))
    stats = pl.BlockSpec((nh, bq), lambda i: (0, i))
    return ride(
        _attnb, riders, plan, dp, grid=(t // bq,),
        ins=[(q, rows), whole(k), whole(v), (do, rows), (lse, stats), (delta, stats), whole(cos), whole(sin)],
        outs=[(sh((t, nd), bf16), rows), (sh((t, 2 * kv * HEAD), bf16), pl.BlockSpec((t, 2 * kv * HEAD), lambda i: (0, 0)))],
        scratch=[pltpu.VMEM((nh, HEAD, bq), f32), pltpu.VMEM((kv, t, HEAD), f32), pltpu.VMEM((kv, t, HEAD), f32)],
        name="attnb", ident=ident)


def _da(dq_ref, dkv_ref, h_ref, dh1_ref, wq_ref, wk_ref, wv_ref, dh_ref, *_):
    nk = wk_ref.shape[1]
    da = dot(dq_ref[...], wq_ref[...], 1, 1) + dot(dkv_ref[:, :nk], wk_ref[...], 1, 1) + dot(dkv_ref[:, nk:], wv_ref[...], 1, 1)
    dh_ref[...] = dh1_ref[...] + norm_back(h_ref[...].astype(f32), da.astype(bf16).astype(f32)).astype(bf16)


def states(dq, dkv, h, dh1, wq, wk, wv, riders, plan, dp, ident, tm=512):
    t, d = h.shape
    rows = lambda n: pl.BlockSpec((tm, n), lambda i: (i, 0))
    return ride(
        _da, riders, plan, dp, grid=(t // tm,),
        ins=[(dq, rows(dq.shape[1])), (dkv, rows(dkv.shape[1])), (h, rows(d)), (dh1, rows(d)), whole(wq), whole(wk), whole(wv)],
        outs=[(sh((t, d), bf16), rows(d))], scratch=[], name="states", ident=ident)


def _wgrad(nt, nr, splits, dp, lhs_ref, *refs):
    place, _ = refs[-2:]
    rhs, refs = refs[:nr], refs[nr:-2]
    sends, owns, (stage, got, acc, send_sem, recv_sem) = refs[: len(splits)], refs[len(splits) : 2 * len(splits)], refs[2 * len(splits) :]
    s = pl.program_id(0)
    chips = dp // 2
    first = s < nt
    tile = lambda n: remote(stage.at[n], got.at[n], send_sem.at[n], recv_sem.at[n], place.partner())

    @pl.when((s > 0) & (s <= nt))
    def _():
        tile(s - 1).start()

    kk = jnp.where(first, place.other, place.core)
    b = rhs[0][...] if nr == 1 else jnp.concatenate([r[...] for r in rhs], 1)
    if lhs_ref.ndim == 2:
        rows = lhs_ref.shape[1] // dp
        parts = [lhs_ref[:, pl.ds(pl.multiple_of((2 * n + kk) * rows, rows), rows)] for n in range(chips)]
        term = dot(jnp.concatenate(parts, 1), b, 0, 0)
    else:
        rows = lhs_ref.shape[2]
        term = dot(lhs_ref[:, kk].reshape(chips * rows, -1), b)
    term = term.reshape(chips, rows, -1)

    @pl.when(first)
    def _():
        stage[s] = term.astype(bf16)

    @pl.when(s >= nt)
    def _():
        n = s - nt
        tile(n).wait_recv()
        total = term + got[n].astype(f32)
        acc[...] = total
        for (lo, hi), send, own in zip(splits, sends, owns):
            send[...] = total[:, :, lo:hi].astype(bf16)
            own[...] = acc[place.chip, :, lo:hi]

    @pl.when(s == 2 * nt - 1)
    def _():
        for n in range(nt):
            tile(n).wait_send()


def wgrad(lhs, tall, rhs, nt, splits, riders, plan, dp, ident):
    m, t = lhs.shape if tall else lhs.shape[::-1]
    chips, rows = dp // 2, m // dp
    lhs = lhs.reshape(chips, 2, rows, t) if tall else lhs
    w = sum(r.shape[1] for r in rhs) // nt
    at = lambda s: jnp.maximum(s - nt, 0)
    sends = [(sh((chips, rows, nt * (hi - lo)), bf16), pl.BlockSpec((chips, rows, hi - lo), lambda s: (0, 0, at(s)))) for lo, hi in splits]
    owns = [(sh((rows, nt * (hi - lo)), f32), pl.BlockSpec((rows, hi - lo), lambda s: (0, at(s)))) for lo, hi in splits]
    got, rest = ride(
        functools.partial(_wgrad, nt, len(rhs), splits, dp), riders, plan, dp, grid=(2 * nt,),
        ins=[whole(lhs)] + [(r, pl.BlockSpec((t, r.shape[1] // nt), lambda s: (0, lax.rem(s, nt)))) for r in rhs],
        outs=sends + owns,
        scratch=[pltpu.VMEM((nt, chips, rows, w), bf16), pltpu.VMEM((nt, chips, rows, w), bf16), pltpu.VMEM((chips, rows, w), f32),
                 pltpu.SemaphoreType.DMA((nt,)), pltpu.SemaphoreType.DMA((nt,))],
        name="wgrad", ident=ident, greets=(0,), meet=1)
    return list(zip(got[: len(splits)], got[len(splits) :], strict=True)), rest


def _adamw(count, layers, *refs):
    refs = list(refs)
    take = lambda n: [refs.pop(0) for _ in range(n)]
    weights, ms, vs = take(count), take(count), take(count)
    terms = [[take(3) for _ in range(count)] for _ in range(layers)]
    outs = take(count), take(count), take(count)
    for number in range(layers):

        @pl.when(pl.program_id(0) == number)
        def _(number=number):
            for k in range(count):
                own, before, after = terms[number][k]
                g = (own[...] + before[...].astype(f32) + after[...].astype(f32)).astype(bf16).astype(f32)
                w = weights[k][0].astype(f32)
                m = 0.9 * ms[k][0] + 0.1 * g
                v = 0.95 * vs[k][0] + 0.05 * g * g
                move = m * lax.rsqrt(v + 1e-8) + 0.1 * w
                outs[0][k][0] = (w - 0.02 * move).astype(bf16)
                outs[1][k][0], outs[2][k][0] = m, v


def adamw(weights, ms, vs, terms, shares=8):
    count, layers = len(weights), weights[0].shape[0]
    specs, grads = [], [[] for _ in range(layers)]
    for w in weights:
        _, rows, n = w.shape
        by_rows = rows % (16 * shares) == 0
        block = (rows // shares, n) if by_rows else (rows, n // shares)
        place = (lambda i: (i, 0)) if by_rows else (lambda i: (0, i))
        specs.append(pl.BlockSpec((1, *block), lambda l, i, place=place: (l, *place(i))))
        for number in range(layers):
            share = lambda l, i, number=number, place=place: place(jnp.where(l < number, 0, jnp.where(l > number, shares - 1, i)))
            grads[number] += [pl.BlockSpec(block, share)] * 3
    outs = pl.pallas_call(
        functools.partial(_adamw, count, layers), grid=(layers, shares),
        in_specs=specs * 3 + [s for one in grads for s in one], out_specs=specs * 3,
        out_shape=[sh(w.shape, bf16) for w in weights] + [sh(w.shape, f32) for w in weights] * 2,
        compiler_params=params(2), name="adamw",
    )(*weights, *ms, *vs, *[a for layer in terms for one in layer for a in one])
    return tuple(outs)


def solution(mesh):
    dp = mesh.shape["dp"]

    def step(x, dy, *arrays):
        weights, ms, vs = (arrays[i : i + 7] for i in (0, 7, 14))
        layers = weights[0].shape[0]
        do = lambda *named: [(r, act) for act, which in named for r in which]
        idents = iter(range(1000))
        saved, fetched = voyage(x[0], weights, dp, next(idents))
        cos, sin = saved["cos",], saved["sin",]
        dh, owns, sent, waiting = dy[0], {}, {}, []

        def done(names, number, pairs):
            for name, (send, own) in zip(names, pairs, strict=True):
                owns[name, number] = own
                waiting.append((name, number, send))

        def ridden(call, times, leave=()):
            taken = [w for w in waiting if w[0] not in leave]
            waiting[:] = [w for w in waiting if w[0] in leave]
            names, riders = [w[:2] for w in taken], [Reduce(w[2]) for w in taken]
            every = range(len(riders))
            plan = [(when, do(*((act, every) for act in acts))) for when, acts in times] if riders else []
            own, got = call(riders, plan, dp, next(idents))
            sent.update({name: tuple(got[2 * n : 2 * n + 2]) for n, name in enumerate(names)})
            return own

        for number in reversed(range(layers)):
            h, a, q, k, vv, o, lse, h1, b, gu, actt = (saved[name, number] for name in ("h", "a", "q", "k", "v", "o", "lse", "h1", "b", "gu", "actt"))
            w_q, w_k, w_v, w_o, pairs, w_d = fetched[number]
            nc, cw = len(pairs), pairs[0][0].shape[1]
            riders, plan = [], []
            if w_d is None:
                riders = [Gather(weights[6], number, dp)]
                plan = [(1, do(("start", [0]))), (3.5, do(("forward", [0]))), (5.5, do(("last", [0]))), (7.5, do(("finish", [0])))]
            sums, got = wgrad(actt, True, [dh], 4, ((0, 256),), riders, plan, dp, next(idents))
            w_d = got[0].reshape(-1, got[0].shape[2]) if riders else w_d
            done(["w_down"], number, sums)
            dgu, dh1, d_o, delta = ridden(functools.partial(mlpb, dh, gu, h1, o, w_o, pairs, w_d),
                                          [(0, ["start", "rest"]), (1.5, ["add"]), (2, ["pass_on"]), (3.5, ["finish"])], ["wq", "wk", "wv"])
            sums, _ = wgrad(o, False, [dh1], 1, ((0, dh1.shape[1]),), [], [], dp, next(idents))
            done(["wo"], number, sums)
            sums = ridden(functools.partial(wgrad, b, False, [dgu], nc, ((0, cw), (cw, 2 * cw))),
                          [(1, ["start", "rest"]), (3.5, ["add"]), (4.5, ["pass_on"]), (9.5, ["finish"])])
            done(["w_gate", "w_up"], number, sums)
            dq, dkv = ridden(functools.partial(attnb, q, k, vv, d_o, lse, delta, cos, sin),
                             [(0, ["start", "rest"]), (1.5, ["add"]), (2, ["pass_on"]), (3.5, ["finish"])], ["w_up"] if number else [])
            nq, nk = q.shape[1], k.shape[1]
            sums, _ = wgrad(a, False, [dq, dkv], 1, ((0, nq), (nq, nq + nk), (nq + nk, nq + 2 * nk)), [], [], dp, next(idents))
            done(["wq", "wk", "wv"], number, sums)
            if number:
                (dh,), _ = states(dq, dkv, h, dh1, w_q, w_k, w_v, [], [], dp, 0)
        ridden(functools.partial(ride, lambda *_: None, grid=(1,), ins=[], outs=[], scratch=[], name="closing"),
               [(0, ["start", "rest"]), (0.5, ["add", "pass_on", "finish"])])
        names = ("wq", "wk", "wv", "wo", "w_gate", "w_up", "w_down")
        return adamw(weights, ms, vs, [[(owns[name, number], *sent[name, number]) for name in names] for number in range(layers)])

    rows, cut = P(("rep", "dp"), None, None), P(None, "dp", None)
    return jax.shard_map(
        step,
        mesh=mesh,
        in_specs=(rows, rows) + (cut,) * 21,
        out_specs=(P("rep", "dp", None),) * 21,
        check_vma=False,
    )
```

```python
import functools

import jax
import jax.numpy as jnp
import numpy as np
from jax import lax
from jax.experimental import pallas as pl
from jax.experimental.pallas import tpu as pltpu
from jax.sharding import PartitionSpec as P

f32, bf16 = jnp.float32, jnp.bfloat16
sh = jax.ShapeDtypeStruct
HEAD = 128
THETA = 10000
NEG = -1e30
HIDDEN = 2 * NEG
LOG2E = 1.4426950408889634
ANY = pl.BlockSpec(memory_space=pl.ANY)
BIG = 63 * 2**20


def dot(a, b, ca=1, cb=0):
    return lax.dot_general(a, b, (((ca,), (cb,)), ((), ())), preferred_element_type=f32)


def _fit(size, want):
    return max(n for n in range(128, want + 1, 128) if size % n == 0)


def once(shape, index):
    return pl.BlockSpec(shape, index, pipeline_mode=pl.Buffered(1))


def whole(a):
    return a, once(a.shape, lambda *_: (0,) * a.ndim)


def rms(wide):
    return lax.rsqrt(jnp.mean(wide * wide, -1, keepdims=True) + 1e-6)


def norm_back(wide, db):
    r = rms(wide)
    return r * db - wide * (r * r * r * (jnp.sum(db * wide, -1, keepdims=True) * (1 / wide.shape[1])))


def params(n, **kw):
    return pltpu.CompilerParams(dimension_semantics=("arbitrary",) * n, vmem_limit_bytes=BIG, **kw)


class Place:
    def __init__(self, dp):
        me = lax.axis_index("dp")
        self.chips = dp // 2
        self.chip, self.core = me // 2, lax.rem(me, 2)
        self.other = 1 - self.core

    def at(self, step):
        return lax.rem(self.chip + step + self.chips, self.chips)

    def slot(self, step, core):
        return 2 * self.at(step) + core

    def partner(self):
        return {"dp": self.slot(0, self.other)}

    def neighbour(self, step):
        return {"dp": self.slot(step, self.core)}


def remote(src, dst, send, recv, device):
    return pltpu.make_async_remote_copy(src_ref=src, dst_ref=dst, send_sem=send, recv_sem=recv, device_id=device,
                                        device_id_type=pl.DeviceIdType.MESH)


def _half(rows):
    return -(-rows // 32) * 16


class Rider:
    greets = ()

    def bind(self, ins, outs, scratch, place):
        bound = object.__new__(type(self))
        bound.__dict__.update(self.__dict__)
        bound.p = place
        bound.refs(ins, outs, scratch)
        return bound


class Gather(Rider):
    greets = (1, -1, 0)

    def __init__(self, w, number, dp, cols=None):
        self.number = number
        self.first, end = cols or (0, w.shape[2])
        self.rows, self.n = w.shape[1], end - self.first
        self.inputs = [w]
        self.outs = [sh((dp, self.rows, self.n), w.dtype)]
        self.scratch = [pltpu.VMEM((self.rows, self.n), w.dtype), pltpu.SemaphoreType.DMA((8,)), pltpu.SemaphoreType.DMA((8,)),
                        pltpu.SemaphoreType.DMA((2,))]

    def refs(self, ins, outs, scratch):
        self.src, self.out = ins[0].at[self.number, :, pl.ds(self.first, self.n)], outs[0]
        self.stage, self.send, self.recv, self.own = scratch

    def _copy(self, t, incoming=False):
        p, half = self.p, _half(self.rows)
        whole, top, low = pl.ds(0, self.rows), pl.ds(0, half), pl.ds(half, self.rows - half)
        step, core, rows, to = (
            (0, p.core, whole, 1), (0, p.core, whole, -1), (0, p.core, whole, 0),
            (-1, p.core, top, 1), (1, p.core, low, -1),
            (-1, p.core, whole, 0), (1, p.core, whole, 0), (2, p.core, whole, 0),
        )[t]
        if incoming:
            step, core = (step, p.other) if to == 0 else (step - to, core)
        at = self.out.at[p.slot(step, core), rows]
        src = self.src if t < 3 and not incoming else at
        return remote(src, at, self.send.at[t], self.recv.at[t], p.partner() if to == 0 else p.neighbour(to))

    def _into(self):
        return pltpu.make_async_copy(self.src, self.stage, self.own.at[0])

    def _out_of(self):
        return pltpu.make_async_copy(self.stage, self.out.at[self.p.slot(0, self.p.core)], self.own.at[1])

    def start(self):
        for t in (0, 1, 2):
            self._copy(t).start()
        self._into().start()

    def forward(self):
        self._copy(0, True).wait_recv()
        self._copy(3).start()
        self._copy(5).start()
        self._copy(1, True).wait_recv()
        self._copy(4).start()
        self._copy(6).start()
        self._into().wait()
        self._out_of().start()

    def last(self):
        self._copy(3, True).wait_recv()
        self._copy(4, True).wait_recv()
        self._copy(7).start()

    def finish(self):
        for t in (2, 5, 6, 7):
            self._copy(t, True).wait_recv()
        for t in range(8):
            self._copy(t).wait_send()
        self._out_of().wait()


class Reduce(Rider):
    greets = (1, -1)

    def __init__(self, blocks):
        self.rows, self.n = blocks.shape[1:]
        half = _half(self.rows)
        self.inputs = [blocks]
        self.outs = [sh((self.rows, self.n), blocks.dtype)] * 2
        parts = [pltpu.VMEM((half, self.n), blocks.dtype), pltpu.VMEM((self.rows - half, self.n), blocks.dtype)]
        self.scratch = parts + parts + [pltpu.SemaphoreType.DMA((6,)), pltpu.SemaphoreType.DMA((6,)), pltpu.SemaphoreType.DMA((2,))]

    def refs(self, ins, outs, scratch):
        self.blocks, (self.before, self.after) = ins[0], outs
        self.top, self.low, self.own_top, self.own_low, self.send, self.recv, self.local = scratch

    def _copy(self, t):
        p, half = self.p, _half(self.rows)
        top, low = pl.ds(0, half), pl.ds(half, self.rows - half)
        block = lambda step, rows: self.blocks.at[p.at(step), rows]
        src, dst, to = (
            (block(2, top), self.top, 1), (block(2, low), self.low, -1),
            (self.own_top, self.before.at[top], 1), (block(1, low), self.before.at[low], 1),
            (block(-1, top), self.after.at[top], -1), (self.own_low, self.after.at[low], -1),
        )[t]
        return remote(src, dst, self.send.at[t], self.recv.at[t], p.neighbour(to))

    def _own(self):
        p, half = self.p, _half(self.rows)
        return (pltpu.make_async_copy(self.blocks.at[p.at(1), pl.ds(0, half)], self.own_top, self.local.at[0]),
                pltpu.make_async_copy(self.blocks.at[p.at(-1), pl.ds(half, self.rows - half)], self.own_low, self.local.at[1]))

    def start(self):
        for t in (0, 1):
            self._copy(t).start()
        for one in self._own():
            one.start()

    def rest(self):
        for t in (3, 4):
            self._copy(t).start()

    def add(self):
        for one in self._own():
            one.wait()
        self._copy(0).wait_recv()
        self.own_top[...] = (self.own_top[...].astype(f32) + self.top[...].astype(f32)).astype(bf16)
        self._copy(1).wait_recv()
        self.own_low[...] = (self.own_low[...].astype(f32) + self.low[...].astype(f32)).astype(bf16)

    def pass_on(self):
        for t in (2, 5):
            self._copy(t).start()

    def finish(self):
        for t in (2, 3, 4, 5):
            self._copy(t).wait_recv()
        for t in range(6):
            self._copy(t).wait_send()


def greet(place, whom):
    for to in whom:
        pl.semaphore_signal(pltpu.get_barrier_semaphore(), inc=1, device_id=place.neighbour(to) if to else place.partner(),
                            device_id_type=pl.DeviceIdType.MESH)


def greeted(whom):
    pl.semaphore_wait(pltpu.get_barrier_semaphore(), len(whom))


def ride(kernel, riders, plan, dp, ident, *, grid, ins, outs, scratch, name, greets=(), meet=None):
    counts = (len(ins), len(outs), len(scratch))
    steps = 1
    for n in grid:
        steps *= n
    whom = tuple(to for to in (1, -1, 0) if to in greets or any(to in r.greets for r in riders))
    plan = ([(meet, [])] if meet is not None else []) + list(plan)

    def body(*refs):
        refs = list(refs)
        take = lambda n: [refs.pop(0) for _ in range(n)]
        own_in, ride_in = take(counts[0]), [take(len(r.inputs)) for r in riders]
        own_out, ride_out = take(counts[1]), [take(len(r.outs)) for r in riders]
        own_scr, ride_scr = take(counts[2]), [take(len(r.scratch)) for r in riders]
        step = 0
        for axis, n in enumerate(grid):
            step = step * n + pl.program_id(axis)
        place = Place(dp) if whom else None
        bound = [r.bind(a, b, c, place) for r, a, b, c in zip(riders, ride_in, ride_out, ride_scr)]

        def act(half):
            for k, (when, what) in enumerate(plan):
                if int(2 * when) % 2 == half:

                    def do(k=k, what=what):
                        if k == 0:
                            greeted(whom)
                        for number, action in what:
                            getattr(bound[number], action)()

                    pl.when(step == int(when))(do)

        if whom:
            pl.when(step == 0)(lambda: greet(place, whom))
        act(0)
        kernel(*own_in, *own_out, *own_scr, place, bound)
        act(1)

    flat = lambda name: [x for r in riders for x in getattr(r, name)]
    got = pl.pallas_call(
        body, grid=grid,
        in_specs=[s for _, s in ins] + [ANY] * len(flat("inputs")),
        out_specs=[s for _, s in outs] + [ANY] * len(flat("outs")),
        out_shape=[s for s, _ in outs] + flat("outs"),
        scratch_shapes=list(scratch) + flat("scratch"),
        compiler_params=params(len(grid), **(dict(collective_id=ident, has_side_effects=True) if whom else {})), name=name,
    )(*[a for a, _ in ins], *flat("inputs"))
    own, rest = got[: counts[1]], list(got[counts[1] :])
    return own, rest


class Voyage:
    def __init__(self, hbm, hold, sems, gu_sems, gathers, place):
        self.hbm, self.hold, self.sems, self.gu_sems, self.gathers, self.place = hbm, hold, sems, gu_sems, gathers, place

    def start(self, group):
        for r in self.gathers[group]:
            r.start()

    def forward(self, group):
        for r in self.gathers[group]:
            r.forward()

    def last(self, group):
        for r in self.gathers[group]:
            r.last()

    def finish(self, group):
        for r in self.gathers[group]:
            r.finish()

    def _loads(self, group):
        name, slot = group[0], group[-1] % 2
        if name == "gu":
            gate, up = self.gathers[group]
            return [pltpu.make_async_copy(r.out.at[:, :, pl.ds(n * HEAD, HEAD)], self.hold[name].at[slot, :, :, pl.ds((2 * n + k) * HEAD, HEAD)],
                                          self.gu_sems.at[slot, 2 * n + k])
                    for n in range(gate.n // HEAD) for k, r in enumerate((gate, up))]
        at = {"qkv": 0, "wo": 3, "wd": 4}[name]
        first, copies = 0, []
        for n, r in enumerate(self.gathers[group]):
            copies.append(pltpu.make_async_copy(r.out, self.hold[name].at[:, :, pl.ds(first, r.n)], self.sems.at[at + n]))
            first += r.n
        return copies

    def load(self, group):
        for one in self._loads(group):
            one.start()

    def loaded(self, group):
        for one in self._loads(group):
            one.wait()


def _matrix(ref):
    return ref[...].reshape(-1, ref.shape[-1])


def _qkv(s, ship, h_ref, a_ref, q_ref, k_ref, v_ref):
    tm = h_ref.shape[0]
    wide = h_ref[...].astype(f32)
    a = (wide * rms(wide)).astype(bf16)
    a_ref[...] = a
    rows = pl.ds(pl.multiple_of(s * tm, tm), tm)
    cos, sin = ship.hold["cos"][rows, :], ship.hold["sin"][rows, :]
    t = dot(a, _matrix(ship.hold["qkv"])).astype(bf16)
    first = 0
    for out_ref in (q_ref, k_ref):
        for n in range(0, out_ref.shape[1], HEAD):
            one = t[:, first + n : first + n + HEAD].astype(f32)
            out_ref[:, n : n + HEAD] = (one * cos + pltpu.roll(one, HEAD // 2, 1) * sin).astype(bf16)
        first += out_ref.shape[1]
    v_ref[...] = t[:, first:]


def _below(bk, bq):
    return lax.broadcasted_iota(jnp.int32, (bk, bq), 1) >= lax.broadcasted_iota(jnp.int32, (bk, bq), 0)


def _attn(iq, ship, q_ref, k_ref, v_ref, h_ref, o_ref, lse_ref, h1_ref, b_ref, top_s, mix_s):
    bq, nh, kv = q_ref.shape[0], q_ref.shape[1] // HEAD, k_ref.shape[1] // HEAD
    g = nh // kv
    e = HEAD**-0.5 * LOG2E
    top_s[...] = jnp.full(top_s.shape, NEG, f32)
    mix_s[...] = jnp.zeros(mix_s.shape, f32)
    ones = jnp.ones((8, bq), bf16)
    at = lambda n: slice(n * HEAD, (n + 1) * HEAD)

    def block(j, _):
        here = pl.ds(pl.multiple_of(j * bq, bq), bq)
        scores = [dot(k_ref[here, at(n // g)], q_ref[:, at(n)], 1, 1) for n in range(nh)]
        values = [jnp.concatenate([v_ref[here, at(i)].T, ones], axis=0) for i in range(kv)]
        weights, keeps = [], []
        for n, s in enumerate(scores):
            old = top_s[n : n + 1, :]
            top = jnp.maximum(old, s.max(axis=0, keepdims=True))
            top_s[n : n + 1, :] = top
            weights.append(jnp.exp2((s - top) * e).astype(bf16))
            keeps.append(jnp.exp2((old - top) * e))
        for n, (p, keep) in enumerate(zip(weights, keeps, strict=True)):
            mix_s[n] = mix_s[n] * keep + dot(values[n // g], p)

    def diagonal():
        half = bq // 2
        keys = [pl.ds(pl.multiple_of(iq * bq + n * half, half), half) for n in range(2)]
        both = [(dot(k_ref[keys[0], at(n // g)], q_ref[:, at(n)], 1, 1), dot(k_ref[keys[1], at(n // g)], q_ref[half:, at(n)], 1, 1))
                for n in range(nh)]
        values = [[jnp.concatenate([v_ref[rows, at(i)].T, ones[:, :half]], axis=0) for rows in keys] for i in range(kv)]
        weights, keeps = [], []
        for n, (s, s2) in enumerate(both):
            s, s2 = jnp.where(_below(half, bq), s, HIDDEN), jnp.where(_below(half, half), s2, HIDDEN)
            old = top_s[n : n + 1, :]
            top = jnp.maximum(old, s.max(axis=0, keepdims=True))
            top = jnp.concatenate([top[:, :half], jnp.maximum(top[:, half:], s2.max(axis=0, keepdims=True))], 1)
            top_s[n : n + 1, :] = top
            weights.append((jnp.exp2((s - top) * e).astype(bf16), jnp.exp2((s2 - top[:, half:]) * e).astype(bf16)))
            keeps.append(jnp.exp2((old - top) * e))
        for n, ((p, p2), keep) in enumerate(zip(weights, keeps, strict=True)):
            mix_s[n] = mix_s[n] * keep + dot(values[n // g][0], p)
            mix_s[n, :, half:] += dot(values[n // g][1], p2)

    lax.fori_loop(0, iq, block, None)
    diagonal()
    for n in range(nh):
        total = mix_s[n, HEAD : HEAD + 1, :]
        o_ref[:, at(n)] = (mix_s[n, :HEAD, :] * (1 / total)).astype(bf16).T
        lse_ref[n : n + 1, :] = top_s[n : n + 1, :] * HEAD**-0.5 + jnp.log(total)
    ship.between(iq)
    _wo(iq, ship, h_ref, o_ref, h1_ref, b_ref)


def _wo(_, ship, h_ref, o_ref, h1_ref, b_ref):
    h1 = h_ref[...] + dot(o_ref[...], _matrix(ship.hold["wo"])).astype(bf16)
    h1_ref[...] = h1
    wide = h1.astype(f32)
    b_ref[...] = (wide * rms(wide)).astype(bf16)


def _gu(per, first, s, ship, b_ref, gu_ref, actt_ref):
    cw = actt_ref.shape[0]
    tb = actt_ref.shape[1]
    rows = pl.ds(pl.multiple_of(lax.rem(s, per) * tb, tb), tb)
    gu = dot(b_ref[rows, :], _matrix(ship.hold["gu"].at[lax.rem(s // per + first, 2)]))
    for n in range(0, cw, HEAD):
        g, u = gu[:, 2 * n : 2 * n + HEAD], gu[:, 2 * n + HEAD : 2 * n + 2 * HEAD]
        p = lax.logistic(g)
        silu = g * p
        gu_ref[:, n : n + HEAD] = u * (p + silu * (1 - p))
        gu_ref[:, cw + n : cw + n + HEAD] = silu
        actt_ref[n : n + HEAD, :] = (silu * u).astype(bf16).T


def _down(s, ship, actt_ref, h1_ref, h2_ref):
    h2_ref[...] = h1_ref[...] + dot(actt_ref[...], _matrix(ship.hold["wd"]), 0, 0).astype(bf16)


RATE, HOP, SIDE = 91.0, 4.0, 2.5
STEPS = {"qkv": [3.3] * 4, "attn": [5.0, 8.0, 11.0, 14.0], "gu": [4.0] * 10, "down": [5.0] * 4}
AHEAD = 12.0


def timetable(phases, groups, need, size, clear):
    script = [{} for _ in phases]
    state = {g: ["wait", 0.0] for g in groups}
    now, link, here = 0.0, 0.0, (0, 0.0)

    def put(act, g):
        script[here[0]].setdefault(here[1], []).append((act, g))

    def step(g, force=False):
        nonlocal now, link
        what, ready = state[g]
        if what in ("wait", "held") or (ready > now and not force):
            return False
        now = max(now, ready)
        if what == "sent":
            link = max(link, now) + size[g] / RATE / 1e3
            state[g] = ["passed", link + HOP]
            put("forward", g)
        elif what == "passed":
            state[g] = ["aside", now + SIDE]
            put("last", g)
        elif what == "aside":
            if clear[g] is not None and (here[0], here[1]) < clear[g]:
                return False
            state[g] = ["held", now + 2.0]
            put("finish", g)
            if g in need:
                put("load", g)
        return True

    def send(g):
        nonlocal link
        link = max(link, now) + 2 * size[g] / RATE / 1e3
        state[g] = ["sent", link + HOP]
        put("start", g)

    def settle():
        for g in groups:
            while step(g):
                pass
        for g in groups:
            if state[g][0] == "wait" and link - now < AHEAD:
                send(g)

    def force(point):
        nonlocal now
        for g in groups:
            if need.get(g) == point:
                if state[g][0] == "wait":
                    send(g)
                while state[g][0] != "held":
                    step(g, True)
                    if state[g][0] != "held":
                        settle()
                now = max(now, state[g][1])
                put("loaded", g)

    for p, (_, _, durations) in enumerate(phases):
        for k, d in enumerate(durations):
            here = (p, float(k))
            force((p, k))
            settle() if k == 0 and p == 0 else None
            now += d
            here = (p, k + 0.25)
            force((p, k + 0.25))
            here = (p, k + 0.5)
            settle()
    for g in groups:
        if state[g][0] == "wait":
            send(g)
        while state[g][0] != "held":
            step(g, True)
    return script, now


def voyage(h, weights, dp, ident, tm=512, bq=512, tb=1024):
    wq, wk, wv, wo, wg, wu, wd = weights
    t, d = h.shape
    layers, ff = wq.shape[0], wg.shape[2]
    nq, nk = wq.shape[2], wk.shape[2]
    cw = _fit(ff, 640)
    nc, per = ff // cw, t // tb
    half = HEAD // 2
    freq = np.float32(THETA) ** (-np.arange(half, dtype=np.float32) / half)
    freq = jnp.asarray(np.concatenate([freq, freq])[None], f32)

    gathers, shapes = {}, {("cos",): sh((t, HEAD), f32), ("sin",): sh((t, HEAD), f32)}
    phases, need, clear = [("open", 0, [5.0])], {}, {}
    for n in range(layers):
        gathers["qkv", n] = [Gather(w, n, dp) for w in (wq, wk, wv)]
        gathers["wo", n] = [Gather(wo, n, dp)]
        for c in range(nc):
            gathers["gu", n, n * nc + c] = [Gather(w, n, dp, (c * cw, c * cw + cw)) for w in (wg, wu)]
        gathers["wd", n] = [Gather(wd, n, dp)]
        first = len(phases)
        names = ["qkv", "attn", "gu"] + (["down"] if n + 1 < layers else [])
        phases += [(name, n, STEPS[name]) for name in names]
        need["qkv", n], need["wo", n] = (first, 0), (first + 1, 0.25)
        for c in range(nc):
            need["gu", n, n * nc + c] = (first + 2, c * per)
            clear["gu", n, n * nc + c + 2] = (first + 2, c * per + per - 0.5)
        if n + 1 < layers:
            need["wd", n] = (first + 3, 0)
        clear["qkv", n + 1], clear["wo", n + 1], clear["wd", n + 1] = (first, 3.5), (first + 1, 3.5), (first + 3, 3.5)
        for name, shape, kind in (("a", (t, d), bf16), ("q", (t, nq), bf16), ("k", (t, nk), bf16), ("v", (t, nk), bf16), ("o", (t, nq), bf16),
                                  ("lse", (nq // HEAD, t), f32), ("h1", (t, d), bf16), ("b", (t, d), bf16), ("gu", (t, 2 * ff), f32),
                                  ("actt", (ff, t), bf16)):
            shapes[name, n] = sh(shape, kind)
        if n + 1 < layers:
            shapes["h", n + 1] = sh((t, d), bf16)
    order = [g for g in gathers if g[0] == "gu"]
    for one, later in zip(order, order[2:]):
        p, k = need[one]
        clear[later] = (p, k + per - 0.5)
    groups = list(gathers)
    size = {g: sum(r.rows * r.n * 2 for r in gathers[g]) for g in groups}
    script, _ = timetable(phases, groups, need, size, {g: clear.get(g) for g in groups})

    rows = lambda n, m=tm: pl.BlockSpec((m, n), lambda s: (s, 0))
    all_of = lambda n: pl.BlockSpec((t, n), lambda s: (0, 0))
    nh = nq // HEAD

    def specs(name, n):
        return {
            "qkv": (_qkv, t // tm, [("h", rows(d))], [("a", rows(d)), ("q", rows(nq)), ("k", rows(nk)), ("v", rows(nk))], []),
            "attn": (_attn, t // bq, [("q", rows(nq, bq)), ("k", all_of(nk)), ("v", all_of(nk)), ("h", rows(d, bq))],
                     [("o", rows(nq, bq)), ("lse", pl.BlockSpec((nh, bq), lambda s: (0, s))), ("h1", rows(d, bq)), ("b", rows(d, bq))],
                     [pltpu.VMEM((nh, bq), f32), pltpu.VMEM((nh, HEAD + 8, bq), f32)]),
            "gu": (functools.partial(_gu, per, n * nc), nc * per, [("b", all_of(d))],
                   [("gu", pl.BlockSpec((tb, 2 * cw), lambda s: (lax.rem(s, per), s // per))),
                    ("actt", pl.BlockSpec((cw, tb), lambda s: (s // per, lax.rem(s, per))))], []),
            "down": (_down, t // tm, [("actt", pl.BlockSpec((ff, tm), lambda s: (0, s))), ("h1", rows(d))], [(("h", n + 1), rows(d))], []),
        }[name]

    share = d // dp
    hold = {"cos": ((t, HEAD), f32), "sin": ((t, HEAD), f32), "qkv": ((dp, share, nq + 2 * nk), bf16), "wo": ((dp, nq // dp, d), bf16),
            "gu": ((2, dp, share, 2 * cw), bf16), "wd": ((dp, ff // dp, d), bf16)}
    riders = [r for g in groups for r in gathers[g]]
    given, keys = [freq, h, *weights], list(shapes)

    def body(*refs):
        refs = list(refs)
        take = lambda n: [refs.pop(0) for _ in range(n)]
        freq_ref, h_ref, *w_refs = take(len(given))
        hbm = dict(zip(keys, take(len(keys)), strict=True))
        hbm["h", 0] = h_ref
        landed = take(len(riders))
        held = dict(zip(hold, take(len(hold)), strict=True))
        sems, gu_sems, table_sems = take(3)
        place = Place(dp)
        which = {id(w): ref for w, ref in zip(weights, w_refs, strict=True)}
        bound, left = {}, list(landed)
        for g in groups:
            bound[g] = [r.bind([which[id(r.inputs[0])]], [left.pop(0)], take(len(r.scratch)), place) for r in gathers[g]]
        ship = Voyage(hbm, held, sems, gu_sems, bound, place)

        def hook(p, s, part):
            for when, acts in script[p].items():
                if int(4 * when) % 4 == part:

                    @pl.when(s == int(when))
                    def _(acts=acts):
                        for act, g in acts:
                            getattr(ship, act)(g)

        greet(place, Gather.greets)
        greeted(Gather.greets)
        hook(0, 0, 0)
        angle = lax.broadcasted_iota(jnp.int32, (t, HEAD), 0).astype(f32) * freq_ref[...]
        held["cos"][...] = jnp.cos(angle)
        sin = jnp.sin(angle)
        held["sin"][...] = jnp.where(lax.broadcasted_iota(jnp.int32, (t, HEAD), 1) < half, -sin, sin)
        hook(0, 0, 2)
        for p, (name, n, _) in enumerate(phases):
            if p == 0:
                continue
            kernel, steps, ins, outs, scratch = specs(name, n)
            ref = lambda key: hbm[key if isinstance(key, tuple) else (key, n)]

            def inside(*scr, p=p, kernel=kernel, steps=steps, ins=ins, outs=outs, ref=ref):
                def at_step(step, *blocks):
                    s = step.index[0]
                    hook(p, s, 0)
                    ship.between = lambda at: hook(p, at, 1)
                    kernel(s, ship, *blocks, *scr)
                    hook(p, s, 2)

                pltpu.emit_pipeline(at_step, grid=(steps,), in_specs=[x for _, x in ins], out_specs=[x for _, x in outs], _explicit_indices=True)(
                    *[ref(key) for key, _ in ins], *[ref(key) for key, _ in outs])

            pl.run_scoped(inside, *scratch)
        tables = [pltpu.make_async_copy(held[key], hbm[key,], table_sems.at[n]) for n, key in enumerate(("cos", "sin"))]
        for one in tables:
            one.start()
        for one in tables:
            one.wait()

    got = list(pl.pallas_call(
        body,
        in_specs=[pl.BlockSpec(memory_space=pltpu.VMEM)] + [ANY] * (len(given) - 1),
        out_specs=[ANY] * (len(keys) + len(riders)),
        out_shape=list(shapes.values()) + [r.outs[0] for r in riders],
        scratch_shapes=[pltpu.VMEM(*x) for x in hold.values()] + [pltpu.SemaphoreType.DMA((5,)), pltpu.SemaphoreType.DMA((2, 2 * cw // HEAD)), pltpu.SemaphoreType.DMA((2,))]
        + [x for r in riders for x in r.scratch],
        compiler_params=pltpu.CompilerParams(vmem_limit_bytes=BIG, collective_id=ident, has_side_effects=True), name="voyage",
    )(*given))
    saved = dict(zip(keys, got, strict=False))
    saved["h", 0] = h
    full, left = {}, got[len(keys) :]
    for g in groups:
        full[g] = [left.pop(0).reshape(-1, r.n) for r in gathers[g]]
    pairs = lambda n: [tuple(full["gu", n, n * nc + c]) for c in range(nc)]
    return saved, [(*full["qkv", n], full["wo", n][0], pairs(n), full["wd", n][0]) for n in range(layers)]


def _mlpb(cw, nc, dh_ref, h1_ref, o_ref, gu_hbm, wo_hbm, wd_hbm, *refs):
    pairs, refs = [refs[2 * n : 2 * n + 2] for n in range(nc)], refs[2 * nc : -2]
    dgu_hbm, dh1_ref, do_ref, delta_ref, wo_s, wgu_s, wd_s, gu_s, dgu_s, dact_s, acc_s, sems, gu_sems, dgu_sems = refs
    i, last = pl.program_id(0), pl.num_programs(0) - 1
    tm, ring = dh_ref.shape[0], gu_s.shape[0]
    chunk = lambda n: [pltpu.make_async_copy(src, wgu_s.at[n, :, pl.ds(k * cw, cw)], sems.at[n, k]) for k, src in enumerate(pairs[n])]
    wo_copy = pltpu.make_async_copy(wo_hbm, wo_s, sems.at[nc, 0])
    wd_copy = pltpu.make_async_copy(wd_hbm, wd_s, sems.at[nc, 1])
    rows = lambda n: pl.ds(pl.multiple_of(n * tm, tm), tm)
    place = lambda n: lax.rem(i * nc + n, ring)
    fetch = lambda block, n, at: pltpu.make_async_copy(gu_hbm.at[rows(block), pl.ds(n * 2 * cw, 2 * cw)], gu_s.at[at], gu_sems.at[at])
    give = lambda block, n: pltpu.make_async_copy(dgu_s.at[n], dgu_hbm.at[rows(block), pl.ds(n * 2 * cw, 2 * cw)], dgu_sems.at[n])

    @pl.when(i == 0)
    def _():
        wd_copy.start()
        for n in range(ring):
            fetch(0, n, n).start()
        for n in range(nc):
            for one in chunk(n):
                one.start()
        wo_copy.start()
        wd_copy.wait()

    def elementwise(n):
        fetch(i, n, place(n)).wait()

        @pl.when(i > 0)
        def _():
            give(i - 1, n).wait()

        both = gu_s.at[place(n)]
        dact = dact_s[:, n * cw : (n + 1) * cw].astype(f32)
        dgu_s[n, :, :cw] = (dact * both[:, :cw]).astype(bf16)
        dgu_s[n, :, cw:] = (dact * both[:, cw:]).astype(bf16)

    def done(n):
        give(i, n).start()
        later = n + ring
        if later < nc:
            fetch(i, later, place(later)).start()
        else:

            @pl.when(i < last)
            def _():
                fetch(i + 1, later - nc, place(later)).start()

    dact_s[...] = dot(dh_ref[...], wd_s[...], 1, 1).astype(bf16)
    elementwise(0)
    for n in range(nc):
        done(n)

        @pl.when(i == 0)
        def _(n=n):
            for one in chunk(n):
                one.wait()

        term = dot(dgu_s[n], wgu_s[n], 1, 1)
        acc_s[...] = term if n == 0 else acc_s[...] + term
        if n + 1 < nc:
            elementwise(n + 1)

    @pl.when(i == 0)
    def _():
        wo_copy.wait()

    db = acc_s[...].astype(bf16).astype(f32)
    dh1 = dh_ref[...] + norm_back(h1_ref[...].astype(f32), db).astype(bf16)
    dh1_ref[...] = dh1
    do = dot(dh1, wo_s[...], 1, 1).astype(bf16)
    do_ref[...] = do
    each = do.astype(f32) * o_ref[...].astype(f32)
    heads = [each[:, n : n + HEAD].sum(-1, keepdims=True) for n in range(0, each.shape[1], HEAD)]
    delta_ref[...] = jnp.concatenate(heads, 1).T

    @pl.when(i == last)
    def _():
        for n in range(nc):
            give(i, n).wait()


def mlpb(dh, gu, h1, o, wo, chunks, wd, riders, plan, dp, ident, tm=512, ring=3):
    t, d = dh.shape
    cw, ff, nc = chunks[0][0].shape[1], wd.shape[0], len(chunks)
    nh = o.shape[1] // HEAD
    rows = lambda n: pl.BlockSpec((tm, n), lambda i: (i, 0))
    return ride(
        functools.partial(_mlpb, cw, nc), riders, plan, dp, ident, grid=(t // tm,),
        ins=[(dh, rows(d)), (h1, rows(d)), (o, rows(o.shape[1])), (gu, ANY), (wo, ANY), (wd, ANY)] + [(a, ANY) for pair in chunks for a in pair],
        outs=[(sh((t, 2 * ff), bf16), ANY), (sh((t, d), bf16), rows(d)), (sh(o.shape, bf16), rows(o.shape[1])),
              (sh((nh, t), f32), pl.BlockSpec((nh, tm), lambda i: (0, i)))],
        scratch=[pltpu.VMEM(wo.shape, bf16), pltpu.VMEM((nc, d, 2 * cw), bf16), pltpu.VMEM(wd.shape, bf16),
                 pltpu.VMEM((ring, tm, 2 * cw), f32), pltpu.VMEM((nc, tm, 2 * cw), bf16), pltpu.VMEM((tm, ff), bf16), pltpu.VMEM((tm, d), f32),
                 pltpu.SemaphoreType.DMA((nc + 1, 2)), pltpu.SemaphoreType.DMA((ring,)), pltpu.SemaphoreType.DMA((nc,))],
        name="mlpb")


def turn_back(t, cos, sin):
    t = t.astype(f32)
    return (t * cos - pltpu.roll(t, HEAD // 2, 1) * sin).astype(bf16)


def _attnb(q_ref, k_ref, v_ref, do_ref, lse_ref, delta_ref, cos_ref, sin_ref, dq_ref, dkv_ref, dq_s, dk_s, dv_s, *_):
    bq, nh, kv = q_ref.shape[0], q_ref.shape[1] // HEAD, k_ref.shape[1] // HEAD
    g = nh // kv
    iq = pl.program_id(0)
    scale = HEAD**-0.5
    e = scale * LOG2E
    at = lambda n: slice(n * HEAD, (n + 1) * HEAD)

    @pl.when(iq == 0)
    def _():
        dk_s[...] = jnp.zeros_like(dk_s)
        dv_s[...] = jnp.zeros_like(dv_s)

    dq_s[...] = jnp.zeros_like(dq_s)

    def block(first, size, queries, masked):
        here = pl.ds(pl.multiple_of(first, size), size)
        ks = [k_ref[here, at(i)] for i in range(kv)]
        vs = [v_ref[here, at(i)] for i in range(kv)]
        for n in range(nh):
            i = n // g
            q, do = q_ref[queries:, at(n)], do_ref[queries:, at(n)]
            s = dot(ks[i], q, 1, 1)
            dp = dot(vs[i], do, 1, 1)
            p = jnp.exp2(s * e - lse_ref[n : n + 1, queries:] * LOG2E)
            if masked:
                p = jnp.where(_below(size, bq - queries), p, 0.0)
            ds = (p * (dp - delta_ref[n : n + 1, queries:])).astype(bf16)
            dv_s[i, here, :] += dot(p.astype(bf16), do)
            dk_s[i, here, :] += dot(ds, q)
            dq_s[n, :, queries:] += dot(ks[i].T, ds)

    lax.fori_loop(0, iq, lambda j, _: block(j * bq, bq, 0, False), None)
    half = bq // 2
    block(iq * bq, half, 0, True)
    block(iq * bq + half, half, half, True)
    mine = pl.ds(pl.multiple_of(iq * bq, bq), bq)
    cos, sin = cos_ref[mine, :], sin_ref[mine, :]
    for n in range(nh):
        dq_ref[:, at(n)] = turn_back((dq_s[n] * scale).astype(bf16).T, cos, sin)

    @pl.when(iq == pl.num_programs(0) - 1)
    def _():
        for i in range(kv):
            dkv_ref[:, at(i)] = turn_back((dk_s[i] * scale).astype(bf16), cos_ref[...], sin_ref[...])
            dkv_ref[:, at(kv + i)] = dv_s[i].astype(bf16)


def attnb(q, k, v, do, lse, delta, cos, sin, riders, plan, dp, ident, bq=512):
    t, nd = q.shape
    nh, kv = nd // HEAD, k.shape[1] // HEAD
    rows = pl.BlockSpec((bq, nd), lambda i: (i, 0))
    stats = pl.BlockSpec((nh, bq), lambda i: (0, i))
    return ride(
        _attnb, riders, plan, dp, grid=(t // bq,),
        ins=[(q, rows), whole(k), whole(v), (do, rows), (lse, stats), (delta, stats), whole(cos), whole(sin)],
        outs=[(sh((t, nd), bf16), rows), (sh((t, 2 * kv * HEAD), bf16), pl.BlockSpec((t, 2 * kv * HEAD), lambda i: (0, 0)))],
        scratch=[pltpu.VMEM((nh, HEAD, bq), f32), pltpu.VMEM((kv, t, HEAD), f32), pltpu.VMEM((kv, t, HEAD), f32)],
        name="attnb", ident=ident)


def _da(dq_ref, dkv_ref, h_ref, dh1_ref, wq_ref, wk_ref, wv_ref, dh_ref, *_):
    nk = wk_ref.shape[1]
    da = dot(dq_ref[...], wq_ref[...], 1, 1) + dot(dkv_ref[:, :nk], wk_ref[...], 1, 1) + dot(dkv_ref[:, nk:], wv_ref[...], 1, 1)
    dh_ref[...] = dh1_ref[...] + norm_back(h_ref[...].astype(f32), da.astype(bf16).astype(f32)).astype(bf16)


def states(dq, dkv, h, dh1, wq, wk, wv, riders, plan, dp, ident, tm=512):
    t, d = h.shape
    rows = lambda n: pl.BlockSpec((tm, n), lambda i: (i, 0))
    return ride(
        _da, riders, plan, dp, grid=(t // tm,),
        ins=[(dq, rows(dq.shape[1])), (dkv, rows(dkv.shape[1])), (h, rows(d)), (dh1, rows(d)), whole(wq), whole(wk), whole(wv)],
        outs=[(sh((t, d), bf16), rows(d))], scratch=[], name="states", ident=ident)


def _wgrad(nt, nr, splits, dp, tall, lhs_hbm, *refs):
    place, _ = refs[-2:]
    rhs, refs = refs[:nr], refs[nr:-2]
    sends, owns = refs[: len(splits)], refs[len(splits) : 2 * len(splits)]
    lhs_s, stage, got, acc, lhs_sem, send_sem, recv_sem = refs[2 * len(splits) :]
    s = pl.program_id(0)
    chips, rows = acc.shape[:2]
    tile = lambda n: remote(stage.at[n], got.at[n], send_sem.at[n], recv_sem.at[n], place.partner())

    def half(which):
        copies = []
        for n in range(chips):
            there = pl.ds(pl.multiple_of((2 * n + (place.core if which else place.other)) * rows, 16 if tall else rows), rows)
            here = pl.ds(n * rows, rows)
            src, dst = (lhs_hbm.at[there], lhs_s.at[which, here]) if tall else (lhs_hbm.at[:, there], lhs_s.at[which, :, here])
            copies.append(pltpu.make_async_copy(src, dst, lhs_sem.at[which, n]))
        return copies

    @pl.when(s == 0)
    def _():
        for one in half(0) + half(1):
            one.start()
        for one in half(0):
            one.wait()

    @pl.when((s > 0) & (s <= nt))
    def _():
        tile(s - 1).start()

    @pl.when(s == nt)
    def _():
        for one in half(1):
            one.wait()

    b = rhs[0][...] if nr == 1 else jnp.concatenate([r[...] for r in rhs], 1)
    term = dot(lhs_s[s // nt], b, 1 if tall else 0, 0).reshape(chips, rows, -1)

    @pl.when(s < nt)
    def _():
        stage[s] = term.astype(bf16)

    @pl.when(s >= nt)
    def _():
        n = s - nt
        tile(n).wait_recv()
        total = term + got[n].astype(f32)
        acc[...] = total
        for (lo, hi), send, own in zip(splits, sends, owns, strict=True):
            send[...] = total[:, :, lo:hi].astype(bf16)
            own[...] = acc[place.chip, :, lo:hi]

    @pl.when(s == 2 * nt - 1)
    def _():
        for n in range(nt):
            tile(n).wait_send()


def wgrad(lhs, tall, rhs, nt, splits, riders, plan, dp, ident):
    m, t = lhs.shape if tall else lhs.shape[::-1]
    chips, rows = dp // 2, m // dp
    w = sum(r.shape[1] for r in rhs) // nt
    at = lambda s: jnp.maximum(s - nt, 0)
    sends = [(sh((chips, rows, nt * (hi - lo)), bf16), pl.BlockSpec((chips, rows, hi - lo), lambda s: (0, 0, at(s)))) for lo, hi in splits]
    owns = [(sh((rows, nt * (hi - lo)), f32), pl.BlockSpec((rows, hi - lo), lambda s: (0, at(s)))) for lo, hi in splits]
    got, rest = ride(
        functools.partial(_wgrad, nt, len(rhs), splits, dp, tall), riders, plan, dp, ident, grid=(2 * nt,),
        ins=[(lhs, ANY)] + [(r, pl.BlockSpec((t, r.shape[1] // nt), lambda s: (0, lax.rem(s, nt)))) for r in rhs],
        outs=sends + owns,
        scratch=[pltpu.VMEM((2, m // 2, t) if tall else (2, t, m // 2), bf16), pltpu.VMEM((nt, chips, rows, w), bf16),
                 pltpu.VMEM((nt, chips, rows, w), bf16), pltpu.VMEM((chips, rows, w), f32), pltpu.SemaphoreType.DMA((2, chips)),
                 pltpu.SemaphoreType.DMA((nt,)), pltpu.SemaphoreType.DMA((nt,))],
        name="wgrad", greets=(0,), meet=1)
    return list(zip(got[: len(splits)], got[len(splits) :], strict=True)), rest


def _adamw(count, layers, *refs):
    refs = list(refs)
    take = lambda n: [refs.pop(0) for _ in range(n)]
    weights, ms, vs = take(count), take(count), take(count)
    terms = [[take(3) for _ in range(count)] for _ in range(layers)]
    outs = take(count), take(count), take(count)
    for number in range(layers):

        @pl.when(pl.program_id(0) == number)
        def _(number=number):
            for k in range(count):
                own, before, after = terms[number][k]
                g = (own[...] + before[...].astype(f32) + after[...].astype(f32)).astype(bf16).astype(f32)
                w = weights[k][0].astype(f32)
                m = 0.9 * ms[k][0] + 0.1 * g
                v = 0.95 * vs[k][0] + 0.05 * g * g
                move = m * lax.rsqrt(v + 1e-8) + 0.1 * w
                outs[0][k][0] = (w - 0.02 * move).astype(bf16)
                outs[1][k][0], outs[2][k][0] = m, v


def adamw(weights, ms, vs, terms, shares=4):
    count, layers = len(weights), weights[0].shape[0]
    specs, grads = [], [[] for _ in range(layers)]
    for w in weights:
        _, rows, n = w.shape
        by_rows = rows % (16 * shares) == 0
        block = (rows // shares, n) if by_rows else (rows, n // shares)
        place = (lambda i: (i, 0)) if by_rows else (lambda i: (0, i))
        specs.append(pl.BlockSpec((1, *block), lambda l, i, place=place: (l, *place(i))))
        for number in range(layers):
            share = lambda l, i, number=number, place=place: place(jnp.where(l < number, 0, jnp.where(l > number, shares - 1, i)))
            grads[number] += [pl.BlockSpec(block, share)] * 3
    outs = pl.pallas_call(
        functools.partial(_adamw, count, layers), grid=(layers, shares),
        in_specs=specs * 3 + [s for one in grads for s in one], out_specs=specs * 3,
        out_shape=[sh(w.shape, bf16) for w in weights] + [sh(w.shape, f32) for w in weights] * 2,
        compiler_params=params(2), name="adamw",
    )(*weights, *ms, *vs, *[a for layer in terms for one in layer for a in one])
    return tuple(outs)


def solution(mesh):
    dp = mesh.shape["dp"]

    def step(x, dy, *arrays):
        weights, ms, vs = (arrays[i : i + 7] for i in (0, 7, 14))
        layers = weights[0].shape[0]
        do = lambda *named: [(r, act) for act, which in named for r in which]
        idents = iter(range(1000))
        saved, fetched = voyage(x[0], weights, dp, next(idents))
        cos, sin = saved["cos",], saved["sin",]
        dh, owns, sent, waiting = dy[0], {}, {}, []

        def done(names, number, pairs):
            for name, (send, own) in zip(names, pairs, strict=True):
                owns[name, number] = own
                waiting.append((name, number, send))

        def ridden(call, times, leave=()):
            taken = [w for w in waiting if w[0] not in leave]
            waiting[:] = [w for w in waiting if w[0] in leave]
            names, riders = [w[:2] for w in taken], [Reduce(w[2]) for w in taken]
            every = range(len(riders))
            plan = [(when, do(*((act, every) for act in acts))) for when, acts in times] if riders else []
            own, got = call(riders, plan, dp, next(idents))
            sent.update({name: tuple(got[2 * n : 2 * n + 2]) for n, name in enumerate(names)})
            return own

        for number in reversed(range(layers)):
            h, a, q, k, vv, o, lse, h1, b, gu, actt = (saved[name, number] for name in ("h", "a", "q", "k", "v", "o", "lse", "h1", "b", "gu", "actt"))
            w_q, w_k, w_v, w_o, pairs, w_d = fetched[number]
            nc, cw = len(pairs), pairs[0][0].shape[1]
            riders, plan = [], []
            if w_d is None:
                riders = [Gather(weights[6], number, dp)]
                plan = [(1, do(("start", [0]))), (3.5, do(("forward", [0]))), (5.5, do(("last", [0]))), (7.5, do(("finish", [0])))]
            sums, got = wgrad(actt, True, [dh], 2, ((0, dh.shape[1] // 2),), riders, plan, dp, next(idents))
            w_d = got[0].reshape(-1, got[0].shape[2]) if riders else w_d
            done(["w_down"], number, sums)
            dgu, dh1, d_o, delta = ridden(functools.partial(mlpb, dh, gu, h1, o, w_o, pairs, w_d),
                                          [(0, ["start", "rest"]), (1.5, ["add"]), (2, ["pass_on"]), (3.5, ["finish"])], ["wq", "wk", "wv"])
            sums, _ = wgrad(o, False, [dh1], 1, ((0, dh1.shape[1]),), [], [], dp, next(idents))
            done(["wo"], number, sums)
            sums = ridden(functools.partial(wgrad, b, False, [dgu], nc, ((0, cw), (cw, 2 * cw))),
                          [(1, ["start", "rest"]), (3.5, ["add"]), (4.5, ["pass_on"]), (9.5, ["finish"])])
            done(["w_gate", "w_up"], number, sums)
            dq, dkv = ridden(functools.partial(attnb, q, k, vv, d_o, lse, delta, cos, sin),
                             [(0, ["start", "rest"]), (1.5, ["add"]), (2, ["pass_on"]), (3.5, ["finish"])], ["w_up"] if number else [])
            nq, nk = q.shape[1], k.shape[1]
            sums, _ = wgrad(a, False, [dq, dkv], 1, ((0, nq), (nq, nq + nk), (nq + nk, nq + 2 * nk)), [], [], dp, next(idents))
            done(["wq", "wk", "wv"], number, sums)
            if number:
                (dh,), _ = states(dq, dkv, h, dh1, w_q, w_k, w_v, [], [], dp, 0)
        ridden(functools.partial(ride, lambda *_: None, grid=(1,), ins=[], outs=[], scratch=[], name="closing"),
               [(0, ["start", "rest"]), (0.5, ["add", "pass_on", "finish"])])
        names = ("wq", "wk", "wv", "wo", "w_gate", "w_up", "w_down")
        return adamw(weights, ms, vs, [[(owns[name, number], *sent[name, number]) for name in names] for number in range(layers)])

    rows, cut = P(("rep", "dp"), None, None), P(None, "dp", None)
    return jax.shard_map(
        step,
        mesh=mesh,
        in_specs=(rows, rows) + (cut,) * 21,
        out_specs=(P("rep", "dp", None),) * 21,
        check_vma=False,
    )
```

```python
import functools

import jax
import jax.numpy as jnp
import numpy as np
from jax import lax
from jax.experimental import pallas as pl
from jax.experimental.pallas import tpu as pltpu
from jax.sharding import PartitionSpec as P

f32, bf16 = jnp.float32, jnp.bfloat16
sh = jax.ShapeDtypeStruct
HEAD = 128
THETA = 10000
NEG = -1e30
HIDDEN = 2 * NEG
LOG2E = 1.4426950408889634
ANY = pl.BlockSpec(memory_space=pl.ANY)
BIG = 63 * 2**20


def dot(a, b, ca=1, cb=0):
    return lax.dot_general(a, b, (((ca,), (cb,)), ((), ())), preferred_element_type=f32)


def _fit(size, want):
    return max(n for n in range(128, want + 1, 128) if size % n == 0)


def once(shape, index):
    return pl.BlockSpec(shape, index, pipeline_mode=pl.Buffered(1))


def whole(a):
    return a, once(a.shape, lambda *_: (0,) * a.ndim)


def rms(wide):
    return lax.rsqrt(jnp.mean(wide * wide, -1, keepdims=True) + 1e-6)


def norm_back(wide, db):
    r = rms(wide)
    return r * db - wide * (r * r * r * (jnp.sum(db * wide, -1, keepdims=True) * (1 / wide.shape[1])))


def params(n, **kw):
    return pltpu.CompilerParams(dimension_semantics=("arbitrary",) * n, vmem_limit_bytes=BIG, **kw)


class Place:
    def __init__(self, dp):
        me = lax.axis_index("dp")
        self.chips = dp // 2
        self.chip, self.core = me // 2, lax.rem(me, 2)
        self.other = 1 - self.core

    def at(self, step):
        return lax.rem(self.chip + step + self.chips, self.chips)

    def slot(self, step, core):
        return 2 * self.at(step) + core

    def partner(self):
        return {"dp": self.slot(0, self.other)}

    def neighbour(self, step):
        return {"dp": self.slot(step, self.core)}


def remote(src, dst, send, recv, device):
    return pltpu.make_async_remote_copy(src_ref=src, dst_ref=dst, send_sem=send, recv_sem=recv, device_id=device,
                                        device_id_type=pl.DeviceIdType.MESH)


def _half(rows):
    return -(-rows // 32) * 16


class Rider:
    greets = ()

    def bind(self, ins, outs, scratch, place):
        bound = object.__new__(type(self))
        bound.__dict__.update(self.__dict__)
        bound.p = place
        bound.refs(ins, outs, scratch)
        return bound


class Gather(Rider):
    greets = (1, -1, 0)

    def __init__(self, w, number, dp, cols=None):
        self.number = number
        self.first, end = cols or (0, w.shape[2])
        self.rows, self.n = w.shape[1], end - self.first
        self.inputs = [w]
        self.outs = [sh((dp, self.rows, self.n), w.dtype)]
        self.scratch = [pltpu.VMEM((self.rows, self.n), w.dtype), pltpu.SemaphoreType.DMA((8,)), pltpu.SemaphoreType.DMA((8,)),
                        pltpu.SemaphoreType.DMA((2,))]

    def refs(self, ins, outs, scratch):
        self.src, self.out = ins[0].at[self.number, :, pl.ds(self.first, self.n)], outs[0]
        self.stage, self.send, self.recv, self.own = scratch

    def _copy(self, t, incoming=False):
        p, half = self.p, _half(self.rows)
        whole, top, low = pl.ds(0, self.rows), pl.ds(0, half), pl.ds(half, self.rows - half)
        step, core, rows, to = (
            (0, p.core, whole, 1), (0, p.core, whole, -1), (0, p.core, whole, 0),
            (-1, p.core, top, 1), (1, p.core, low, -1),
            (-1, p.core, whole, 0), (1, p.core, whole, 0), (2, p.core, whole, 0),
        )[t]
        if incoming:
            step, core = (step, p.other) if to == 0 else (step - to, core)
        at = self.out.at[p.slot(step, core), rows]
        src = self.src if t < 3 and not incoming else at
        return remote(src, at, self.send.at[t], self.recv.at[t], p.partner() if to == 0 else p.neighbour(to))

    def _into(self):
        return pltpu.make_async_copy(self.src, self.stage, self.own.at[0])

    def _out_of(self):
        return pltpu.make_async_copy(self.stage, self.out.at[self.p.slot(0, self.p.core)], self.own.at[1])

    def start(self):
        for t in (0, 1, 2):
            self._copy(t).start()
        self._into().start()

    def forward(self):
        self._copy(0, True).wait_recv()
        self._copy(3).start()
        self._copy(5).start()
        self._copy(1, True).wait_recv()
        self._copy(4).start()
        self._copy(6).start()
        self._into().wait()
        self._out_of().start()

    def last(self):
        self._copy(3, True).wait_recv()
        self._copy(4, True).wait_recv()
        self._copy(7).start()

    def finish(self):
        for t in (2, 5, 6, 7):
            self._copy(t, True).wait_recv()
        for t in range(8):
            self._copy(t).wait_send()
        self._out_of().wait()


class Reduce(Rider):
    greets = (1, -1)

    def __init__(self, blocks):
        self.rows, self.n = blocks.shape[1:]
        half = _half(self.rows)
        self.inputs = [blocks]
        self.outs = [sh((self.rows, self.n), blocks.dtype)] * 2
        parts = [pltpu.VMEM((half, self.n), blocks.dtype), pltpu.VMEM((self.rows - half, self.n), blocks.dtype)]
        self.scratch = parts + parts + [pltpu.SemaphoreType.DMA((6,)), pltpu.SemaphoreType.DMA((6,)), pltpu.SemaphoreType.DMA((2,))]

    def refs(self, ins, outs, scratch):
        self.blocks, (self.before, self.after) = ins[0], outs
        self.top, self.low, self.own_top, self.own_low, self.send, self.recv, self.local = scratch

    def _copy(self, t):
        p, half = self.p, _half(self.rows)
        top, low = pl.ds(0, half), pl.ds(half, self.rows - half)
        block = lambda step, rows: self.blocks.at[p.at(step), rows]
        src, dst, to = (
            (block(2, top), self.top, 1), (block(2, low), self.low, -1),
            (self.own_top, self.before.at[top], 1), (block(1, low), self.before.at[low], 1),
            (block(-1, top), self.after.at[top], -1), (self.own_low, self.after.at[low], -1),
        )[t]
        return remote(src, dst, self.send.at[t], self.recv.at[t], p.neighbour(to))

    def _own(self):
        p, half = self.p, _half(self.rows)
        return (pltpu.make_async_copy(self.blocks.at[p.at(1), pl.ds(0, half)], self.own_top, self.local.at[0]),
                pltpu.make_async_copy(self.blocks.at[p.at(-1), pl.ds(half, self.rows - half)], self.own_low, self.local.at[1]))

    def start(self):
        for t in (0, 1):
            self._copy(t).start()
        for one in self._own():
            one.start()

    def rest(self):
        for t in (3, 4):
            self._copy(t).start()

    def add(self):
        for one in self._own():
            one.wait()
        self._copy(0).wait_recv()
        self.own_top[...] = (self.own_top[...].astype(f32) + self.top[...].astype(f32)).astype(bf16)
        self._copy(1).wait_recv()
        self.own_low[...] = (self.own_low[...].astype(f32) + self.low[...].astype(f32)).astype(bf16)

    def pass_on(self):
        for t in (2, 5):
            self._copy(t).start()

    def finish(self):
        for t in (2, 3, 4, 5):
            self._copy(t).wait_recv()
        for t in range(6):
            self._copy(t).wait_send()


def greet(place, whom):
    for to in whom:
        pl.semaphore_signal(pltpu.get_barrier_semaphore(), inc=1, device_id=place.neighbour(to) if to else place.partner(),
                            device_id_type=pl.DeviceIdType.MESH)


def greeted(whom):
    pl.semaphore_wait(pltpu.get_barrier_semaphore(), len(whom))


def ride(kernel, riders, plan, dp, ident, *, grid, ins, outs, scratch, name, greets=(), meet=None):
    counts = (len(ins), len(outs), len(scratch))
    steps = 1
    for n in grid:
        steps *= n
    whom = tuple(to for to in (1, -1, 0) if to in greets or any(to in r.greets for r in riders))
    plan = ([(meet, [])] if meet is not None else []) + list(plan)

    def body(*refs):
        refs = list(refs)
        take = lambda n: [refs.pop(0) for _ in range(n)]
        own_in, ride_in = take(counts[0]), [take(len(r.inputs)) for r in riders]
        own_out, ride_out = take(counts[1]), [take(len(r.outs)) for r in riders]
        own_scr, ride_scr = take(counts[2]), [take(len(r.scratch)) for r in riders]
        step = 0
        for axis, n in enumerate(grid):
            step = step * n + pl.program_id(axis)
        place = Place(dp) if whom else None
        bound = [r.bind(a, b, c, place) for r, a, b, c in zip(riders, ride_in, ride_out, ride_scr)]

        def act(half):
            for k, (when, what) in enumerate(plan):
                if int(2 * when) % 2 == half:

                    def do(k=k, what=what):
                        if k == 0:
                            greeted(whom)
                        for number, action in what:
                            getattr(bound[number], action)()

                    pl.when(step == int(when))(do)

        if whom:
            pl.when(step == 0)(lambda: greet(place, whom))
        act(0)
        kernel(*own_in, *own_out, *own_scr, place, bound)
        act(1)

    flat = lambda name: [x for r in riders for x in getattr(r, name)]
    got = pl.pallas_call(
        body, grid=grid,
        in_specs=[s for _, s in ins] + [ANY] * len(flat("inputs")),
        out_specs=[s for _, s in outs] + [ANY] * len(flat("outs")),
        out_shape=[s for s, _ in outs] + flat("outs"),
        scratch_shapes=list(scratch) + flat("scratch"),
        compiler_params=params(len(grid), **(dict(collective_id=ident, has_side_effects=True) if whom else {})), name=name,
    )(*[a for a, _ in ins], *flat("inputs"))
    own, rest = got[: counts[1]], list(got[counts[1] :])
    return own, rest


class Voyage:
    def __init__(self, hbm, hold, sems, gu_sems, gathers, place):
        self.hbm, self.hold, self.sems, self.gu_sems, self.gathers, self.place = hbm, hold, sems, gu_sems, gathers, place

    def start(self, group):
        for r in self.gathers[group]:
            r.start()

    def forward(self, group):
        for r in self.gathers[group]:
            r.forward()

    def last(self, group):
        for r in self.gathers[group]:
            r.last()

    def finish(self, group):
        for r in self.gathers[group]:
            r.finish()

    def _loads(self, group):
        name, slot = group[0], group[-1] % 2
        if name == "gu":
            gate, up = self.gathers[group]
            return [pltpu.make_async_copy(r.out.at[:, :, pl.ds(n * HEAD, HEAD)], self.hold[name].at[slot, :, :, pl.ds((2 * n + k) * HEAD, HEAD)],
                                          self.gu_sems.at[slot, 2 * n + k])
                    for n in range(gate.n // HEAD) for k, r in enumerate((gate, up))]
        at = {"qkv": 0, "wo": 3, "wd": 4}[name]
        first, copies = 0, []
        for n, r in enumerate(self.gathers[group]):
            copies.append(pltpu.make_async_copy(r.out, self.hold[name].at[:, :, pl.ds(first, r.n)], self.sems.at[at + n]))
            first += r.n
        return copies

    def load(self, group):
        for one in self._loads(group):
            one.start()

    def loaded(self, group):
        for one in self._loads(group):
            one.wait()


def _matrix(ref):
    return ref[...].reshape(-1, ref.shape[-1])


def _qkv(s, ship, h_ref, a_ref, q_ref, k_ref, v_ref):
    tm = h_ref.shape[0]
    wide = h_ref[...].astype(f32)
    a = (wide * rms(wide)).astype(bf16)
    a_ref[...] = a
    rows = pl.ds(pl.multiple_of(s * tm, tm), tm)
    cos, sin = ship.hold["cos"][rows, :], ship.hold["sin"][rows, :]
    t = dot(a, _matrix(ship.hold["qkv"])).astype(bf16)
    first = 0
    for out_ref in (q_ref, k_ref):
        for n in range(0, out_ref.shape[1], HEAD):
            one = t[:, first + n : first + n + HEAD].astype(f32)
            out_ref[:, n : n + HEAD] = (one * cos + pltpu.roll(one, HEAD // 2, 1) * sin).astype(bf16)
        first += out_ref.shape[1]
    v_ref[...] = t[:, first:]


def _below(bk, bq):
    return lax.broadcasted_iota(jnp.int32, (bk, bq), 1) >= lax.broadcasted_iota(jnp.int32, (bk, bq), 0)


def _attn(iq, ship, q_ref, k_ref, v_ref, h_ref, o_ref, lse_ref, h1_ref, b_ref, top_s, mix_s):
    bq, nh, kv = q_ref.shape[0], q_ref.shape[1] // HEAD, k_ref.shape[1] // HEAD
    g = nh // kv
    e = HEAD**-0.5 * LOG2E
    top_s[...] = jnp.full(top_s.shape, NEG, f32)
    mix_s[...] = jnp.zeros(mix_s.shape, f32)
    ones = jnp.ones((8, bq), bf16)
    at = lambda n: slice(n * HEAD, (n + 1) * HEAD)

    def block(j, _):
        here = pl.ds(pl.multiple_of(j * bq, bq), bq)
        scores = [dot(k_ref[here, at(n // g)], q_ref[:, at(n)], 1, 1) for n in range(nh)]
        values = [jnp.concatenate([v_ref[here, at(i)].T, ones], axis=0) for i in range(kv)]
        weights, keeps = [], []
        for n, s in enumerate(scores):
            old = top_s[n : n + 1, :]
            top = jnp.maximum(old, s.max(axis=0, keepdims=True))
            top_s[n : n + 1, :] = top
            weights.append(jnp.exp2((s - top) * e).astype(bf16))
            keeps.append(jnp.exp2((old - top) * e))
        for n, (p, keep) in enumerate(zip(weights, keeps, strict=True)):
            mix_s[n] = mix_s[n] * keep + dot(values[n // g], p)

    def diagonal():
        half = bq // 2
        keys = [pl.ds(pl.multiple_of(iq * bq + n * half, half), half) for n in range(2)]
        both = [(dot(k_ref[keys[0], at(n // g)], q_ref[:, at(n)], 1, 1), dot(k_ref[keys[1], at(n // g)], q_ref[half:, at(n)], 1, 1))
                for n in range(nh)]
        values = [[jnp.concatenate([v_ref[rows, at(i)].T, ones[:, :half]], axis=0) for rows in keys] for i in range(kv)]
        weights, keeps = [], []
        for n, (s, s2) in enumerate(both):
            s, s2 = jnp.where(_below(half, bq), s, HIDDEN), jnp.where(_below(half, half), s2, HIDDEN)
            old = top_s[n : n + 1, :]
            top = jnp.maximum(old, s.max(axis=0, keepdims=True))
            top = jnp.concatenate([top[:, :half], jnp.maximum(top[:, half:], s2.max(axis=0, keepdims=True))], 1)
            top_s[n : n + 1, :] = top
            weights.append((jnp.exp2((s - top) * e).astype(bf16), jnp.exp2((s2 - top[:, half:]) * e).astype(bf16)))
            keeps.append(jnp.exp2((old - top) * e))
        for n, ((p, p2), keep) in enumerate(zip(weights, keeps, strict=True)):
            mix_s[n] = mix_s[n] * keep + dot(values[n // g][0], p)
            mix_s[n, :, half:] += dot(values[n // g][1], p2)

    lax.fori_loop(0, iq, block, None)
    diagonal()
    for n in range(nh):
        total = mix_s[n, HEAD : HEAD + 1, :]
        o_ref[:, at(n)] = (mix_s[n, :HEAD, :] * (1 / total)).astype(bf16).T
        lse_ref[n : n + 1, :] = top_s[n : n + 1, :] * HEAD**-0.5 + jnp.log(total)
    ship.between(iq)
    _wo(iq, ship, h_ref, o_ref, h1_ref, b_ref)


def _wo(_, ship, h_ref, o_ref, h1_ref, b_ref):
    h1 = h_ref[...] + dot(o_ref[...], _matrix(ship.hold["wo"])).astype(bf16)
    h1_ref[...] = h1
    wide = h1.astype(f32)
    b_ref[...] = (wide * rms(wide)).astype(bf16)


def _gu(per, first, s, ship, b_ref, gu_ref, actt_ref):
    cw = actt_ref.shape[0]
    tb = actt_ref.shape[1]
    rows = pl.ds(pl.multiple_of(lax.rem(s, per) * tb, tb), tb)
    gu = dot(b_ref[rows, :], _matrix(ship.hold["gu"].at[lax.rem(s // per + first, 2)]))
    for n in range(0, cw, HEAD):
        g, u = gu[:, 2 * n : 2 * n + HEAD], gu[:, 2 * n + HEAD : 2 * n + 2 * HEAD]
        p = lax.logistic(g)
        silu = g * p
        gu_ref[:, n : n + HEAD] = u * (p + silu * (1 - p))
        gu_ref[:, cw + n : cw + n + HEAD] = silu
        actt_ref[n : n + HEAD, :] = (silu * u).astype(bf16).T


def _down(s, ship, actt_ref, h1_ref, h2_ref):
    h2_ref[...] = h1_ref[...] + dot(actt_ref[...], _matrix(ship.hold["wd"]), 0, 0).astype(bf16)


RATE, HOP, SIDE = 91.0, 4.0, 2.5
STEPS = {"qkv": [3.3] * 4, "attn": [5.0, 8.0, 11.0, 14.0], "gu": [4.0] * 10, "down": [5.0] * 4}
AHEAD = 12.0


def timetable(phases, groups, need, size, clear):
    script = [{} for _ in phases]
    state = {g: ["wait", 0.0] for g in groups}
    now, link, here = 0.0, 0.0, (0, 0.0)

    def put(act, g):
        script[here[0]].setdefault(here[1], []).append((act, g))

    def step(g, force=False):
        nonlocal now, link
        what, ready = state[g]
        if what in ("wait", "held") or (ready > now and not force):
            return False
        now = max(now, ready)
        if what == "sent":
            link = max(link, now) + size[g] / RATE / 1e3
            state[g] = ["passed", link + HOP]
            put("forward", g)
        elif what == "passed":
            state[g] = ["aside", now + SIDE]
            put("last", g)
        elif what == "aside":
            if clear[g] is not None and (here[0], here[1]) < clear[g]:
                return False
            state[g] = ["held", now + 2.0]
            put("finish", g)
            if g in need:
                put("load", g)
        return True

    def send(g):
        nonlocal link
        link = max(link, now) + 2 * size[g] / RATE / 1e3
        state[g] = ["sent", link + HOP]
        put("start", g)

    def settle():
        for g in groups:
            while step(g):
                pass
        for g in groups:
            if state[g][0] == "wait" and link - now < AHEAD:
                send(g)

    def force(point):
        nonlocal now
        for g in groups:
            if need.get(g) == point:
                if state[g][0] == "wait":
                    send(g)
                while state[g][0] != "held":
                    step(g, True)
                    if state[g][0] != "held":
                        settle()
                now = max(now, state[g][1])
                put("loaded", g)

    for p, (_, _, durations) in enumerate(phases):
        for k, d in enumerate(durations):
            here = (p, float(k))
            force((p, k))
            settle() if k == 0 and p == 0 else None
            now += d
            here = (p, k + 0.25)
            force((p, k + 0.25))
            here = (p, k + 0.5)
            settle()
    for g in groups:
        if state[g][0] == "wait":
            send(g)
        while state[g][0] != "held":
            step(g, True)
    return script, now


def voyage(h, weights, dp, ident, tm=512, bq=512, tb=1024):
    wq, wk, wv, wo, wg, wu, wd = weights
    t, d = h.shape
    layers, ff = wq.shape[0], wg.shape[2]
    nq, nk = wq.shape[2], wk.shape[2]
    cw = _fit(ff, 640)
    nc, per = ff // cw, t // tb
    half = HEAD // 2
    freq = np.float32(THETA) ** (-np.arange(half, dtype=np.float32) / half)
    freq = jnp.asarray(np.concatenate([freq, freq])[None], f32)

    gathers, shapes = {}, {("cos",): sh((t, HEAD), f32), ("sin",): sh((t, HEAD), f32)}
    phases, need, clear = [("open", 0, [5.0])], {}, {}
    for n in range(layers):
        gathers["qkv", n] = [Gather(w, n, dp) for w in (wq, wk, wv)]
        gathers["wo", n] = [Gather(wo, n, dp)]
        for c in range(nc):
            gathers["gu", n, n * nc + c] = [Gather(w, n, dp, (c * cw, c * cw + cw)) for w in (wg, wu)]
        gathers["wd", n] = [Gather(wd, n, dp)]
        first = len(phases)
        names = ["qkv", "attn", "gu"] + (["down"] if n + 1 < layers else [])
        phases += [(name, n, STEPS[name]) for name in names]
        need["qkv", n], need["wo", n] = (first, 0), (first + 1, 0.25)
        for c in range(nc):
            need["gu", n, n * nc + c] = (first + 2, c * per)
            clear["gu", n, n * nc + c + 2] = (first + 2, c * per + per - 0.5)
        if n + 1 < layers:
            need["wd", n] = (first + 3, 0)
        clear["qkv", n + 1], clear["wo", n + 1], clear["wd", n + 1] = (first, 3.5), (first + 1, 3.5), (first + 3, 3.5)
        for name, shape, kind in (("a", (t, d), bf16), ("q", (t, nq), bf16), ("k", (t, nk), bf16), ("v", (t, nk), bf16), ("o", (t, nq), bf16),
                                  ("lse", (nq // HEAD, t), f32), ("h1", (t, d), bf16), ("b", (t, d), bf16), ("gu", (t, 2 * ff), f32),
                                  ("actt", (ff, t), bf16)):
            shapes[name, n] = sh(shape, kind)
        if n + 1 < layers:
            shapes["h", n + 1] = sh((t, d), bf16)
    order = [g for g in gathers if g[0] == "gu"]
    for one, later in zip(order, order[2:]):
        p, k = need[one]
        clear[later] = (p, k + per - 0.5)
    groups = list(gathers)
    size = {g: sum(r.rows * r.n * 2 for r in gathers[g]) for g in groups}
    script, _ = timetable(phases, groups, need, size, {g: clear.get(g) for g in groups})

    rows = lambda n, m=tm: pl.BlockSpec((m, n), lambda s: (s, 0))
    all_of = lambda n: pl.BlockSpec((t, n), lambda s: (0, 0))
    nh = nq // HEAD

    def specs(name, n):
        return {
            "qkv": (_qkv, t // tm, [("h", rows(d))], [("a", rows(d)), ("q", rows(nq)), ("k", rows(nk)), ("v", rows(nk))], []),
            "attn": (_attn, t // bq, [("q", rows(nq, bq)), ("k", all_of(nk)), ("v", all_of(nk)), ("h", rows(d, bq))],
                     [("o", rows(nq, bq)), ("lse", pl.BlockSpec((nh, bq), lambda s: (0, s))), ("h1", rows(d, bq)), ("b", rows(d, bq))],
                     [pltpu.VMEM((nh, bq), f32), pltpu.VMEM((nh, HEAD + 8, bq), f32)]),
            "gu": (functools.partial(_gu, per, n * nc), nc * per, [("b", all_of(d))],
                   [("gu", pl.BlockSpec((tb, 2 * cw), lambda s: (lax.rem(s, per), s // per))),
                    ("actt", pl.BlockSpec((cw, tb), lambda s: (s // per, lax.rem(s, per))))], []),
            "down": (_down, t // tm, [("actt", pl.BlockSpec((ff, tm), lambda s: (0, s))), ("h1", rows(d))], [(("h", n + 1), rows(d))], []),
        }[name]

    share = d // dp
    hold = {"cos": ((t, HEAD), f32), "sin": ((t, HEAD), f32), "qkv": ((dp, share, nq + 2 * nk), bf16), "wo": ((dp, nq // dp, d), bf16),
            "gu": ((2, dp, share, 2 * cw), bf16), "wd": ((dp, ff // dp, d), bf16)}
    riders = [r for g in groups for r in gathers[g]]
    given, keys = [freq, h, *weights], list(shapes)

    def body(*refs):
        refs = list(refs)
        take = lambda n: [refs.pop(0) for _ in range(n)]
        freq_ref, h_ref, *w_refs = take(len(given))
        hbm = dict(zip(keys, take(len(keys)), strict=True))
        hbm["h", 0] = h_ref
        landed = take(len(riders))
        held = dict(zip(hold, take(len(hold)), strict=True))
        sems, gu_sems, table_sems = take(3)
        place = Place(dp)
        which = {id(w): ref for w, ref in zip(weights, w_refs, strict=True)}
        bound, left = {}, list(landed)
        for g in groups:
            bound[g] = [r.bind([which[id(r.inputs[0])]], [left.pop(0)], take(len(r.scratch)), place) for r in gathers[g]]
        ship = Voyage(hbm, held, sems, gu_sems, bound, place)

        def hook(p, s, part):
            for when, acts in script[p].items():
                if int(4 * when) % 4 == part:

                    @pl.when(s == int(when))
                    def _(acts=acts):
                        for act, g in acts:
                            getattr(ship, act)(g)

        greet(place, Gather.greets)
        greeted(Gather.greets)
        hook(0, 0, 0)
        angle = lax.broadcasted_iota(jnp.int32, (t, HEAD), 0).astype(f32) * freq_ref[...]
        held["cos"][...] = jnp.cos(angle)
        sin = jnp.sin(angle)
        held["sin"][...] = jnp.where(lax.broadcasted_iota(jnp.int32, (t, HEAD), 1) < half, -sin, sin)
        hook(0, 0, 2)
        for p, (name, n, _) in enumerate(phases):
            if p == 0:
                continue
            kernel, steps, ins, outs, scratch = specs(name, n)
            ref = lambda key: hbm[key if isinstance(key, tuple) else (key, n)]

            def inside(*scr, p=p, kernel=kernel, steps=steps, ins=ins, outs=outs, ref=ref):
                def at_step(step, *blocks):
                    s = step.index[0]
                    hook(p, s, 0)
                    ship.between = lambda at: hook(p, at, 1)
                    kernel(s, ship, *blocks, *scr)
                    hook(p, s, 2)

                pltpu.emit_pipeline(at_step, grid=(steps,), in_specs=[x for _, x in ins], out_specs=[x for _, x in outs], _explicit_indices=True)(
                    *[ref(key) for key, _ in ins], *[ref(key) for key, _ in outs])

            pl.run_scoped(inside, *scratch)
        tables = [pltpu.make_async_copy(held[key], hbm[key,], table_sems.at[n]) for n, key in enumerate(("cos", "sin"))]
        for one in tables:
            one.start()
        for one in tables:
            one.wait()

    got = list(pl.pallas_call(
        body,
        in_specs=[pl.BlockSpec(memory_space=pltpu.VMEM)] + [ANY] * (len(given) - 1),
        out_specs=[ANY] * (len(keys) + len(riders)),
        out_shape=list(shapes.values()) + [r.outs[0] for r in riders],
        scratch_shapes=[pltpu.VMEM(*x) for x in hold.values()] + [pltpu.SemaphoreType.DMA((5,)), pltpu.SemaphoreType.DMA((2, 2 * cw // HEAD)), pltpu.SemaphoreType.DMA((2,))]
        + [x for r in riders for x in r.scratch],
        compiler_params=pltpu.CompilerParams(vmem_limit_bytes=BIG, collective_id=ident, has_side_effects=True), name="voyage",
    )(*given))
    saved = dict(zip(keys, got, strict=False))
    saved["h", 0] = h
    full, left = {}, got[len(keys) :]
    for g in groups:
        full[g] = [left.pop(0).reshape(-1, r.n) for r in gathers[g]]
    pairs = lambda n: [tuple(full["gu", n, n * nc + c]) for c in range(nc)]
    return saved, [(*full["qkv", n], full["wo", n][0], pairs(n), full["wd", n][0]) for n in range(layers)]


def _mlpb(cw, nc, dh_ref, h1_ref, o_ref, gu_hbm, wo_hbm, wd_hbm, *refs):
    pairs, refs = [refs[2 * n : 2 * n + 2] for n in range(nc)], refs[2 * nc : -2]
    dgu_hbm, dh1_ref, do_ref, delta_ref, wo_s, wgu_s, wd_s, gu_s, dgu_s, dact_s, acc_s, sems, gu_sems, dgu_sems = refs
    i, last = pl.program_id(0), pl.num_programs(0) - 1
    tm, ring = dh_ref.shape[0], gu_s.shape[0]
    chunk = lambda n: [pltpu.make_async_copy(src, wgu_s.at[n, :, pl.ds(k * cw, cw)], sems.at[n, k]) for k, src in enumerate(pairs[n])]
    wo_copy = pltpu.make_async_copy(wo_hbm, wo_s, sems.at[nc, 0])
    wd_copy = pltpu.make_async_copy(wd_hbm, wd_s, sems.at[nc, 1])
    rows = lambda n: pl.ds(pl.multiple_of(n * tm, tm), tm)
    place = lambda n: lax.rem(i * nc + n, ring)
    fetch = lambda block, n, at: pltpu.make_async_copy(gu_hbm.at[rows(block), pl.ds(n * 2 * cw, 2 * cw)], gu_s.at[at], gu_sems.at[at])
    give = lambda block, n: pltpu.make_async_copy(dgu_s.at[n], dgu_hbm.at[rows(block), pl.ds(n * 2 * cw, 2 * cw)], dgu_sems.at[n])

    @pl.when(i == 0)
    def _():
        wd_copy.start()
        for n in range(ring):
            fetch(0, n, n).start()
        for n in range(nc):
            for one in chunk(n):
                one.start()
        wo_copy.start()
        wd_copy.wait()

    def elementwise(n):
        fetch(i, n, place(n)).wait()

        @pl.when(i > 0)
        def _():
            give(i - 1, n).wait()

        both = gu_s.at[place(n)]
        dact = dact_s[:, n * cw : (n + 1) * cw].astype(f32)
        dgu_s[n, :, :cw] = (dact * both[:, :cw]).astype(bf16)
        dgu_s[n, :, cw:] = (dact * both[:, cw:]).astype(bf16)

    def done(n):
        give(i, n).start()
        later = n + ring
        if later < nc:
            fetch(i, later, place(later)).start()
        else:

            @pl.when(i < last)
            def _():
                fetch(i + 1, later - nc, place(later)).start()

    dact_s[...] = dot(dh_ref[...], wd_s[...], 1, 1).astype(bf16)
    elementwise(0)
    for n in range(nc):
        done(n)

        @pl.when(i == 0)
        def _(n=n):
            for one in chunk(n):
                one.wait()

        term = dot(dgu_s[n], wgu_s[n], 1, 1)
        acc_s[...] = term if n == 0 else acc_s[...] + term
        if n + 1 < nc:
            elementwise(n + 1)

    @pl.when(i == 0)
    def _():
        wo_copy.wait()

    db = acc_s[...].astype(bf16).astype(f32)
    dh1 = dh_ref[...] + norm_back(h1_ref[...].astype(f32), db).astype(bf16)
    dh1_ref[...] = dh1
    do = dot(dh1, wo_s[...], 1, 1).astype(bf16)
    do_ref[...] = do
    each = do.astype(f32) * o_ref[...].astype(f32)
    heads = [each[:, n : n + HEAD].sum(-1, keepdims=True) for n in range(0, each.shape[1], HEAD)]
    delta_ref[...] = jnp.concatenate(heads, 1).T

    @pl.when(i == last)
    def _():
        for n in range(nc):
            give(i, n).wait()


def mlpb(dh, gu, h1, o, wo, chunks, wd, riders, plan, dp, ident, tm=512, ring=3):
    t, d = dh.shape
    cw, ff, nc = chunks[0][0].shape[1], wd.shape[0], len(chunks)
    nh = o.shape[1] // HEAD
    rows = lambda n: pl.BlockSpec((tm, n), lambda i: (i, 0))
    return ride(
        functools.partial(_mlpb, cw, nc), riders, plan, dp, ident, grid=(t // tm,),
        ins=[(dh, rows(d)), (h1, rows(d)), (o, rows(o.shape[1])), (gu, ANY), (wo, ANY), (wd, ANY)] + [(a, ANY) for pair in chunks for a in pair],
        outs=[(sh((t, 2 * ff), bf16), ANY), (sh((t, d), bf16), rows(d)), (sh(o.shape, bf16), rows(o.shape[1])),
              (sh((nh, t), f32), pl.BlockSpec((nh, tm), lambda i: (0, i)))],
        scratch=[pltpu.VMEM(wo.shape, bf16), pltpu.VMEM((nc, d, 2 * cw), bf16), pltpu.VMEM(wd.shape, bf16),
                 pltpu.VMEM((ring, tm, 2 * cw), f32), pltpu.VMEM((nc, tm, 2 * cw), bf16), pltpu.VMEM((tm, ff), bf16), pltpu.VMEM((tm, d), f32),
                 pltpu.SemaphoreType.DMA((nc + 1, 2)), pltpu.SemaphoreType.DMA((ring,)), pltpu.SemaphoreType.DMA((nc,))],
        name="mlpb")


def turn_back(t, cos, sin):
    t = t.astype(f32)
    return (t * cos - pltpu.roll(t, HEAD // 2, 1) * sin).astype(bf16)


def _attnb(q_ref, k_ref, v_ref, do_ref, lse_ref, delta_ref, cos_ref, sin_ref, dq_ref, dkv_ref, dq_s, dk_s, dv_s, *_):
    bq, nh, kv = q_ref.shape[0], q_ref.shape[1] // HEAD, k_ref.shape[1] // HEAD
    g = nh // kv
    iq = pl.program_id(0)
    scale = HEAD**-0.5
    e = scale * LOG2E
    at = lambda n: slice(n * HEAD, (n + 1) * HEAD)

    @pl.when(iq == 0)
    def _():
        dk_s[...] = jnp.zeros_like(dk_s)
        dv_s[...] = jnp.zeros_like(dv_s)

    dq_s[...] = jnp.zeros_like(dq_s)

    def block(first, size, queries, masked):
        here = pl.ds(pl.multiple_of(first, size), size)
        ks = [k_ref[here, at(i)] for i in range(kv)]
        vs = [v_ref[here, at(i)] for i in range(kv)]
        for n in range(nh):
            i = n // g
            q, do = q_ref[queries:, at(n)], do_ref[queries:, at(n)]
            s = dot(ks[i], q, 1, 1)
            dp = dot(vs[i], do, 1, 1)
            p = jnp.exp2(s * e - lse_ref[n : n + 1, queries:] * LOG2E)
            if masked:
                p = jnp.where(_below(size, bq - queries), p, 0.0)
            ds = (p * (dp - delta_ref[n : n + 1, queries:])).astype(bf16)
            dv_s[i, here, :] += dot(p.astype(bf16), do)
            dk_s[i, here, :] += dot(ds, q)
            dq_s[n, :, queries:] += dot(ks[i].T, ds)

    lax.fori_loop(0, iq, lambda j, _: block(j * bq, bq, 0, False), None)
    half = bq // 2
    block(iq * bq, half, 0, True)
    block(iq * bq + half, half, half, True)
    mine = pl.ds(pl.multiple_of(iq * bq, bq), bq)
    cos, sin = cos_ref[mine, :], sin_ref[mine, :]
    for n in range(nh):
        dq_ref[:, at(n)] = turn_back((dq_s[n] * scale).astype(bf16).T, cos, sin)

    @pl.when(iq == pl.num_programs(0) - 1)
    def _():
        for i in range(kv):
            dkv_ref[:, at(i)] = turn_back((dk_s[i] * scale).astype(bf16), cos_ref[...], sin_ref[...])
            dkv_ref[:, at(kv + i)] = dv_s[i].astype(bf16)


def attnb(q, k, v, do, lse, delta, cos, sin, riders, plan, dp, ident, bq=512):
    t, nd = q.shape
    nh, kv = nd // HEAD, k.shape[1] // HEAD
    rows = pl.BlockSpec((bq, nd), lambda i: (i, 0))
    stats = pl.BlockSpec((nh, bq), lambda i: (0, i))
    return ride(
        _attnb, riders, plan, dp, grid=(t // bq,),
        ins=[(q, rows), whole(k), whole(v), (do, rows), (lse, stats), (delta, stats), whole(cos), whole(sin)],
        outs=[(sh((t, nd), bf16), rows), (sh((t, 2 * kv * HEAD), bf16), pl.BlockSpec((t, 2 * kv * HEAD), lambda i: (0, 0)))],
        scratch=[pltpu.VMEM((nh, HEAD, bq), f32), pltpu.VMEM((kv, t, HEAD), f32), pltpu.VMEM((kv, t, HEAD), f32)],
        name="attnb", ident=ident)


def _da(dq_ref, dkv_ref, h_ref, dh1_ref, wq_ref, wk_ref, wv_ref, dh_ref, *_):
    nk = wk_ref.shape[1]
    da = dot(dq_ref[...], wq_ref[...], 1, 1) + dot(dkv_ref[:, :nk], wk_ref[...], 1, 1) + dot(dkv_ref[:, nk:], wv_ref[...], 1, 1)
    dh_ref[...] = dh1_ref[...] + norm_back(h_ref[...].astype(f32), da.astype(bf16).astype(f32)).astype(bf16)


def states(dq, dkv, h, dh1, wq, wk, wv, riders, plan, dp, ident, tm=512):
    t, d = h.shape
    rows = lambda n: pl.BlockSpec((tm, n), lambda i: (i, 0))
    return ride(
        _da, riders, plan, dp, grid=(t // tm,),
        ins=[(dq, rows(dq.shape[1])), (dkv, rows(dkv.shape[1])), (h, rows(d)), (dh1, rows(d)), whole(wq), whole(wk), whole(wv)],
        outs=[(sh((t, d), bf16), rows(d))], scratch=[], name="states", ident=ident)


def _wgrad(nt, nr, splits, dp, tall, lhs_hbm, *refs):
    place, _ = refs[-2:]
    rhs, refs = refs[:nr], refs[nr:-2]
    sends, owns = refs[: len(splits)], refs[len(splits) : 2 * len(splits)]
    lhs_s, stage, got, acc, lhs_sem, send_sem, recv_sem = refs[2 * len(splits) :]
    s = pl.program_id(0)
    chips, rows = acc.shape[:2]
    tile = lambda n: remote(stage.at[n], got.at[n], send_sem.at[n], recv_sem.at[n], place.partner())

    def half(which):
        copies = []
        for n in range(chips):
            there = pl.ds(pl.multiple_of((2 * n + (place.core if which else place.other)) * rows, 16 if tall else rows), rows)
            here = pl.ds(n * rows, rows)
            src, dst = (lhs_hbm.at[there], lhs_s.at[which, here]) if tall else (lhs_hbm.at[:, there], lhs_s.at[which, :, here])
            copies.append(pltpu.make_async_copy(src, dst, lhs_sem.at[which, n]))
        return copies

    @pl.when(s == 0)
    def _():
        for one in half(0) + half(1):
            one.start()
        for one in half(0):
            one.wait()

    @pl.when((s > 0) & (s <= nt))
    def _():
        tile(s - 1).start()

    @pl.when(s == nt)
    def _():
        for one in half(1):
            one.wait()

    b = rhs[0][...] if nr == 1 else jnp.concatenate([r[...] for r in rhs], 1)
    term = dot(lhs_s[s // nt], b, 1 if tall else 0, 0).reshape(chips, rows, -1)

    @pl.when(s < nt)
    def _():
        stage[s] = term.astype(bf16)

    @pl.when(s >= nt)
    def _():
        n = s - nt
        tile(n).wait_recv()
        total = term + got[n].astype(f32)
        acc[...] = total
        for (lo, hi), send, own in zip(splits, sends, owns, strict=True):
            send[...] = total[:, :, lo:hi].astype(bf16)
            own[...] = acc[place.chip, :, lo:hi]

    @pl.when(s == 2 * nt - 1)
    def _():
        for n in range(nt):
            tile(n).wait_send()


def wgrad(lhs, tall, rhs, nt, splits, riders, plan, dp, ident):
    m, t = lhs.shape if tall else lhs.shape[::-1]
    chips, rows = dp // 2, m // dp
    w = sum(r.shape[1] for r in rhs) // nt
    at = lambda s: jnp.maximum(s - nt, 0)
    sends = [(sh((chips, rows, nt * (hi - lo)), bf16), pl.BlockSpec((chips, rows, hi - lo), lambda s: (0, 0, at(s)))) for lo, hi in splits]
    owns = [(sh((rows, nt * (hi - lo)), f32), pl.BlockSpec((rows, hi - lo), lambda s: (0, at(s)))) for lo, hi in splits]
    got, rest = ride(
        functools.partial(_wgrad, nt, len(rhs), splits, dp, tall), riders, plan, dp, ident, grid=(2 * nt,),
        ins=[(lhs, ANY)] + [(r, pl.BlockSpec((t, r.shape[1] // nt), lambda s: (0, lax.rem(s, nt)))) for r in rhs],
        outs=sends + owns,
        scratch=[pltpu.VMEM((2, m // 2, t) if tall else (2, t, m // 2), bf16), pltpu.VMEM((nt, chips, rows, w), bf16),
                 pltpu.VMEM((nt, chips, rows, w), bf16), pltpu.VMEM((chips, rows, w), f32), pltpu.SemaphoreType.DMA((2, chips)),
                 pltpu.SemaphoreType.DMA((nt,)), pltpu.SemaphoreType.DMA((nt,))],
        name="wgrad", greets=(0,), meet=1)
    return list(zip(got[: len(splits)], got[len(splits) :], strict=True)), rest


def _sum(terms):
    g = terms[0][...].astype(f32)
    for term in terms[1:]:
        g += term[...].astype(f32)
    return g.astype(bf16).astype(f32)


def _share(rows, n, shares):
    if rows % (16 * shares) == 0:
        return (rows // shares, n), lambda i: (i, 0)
    return (rows, n // shares), lambda i: (0, i)


def _totals(count, *refs):
    for k in range(count):
        refs[3 * count + k][...] = _sum(refs[3 * k : 3 * k + 3]).astype(bf16)


def totals(terms, riders, plan, dp, ident, shares=4):
    ins, outs = [], []
    for one in terms:
        rows, n = one[0].shape
        block, place = _share(rows, n, shares)
        spec = pl.BlockSpec(block, lambda i, place=place: place(i))
        ins += [(a, spec) for a in one]
        outs.append((sh((rows, n), bf16), spec))
    return ride(lambda *refs: _totals(len(terms), *refs[:-2]), riders, plan, dp, ident, grid=(shares,), ins=ins, outs=outs, scratch=[], name="totals")


def _adamw(count, lengths, *refs):
    refs = list(refs)
    take = lambda n: [refs.pop(0) for _ in range(n)]
    weights, ms, vs = take(count), take(count), take(count)
    terms = [[take(n) for n in layer] for layer in lengths]
    outs = take(count), take(count), take(count)
    for number in range(len(lengths)):

        @pl.when(pl.program_id(0) == number)
        def _(number=number):
            for k in range(count):
                g = _sum(terms[number][k])
                w = weights[k][0].astype(f32)
                m = 0.9 * ms[k][0] + 0.1 * g
                v = 0.95 * vs[k][0] + 0.05 * g * g
                move = m * lax.rsqrt(v + 1e-8) + 0.1 * w
                outs[0][k][0] = (w - 0.02 * move).astype(bf16)
                outs[1][k][0], outs[2][k][0] = m, v


def adamw(weights, ms, vs, terms, shares=2):
    count, layers = len(weights), len(terms)
    specs, grads = [], [[] for _ in range(layers)]
    for k, w in enumerate(weights):
        block, place = _share(w.shape[1], w.shape[2], shares)
        specs.append(pl.BlockSpec((1, *block), lambda l, i, place=place: (l, *place(i))))
        for number in range(layers):
            share = lambda l, i, number=number, place=place: place(jnp.where(l < number, 0, jnp.where(l > number, shares - 1, i)))
            grads[number] += [pl.BlockSpec(block, share)] * len(terms[number][k])
    outs = pl.pallas_call(
        functools.partial(_adamw, count, [[len(one) for one in layer] for layer in terms]), grid=(layers, shares),
        in_specs=specs * 3 + [s for one in grads for s in one], out_specs=specs * 3,
        out_shape=[sh(w.shape, bf16) for w in weights] + [sh(w.shape, f32) for w in weights] * 2,
        compiler_params=params(2), name="adamw",
    )(*weights, *ms, *vs, *[a for layer in terms for one in layer for a in one])
    return tuple(outs)


def solution(mesh):
    dp = mesh.shape["dp"]

    def step(x, dy, *arrays):
        weights, ms, vs = (arrays[i : i + 7] for i in (0, 7, 14))
        layers = weights[0].shape[0]
        do = lambda *named: [(r, act) for act, which in named for r in which]
        idents = iter(range(1000))
        saved, fetched = voyage(x[0], weights, dp, next(idents))
        cos, sin = saved["cos",], saved["sin",]
        dh, owns, sent, waiting = dy[0], {}, {}, []

        def done(names, number, pairs):
            for name, (send, own) in zip(names, pairs, strict=True):
                owns[name, number] = own
                waiting.append((name, number, send))

        def ridden(call, times, leave=()):
            taken = [w for w in waiting if w[0] not in leave]
            waiting[:] = [w for w in waiting if w[0] in leave]
            names, riders = [w[:2] for w in taken], [Reduce(w[2]) for w in taken]
            every = range(len(riders))
            plan = [(when, do(*((act, every) for act in acts))) for when, acts in times] if riders else []
            own, got = call(riders, plan, dp, next(idents))
            sent.update({name: tuple(got[2 * n : 2 * n + 2]) for n, name in enumerate(names)})
            return own

        for number in reversed(range(layers)):
            h, a, q, k, vv, o, lse, h1, b, gu, actt = (saved[name, number] for name in ("h", "a", "q", "k", "v", "o", "lse", "h1", "b", "gu", "actt"))
            w_q, w_k, w_v, w_o, pairs, w_d = fetched[number]
            nc, cw = len(pairs), pairs[0][0].shape[1]
            riders, plan = [], []
            if w_d is None:
                riders = [Gather(weights[6], number, dp)]
                plan = [(1, do(("start", [0]))), (3.5, do(("forward", [0]))), (5.5, do(("last", [0]))), (7.5, do(("finish", [0])))]
            sums, got = wgrad(actt, True, [dh], 2, ((0, dh.shape[1] // 2),), riders, plan, dp, next(idents))
            w_d = got[0].reshape(-1, got[0].shape[2]) if riders else w_d
            done(["w_down"], number, sums)
            dgu, dh1, d_o, delta = ridden(functools.partial(mlpb, dh, gu, h1, o, w_o, pairs, w_d),
                                          [(0, ["start", "rest"]), (1.5, ["add"]), (2, ["pass_on"]), (3.5, ["finish"])], ["wq", "wk", "wv"])
            sums, _ = wgrad(o, False, [dh1], 1, ((0, dh1.shape[1]),), [], [], dp, next(idents))
            done(["wo"], number, sums)
            sums = ridden(functools.partial(wgrad, b, False, [dgu], nc, ((0, cw), (cw, 2 * cw))),
                          [(1, ["start", "rest"]), (3.5, ["add"]), (4.5, ["pass_on"]), (9.5, ["finish"])])
            done(["w_gate", "w_up"], number, sums)
            dq, dkv = ridden(functools.partial(attnb, q, k, vv, d_o, lse, delta, cos, sin),
                             [(0, ["start", "rest"]), (1.5 if number else 2.5, ["add"]), (2 if number else 3, ["pass_on"]), (3.5, ["finish"])], ["w_up"] if number else [])
            nq, nk = q.shape[1], k.shape[1]
            sums, _ = wgrad(a, False, [dq, dkv], 1, ((0, nq), (nq, nq + nk), (nq + nk, nq + 2 * nk)), [], [], dp, next(idents))
            done(["wq", "wk", "wv"], number, sums)
            if number:
                (dh,), _ = states(dq, dkv, h, dh1, w_q, w_k, w_v, [], [], dp, 0)
        names = ("wq", "wk", "wv", "wo", "w_gate", "w_up", "w_down")
        there = [(name, number) for number in range(layers) for name in names if (name, number) in sent]
        sums = ridden(functools.partial(totals, [(owns[one], *sent[one]) for one in there]),
                      [(0, ["start", "rest"]), (2.5, ["add"]), (3, ["pass_on"]), (3.5, ["finish"])])
        total = dict(zip(there, sums, strict=True))
        terms = [[(total[one],) if one in total else (owns[one], *sent[one]) for one in ((name, number) for name in names)] for number in range(layers)]
        return adamw(weights, ms, vs, terms)

    rows, cut = P(("rep", "dp"), None, None), P(None, "dp", None)
    return jax.shard_map(
        step,
        mesh=mesh,
        in_specs=(rows, rows) + (cut,) * 21,
        out_specs=(P("rep", "dp", None),) * 21,
        check_vma=False,
    )
```
